32 devices in a mesh: replica: 4 (over x, y), ep: 8 (over z, core).
Axes of the slice: x: 2, y: 2, z: 4, core: 2. Of those that a mesh axis runs over, the one named last changes fastest.
Arguments:
- x: bfloat16 [128, 128, 2048], P(('replica', 'ep')), parts along dimension 0
- wq: bfloat16 [2048, 4096], P('ep')
- wk: bfloat16 [2048, 4096], P('ep')
- wv: bfloat16 [2048, 4096], P('ep')
- wo: bfloat16 [4096, 2048], P('ep')
- wr: float32 [2048, 128], replicated
- w1: bfloat16 [128, 2048, 768], P('ep')
- w3: bfloat16 [128, 2048, 768], P('ep')
- w2: bfloat16 [128, 768, 2048], P('ep')
- idx: int32 [128, 128, 8], P(('replica', 'ep')), parts along dimension 0
Outputs:
- output: bfloat16 [128, 128, 2048], P(('replica', 'ep')), parts along dimension 0
There are 4 independent parts. The reference program is written for one: setup_inputs(seed, part) draws one part's arguments, and reference() takes and returns one part's arrays. A program takes and returns all parts, laid end to end along the dimension named above; an argument that names none is the same for every part.
All inputs are finite; a program needn't handle non-finite values.
Results may differ from the reference program's by a relative error of at most 0.01184.
Values are sent between devices in bfloat16 or wider.
A program may use at most 1 GiB of HBM per device.

```python
import math
import jax
import jax.numpy as jnp
from jax import lax

D = 2048
HEADS = 32
HEAD = 128
EXPERTS = 128
TOP = 8
FF = 768
SEQ = 128
NSEQ = 32
BLOCK = 128

T = NSEQ * SEQ
NHOT = max(1, TOP // 4)
EPS = 1e-6
THETA = 10000.0


def setup_inputs(seed: int = 0, part: int = 0) -> dict:
    key = jax.random.PRNGKey(seed)
    ks = jax.random.split(key, 9)
    kp = jax.random.fold_in(ks[8], part)
    kx, _, _ = jax.random.split(kp, 3)
    kh, kg = jax.random.split(jax.random.fold_in(kp, 7), 2)
    hd = HEADS * HEAD

    def w(k, shape, scale):
        return (jax.random.normal(k, shape, jnp.float32) * scale).astype(jnp.bfloat16)

    x = jax.random.normal(kx, (NSEQ, SEQ, D), jnp.float32).astype(jnp.bfloat16)
    wq = w(ks[0], (D, hd), 1.6 / math.sqrt(D))
    wk = w(ks[1], (D, hd), 1.6 / math.sqrt(D))
    wv = w(ks[2], (D, hd), 1.0 / math.sqrt(D))
    wo = w(ks[3], (hd, D), 1.5 / math.sqrt(hd))
    wr = jax.random.normal(ks[4], (D, EXPERTS), jnp.float32) / math.sqrt(D)
    w1 = w(ks[5], (EXPERTS, D, FF), 1.0 / math.sqrt(D))
    w3 = w(ks[6], (EXPERTS, D, FF), 1.0 / math.sqrt(D))
    w2 = w(ks[7], (EXPERTS, FF, D), 2.0 / math.sqrt(FF))
    nhot = max(1, TOP // 2)
    start = jax.random.randint(kh, (), 0, EXPERTS)
    hot = (start + jnp.arange(nhot)) % EXPERTS
    t = jnp.arange(T)
    int_noise = (jax.random.bits(kg, (T, EXPERTS), jnp.uint32) >> 12).astype(jnp.int32)
    hot_bonus = jnp.zeros((EXPERTS,), jnp.int32).at[hot].set((9 << 20) // 10)
    int_score = (int_noise + hot_bonus).at[t, t % EXPERTS].set(1 << 24)
    int_score = int_score * EXPERTS + jnp.arange(EXPERTS, dtype=jnp.int32)
    idx = lax.top_k(int_score, TOP)[1].astype(jnp.int32).reshape(NSEQ, SEQ, TOP)
    return dict(x=x, wq=wq, wk=wk, wv=wv, wo=wo, wr=wr, w1=w1, w3=w3, w2=w2, idx=idx)


def rmsnorm(v):
    v = v.astype(jnp.float32)
    return v * lax.rsqrt(jnp.mean(v * v, axis=-1, keepdims=True) + EPS)


def rope(z):
    n = z.shape[-3]
    half = HEAD // 2
    freq = THETA ** (-jnp.arange(half, dtype=jnp.float32) / half)
    ang = jnp.arange(n, dtype=jnp.float32)[:, None] * freq
    c = jnp.cos(ang)[:, None, :]
    s = jnp.sin(ang)[:, None, :]
    z1, z2 = z[..., :half], z[..., half:]
    return jnp.concatenate([z1 * c - z2 * s, z2 * c + z1 * s], axis=-1)


def block_plan(eid, ne, cap):
    m = eid.shape[0]
    nb = (cap + ne * (BLOCK - 1)) // BLOCK + 1
    counts = jnp.bincount(eid, length=ne + 1)[:ne]
    nblk = (counts + BLOCK - 1) // BLOCK
    bend = jnp.cumsum(nblk)
    first = jnp.cumsum(counts) - counts
    order = jnp.argsort(eid)
    se = eid[order]
    sc = jnp.minimum(se, ne - 1)
    slot = jnp.where(se < ne, (bend[sc] - nblk[sc]) * BLOCK + jnp.arange(m) - first[sc], nb * BLOCK)
    cand = jnp.full((nb * BLOCK,), m, jnp.int32).at[slot].set(order.astype(jnp.int32), mode='drop')
    blk_e = jnp.minimum(jnp.searchsorted(bend, jnp.arange(nb), side='right'), ne - 1)
    return cand.reshape(nb, BLOCK), blk_e, bend[-1]


def expert_sum(rows, eid, gates, k, w1, w3, w2, cap):
    n, d = rows.shape
    ne = w1.shape[0]
    m = n * k
    cand, blk_e, nused = block_plan(eid, ne, cap)
    ok = cand < m
    row = jnp.where(ok, cand // k, 0)
    gate = jnp.where(ok, gates[jnp.minimum(cand, m - 1)], 0.0)

    def body(acc, xs):
        b, rb, gb, e = xs

        def work(acc):
            xb = rows[rb]
            a1 = jnp.dot(xb, w1[e], preferred_element_type=jnp.float32)
            a3 = jnp.dot(xb, w3[e], preferred_element_type=jnp.float32)
            act = (jax.nn.silu(a1) * a3).astype(jnp.bfloat16)
            o = jnp.dot(act, w2[e], preferred_element_type=jnp.float32).astype(jnp.bfloat16)
            return acc.at[rb].add(gb[:, None] * o.astype(jnp.float32))

        return lax.cond(b < nused, work, lambda acc: acc, acc), None

    acc, _ = lax.scan(body, jnp.zeros((n, d), jnp.float32), (jnp.arange(cand.shape[0]), row, gate, blk_e))
    return acc


def reference(x, wq, wk, wv, wo, wr, w1, w3, w2, idx):
    xf = x.reshape(T, D)
    a = rmsnorm(xf).astype(jnp.bfloat16)

    def proj(w):
        return jnp.dot(a, w, preferred_element_type=jnp.float32).reshape(NSEQ, SEQ, HEADS, HEAD)

    q = rope(proj(wq)).astype(jnp.bfloat16)
    k = rope(proj(wk)).astype(jnp.bfloat16)
    v = proj(wv).astype(jnp.bfloat16)
    causal = jnp.tril(jnp.ones((SEQ, SEQ), bool))

    def one_seq(qkv):
        qs, ks, vs = qkv
        s = jnp.einsum('qhe,khe->hqk', qs.astype(jnp.float32), ks.astype(jnp.float32)) / math.sqrt(HEAD)
        p = jax.nn.softmax(jnp.where(causal, s, -jnp.inf), axis=-1).astype(jnp.bfloat16)
        return jnp.einsum('hqk,khe->qhe', p.astype(jnp.float32), vs.astype(jnp.float32)).astype(jnp.bfloat16)

    o = lax.map(one_seq, (q, k, v))
    ao = jnp.dot(o.reshape(T, HEADS * HEAD), wo, preferred_element_type=jnp.float32)
    h = (xf.astype(jnp.float32) + ao).astype(jnp.bfloat16)
    ids = idx.reshape(T, TOP)
    r = rmsnorm(h)
    logits = jnp.dot(r, wr, precision=lax.Precision.HIGHEST, preferred_element_type=jnp.float32)
    g = jax.nn.softmax(jnp.take_along_axis(logits, ids, axis=1), axis=-1)
    moe = expert_sum(r.astype(jnp.bfloat16), ids.reshape(-1), g.reshape(-1), TOP, w1, w3, w2, T * TOP)
    return (h.astype(jnp.float32) + moe).astype(jnp.bfloat16).reshape(NSEQ, SEQ, D)
```

```python
import functools
import math
import jax
import jax.numpy as jnp
from jax import lax
from jax.experimental import pallas as pl
from jax.experimental.pallas import tpu as pltpu
from jax.sharding import PartitionSpec as P

HEAD = 128
EPS = 1e-6
THETA = 10000.0
BM = 128
PITCH = BM + 1
LANES = 128


def rmsnorm(v):
    v = v.astype(jnp.float32)
    return v * lax.rsqrt(jnp.mean(v * v, axis=-1, keepdims=True) + EPS)


def rope(z):
    n = z.shape[-3]
    half = HEAD // 2
    freq = THETA ** (-jnp.arange(half, dtype=jnp.float32) / half)
    ang = jnp.arange(n, dtype=jnp.float32)[:, None] * freq
    c = jnp.cos(ang)[:, None, :]
    s = jnp.sin(ang)[:, None, :]
    z1, z2 = z[..., :half], z[..., half:]
    return jnp.concatenate([z1 * c - z2 * s, z2 * c + z1 * s], axis=-1)


def attention(x, s, wq, wk, wv, wo):
    t, d = x.shape
    nh = wq.shape[1] // HEAD
    a = rmsnorm(x).astype(jnp.bfloat16)

    def proj(w):
        return jnp.dot(a, w, preferred_element_type=jnp.float32).reshape(t // s, s, nh, HEAD)

    q = rope(proj(wq)).astype(jnp.bfloat16)
    k = rope(proj(wk)).astype(jnp.bfloat16)
    v = proj(wv).astype(jnp.bfloat16)
    sc = jnp.einsum('bqhe,bkhe->bhqk', q, k, preferred_element_type=jnp.float32) / math.sqrt(HEAD)
    sc = jnp.where(jnp.tril(jnp.ones((s, s), bool)), sc, -jnp.inf)
    p = jax.nn.softmax(sc, axis=-1).astype(jnp.bfloat16)
    o = jnp.einsum('bhqk,bkhe->bqhe', p, v, preferred_element_type=jnp.float32).astype(jnp.bfloat16)
    ao = jnp.dot(o.reshape(t, nh * HEAD), wo, preferred_element_type=jnp.float32)
    return (x.astype(jnp.float32) + ao).astype(jnp.bfloat16)


def router(h, wr, ids):
    r = rmsnorm(h)
    logits = jnp.dot(r, wr, precision=lax.Precision.HIGHEST, preferred_element_type=jnp.float32)
    pick = ids[:, :, None] == jnp.arange(wr.shape[1], dtype=ids.dtype)
    g = jax.nn.softmax(jnp.sum(jnp.where(pick, logits[:, None, :], 0.0), axis=-1), axis=-1)
    return r.astype(jnp.bfloat16), g


def moe_kernel(nt, kk, nblk_ref, be_ref, bb_ref, bn_ref, key_ref, gate_ref, u_hbm, w1_hbm, w3_hbm, w2_hbm,
               out_hbm, ub, acc, w1, w3, w2, xs, zs, lhs, usem, wsem, osem):
    cols = ub.shape[1]
    gmask = nt * kk - 1
    shift = kk.bit_length() - 1
    nexp = w1_hbm.shape[0]
    nblk = nblk_ref[0]

    def weights(e, slot):
        return (pltpu.make_async_copy(w1_hbm.at[e], w1.at[slot], wsem.at[slot, 0]),
                pltpu.make_async_copy(w3_hbm.at[e], w3.at[slot], wsem.at[slot, 1]),
                pltpu.make_async_copy(w2_hbm.at[e], w2.at[slot], wsem.at[slot, 2]))

    load_u = pltpu.make_async_copy(u_hbm, ub.at[pl.ds(0, nt)], usem)
    load_u.start()
    for c in weights(0, 0):
        c.start()

    def zero(i, _):
        acc[pl.ds(i * 8, 8)] = jnp.zeros((8,) + acc.shape[1:], jnp.float32)
        return 0

    lax.fori_loop(0, acc.shape[0] // 8, zero, 0)
    load_u.wait()

    def gather(b):
        base = bb_ref[b]
        for i in range(BM):
            t = lax.shift_right_logical(key_ref[base + i] & gmask, shift)
            xs[pl.ds(i, cols, stride=PITCH), :] = ub[t].astype(jnp.float32)

    def scatter(base, n, rows):
        new = []
        for i in rows:
            gi = key_ref[base + i] & gmask
            t = jnp.where(i < n, lax.shift_right_logical(gi, shift), nt)
            new.append((t, acc[t] + gate_ref[gi] * zs[pl.ds(i, cols, stride=PITCH), :]))
        for t, v in new:
            acc[t] = v

    gather(0)

    def body(b, e_prev):
        e = be_ref[b]
        slot = e % 2

        @pl.when(e != e_prev)
        def _():
            for c in weights(e, slot):
                c.wait()

            @pl.when(e + 1 < nexp)
            def _():
                for c in weights(e + 1, 1 - slot):
                    c.start()

        for k in range(cols):
            lhs[:, k * LANES:(k + 1) * LANES] = xs[k * PITCH:k * PITCH + BM, :].astype(jnp.bfloat16)
        gather(b + 1)
        bp = jnp.maximum(b - 1, 0)
        base, n = bb_ref[bp], jnp.where(b > 0, bn_ref[bp], 0)
        for i in range(0, BM, 8):
            scatter(base, n, range(i, i + 8))
        x = lhs[...]
        a1 = jnp.dot(x, w1[slot], preferred_element_type=jnp.float32)
        a3 = jnp.dot(x, w3[slot], preferred_element_type=jnp.float32)
        act = (jax.nn.silu(a1) * a3).astype(jnp.bfloat16)
        z = jnp.dot(act, w2[slot], preferred_element_type=jnp.float32).astype(jnp.bfloat16).astype(jnp.float32)
        for k in range(cols):
            zs[k * PITCH:k * PITCH + BM, :] = z[:, k * LANES:(k + 1) * LANES]
        return e

    lax.fori_loop(0, nblk, body, -1)
    base, n = bb_ref[nblk - 1], bn_ref[nblk - 1]
    for i in range(0, BM, 8):
        scatter(base, n, range(i, i + 8))

    def pack(i, _):
        for j in range(8):
            t = i * 8 + j
            ub[t] = acc[t].astype(jnp.bfloat16)
        return 0

    lax.fori_loop(0, nt // 8, pack, 0)
    store = pltpu.make_async_copy(ub.at[pl.ds(0, nt)], out_hbm, osem)
    store.start()
    store.wait()


def moe(nblk, be, bb, bn, keys, gates, u, w1, w3, w2):
    nt, cols, _ = u.shape
    kk = gates.shape[0] // nt
    ne, d, f = w1.shape
    smem = pl.BlockSpec(memory_space=pltpu.SMEM)
    hbm = pl.BlockSpec(memory_space=pl.ANY)
    rows = nt * kk
    return pl.pallas_call(
        functools.partial(moe_kernel, nt, kk),
        out_shape=jax.ShapeDtypeStruct((nt, cols, LANES), jnp.bfloat16),
        in_specs=[smem] * 6 + [hbm] * 4,
        out_specs=hbm,
        scratch_shapes=[
            pltpu.VMEM((nt + 8, cols, LANES), jnp.bfloat16),
            pltpu.VMEM((nt + 8, cols, LANES), jnp.float32),
            pltpu.VMEM((2, d, f), jnp.bfloat16),
            pltpu.VMEM((2, d, f), jnp.bfloat16),
            pltpu.VMEM((2, f, d), jnp.bfloat16),
            pltpu.VMEM((cols * PITCH, LANES), jnp.float32),
            pltpu.VMEM((cols * PITCH, LANES), jnp.float32),
            pltpu.VMEM((BM, d), jnp.bfloat16),
            pltpu.SemaphoreType.DMA,
            pltpu.SemaphoreType.DMA((2, 3)),
            pltpu.SemaphoreType.DMA,
        ],
        compiler_params=pltpu.CompilerParams(vmem_limit_bytes=60 * 1024 * 1024),
        cost_estimate=pl.CostEstimate(flops=6 * 5000 * d * f, bytes_accessed=ne * 3 * d * f * 2, transcendentals=0),
    )(nblk, be, bb, bn, keys, gates, u, w1, w3, w2)


def block_plan(ids, me, ne):
    nt, k = ids.shape
    le = ids - me * ne
    local = (le >= 0) & (le < ne)
    flat = jnp.arange(nt * k, dtype=jnp.int32).reshape(nt, k)
    keys = jnp.sort(jnp.where(local, le * (nt * k) + flat, ne * nt * k).reshape(-1))
    experts = jnp.arange(ne, dtype=jnp.int32)
    counts = jnp.sum((le.reshape(-1)[None, :] == experts[:, None]).astype(jnp.int32), axis=1)
    low = (experts[None, :] < experts[:, None])
    first = jnp.sum(jnp.where(low, counts[None, :], 0), axis=1)
    nb = jnp.maximum((counts + BM - 1) // BM, 1)
    bfirst = jnp.sum(jnp.where(low, nb[None, :], 0), axis=1)
    maxb = nt * k // BM + ne + 2
    b = jnp.arange(maxb, dtype=jnp.int32)
    inside = (b[:, None] >= bfirst[None, :]) & (b[:, None] < (bfirst + nb)[None, :])

    def of(v):
        return jnp.sum(jnp.where(inside, v[None, :], 0), axis=1)

    done = (b - of(bfirst)) * BM
    be, bb = of(experts), of(first) + done
    bn = jnp.clip(of(counts) - done, 0, BM)
    bb = jnp.where(jnp.any(inside, axis=1), bb, 0)
    keys = jnp.concatenate([keys, jnp.zeros((BM,), jnp.int32)])
    return jnp.sum(nb).reshape(1), be, bb, bn, keys


def solution(mesh):
    nd = mesh.shape['ep']
    nr = mesh.shape['replica']
    tok = P(('replica', 'ep'), None, None)
    rows_ep = P('ep', None)
    by_expert = P('ep', None, None)
    halves = 2

    def local(x, wq, wk, wv, wo, wr, w1, w3, w2, idx):
        b, s, d = x.shape
        t, k, ne = b * s, idx.shape[-1], w1.shape[0]
        me = lax.axis_index('ep')
        cols = d // LANES
        x = lax.all_to_all(x, 'replica', 0, 0, tiled=True)
        idx = lax.all_to_all(idx, 'replica', 0, 0, tiled=True)
        ids = idx.reshape(t, k)
        th = t // halves
        ids_all = lax.all_gather(ids.T, 'ep', axis=0, tiled=False)
        plans = []
        for c in range(halves):
            ids_c = ids_all[:, :, c * th:(c + 1) * th].transpose(0, 2, 1).reshape(nd * th, k)
            plans.append(block_plan(ids_c, me, ne))

        wq, wk, wv, wo = [lax.all_gather(w, 'ep', axis=0, tiled=True) for w in (wq, wk, wv, wo)]
        h = attention(x.reshape(t, d), s, wq, wk, wv, wo)
        u, g = router(h, wr, ids)
        u = u.reshape(t, cols, LANES)
        h = h.reshape(t, cols, LANES)
        g_all = lax.all_gather(g.reshape(halves, th * k), 'ep', axis=1, tiled=False)
        ys = []
        for c in range(halves):
            u_all = lax.all_gather(u[c * th:(c + 1) * th], 'ep', axis=0, tiled=True)
            part = moe(*plans[c], g_all[c].reshape(-1), u_all, w1, w3, w2)
            back = lax.all_to_all(part.reshape(nd, th, cols, LANES), 'ep', 0, 0, tiled=True)
            total = h[c * th:(c + 1) * th].astype(jnp.float32) + jnp.sum(back.astype(jnp.float32), axis=0)
            ys.append(total.astype(jnp.bfloat16))
        y = jnp.concatenate(ys, axis=0).reshape(b, s, d)
        return lax.all_to_all(y, 'replica', 0, 0, tiled=True)

    return jax.shard_map(local, mesh=mesh,
                         in_specs=(tok, rows_ep, rows_ep, rows_ep, rows_ep, P(None, None),
                                   by_expert, by_expert, by_expert, tok),
                         out_specs=tok, check_vma=False)
```

```python
import functools
import math
import jax
import jax.numpy as jnp
from jax import lax
from jax.experimental import pallas as pl
from jax.experimental.pallas import tpu as pltpu
from jax.sharding import PartitionSpec as P

HEAD = 128
EPS = 1e-6
THETA = 10000.0
BM = 128
PITCH = BM + 1
LANES = 128


def rmsnorm(v):
    v = v.astype(jnp.float32)
    return v * lax.rsqrt(jnp.mean(v * v, axis=-1, keepdims=True) + EPS)


STEPS = 8
MESH_ID = pl.DeviceIdType.MESH


def attn_kernel(seq, x_ref, cos_ref, sin_ref, wq_ref, wk_ref, wv_ref, wo_ref, h_ref, gw, go,
                a_ref, acc, wbuf, obuf, zr, xr, yr, dr, pr, zp, zm, xs, xd, ys, yd, ps, lsem):
    r, e = lax.axis_index('replica'), lax.axis_index('ep')
    nz, nq = 4, 4
    z, c = e // 2, e % 2
    me_p = e + 1 - 2 * c
    r_y = r + 1 - 2 * (r % 2)
    r_x = (r + 2) % 4
    r_d = (r_y + 2) % 4
    rows, wide = wq_ref.shape[0], wq_ref.shape[1] // STEPS
    quarter = rows // nq
    orows = go.shape[0] // STEPS
    oquarter = orows // nq
    tokens, d = x_ref.shape

    barrier = pltpu.get_barrier_semaphore()

    def greet(dev):
        pl.semaphore_signal(barrier, inc=1, device_id=dev, device_id_type=MESH_ID)

    greet((r_x, e))
    greet((r_y, e))
    greet((r, me_p))

    @pl.when(z > 0)
    def _():
        greet((r, e - 2))

    @pl.when(z < nz - 1)
    def _():
        greet((r, e + 2))

    pl.semaphore_wait(barrier, 3 + (z + 2) // 3 + (nz + 1 - z) // 3)

    def piece(s, src_e, q):
        return gw.at[s, :, pl.ds(src_e * rows + q * quarter, quarter), :]

    def opiece(s, q):
        return go.at[pl.ds(s * orows + q * oquarter, oquarter), :]

    def rcopy(src, dst, ssem, rsem, dev):
        return pltpu.make_async_remote_copy(src_ref=src, dst_ref=dst, send_sem=ssem, recv_sem=rsem,
                                            device_id=dev, device_id_type=MESH_ID)

    def z_send(w, s, zs, up):
        dev = (r, e + 2) if up else (r, e - 2)
        sem = (zp if up else zm).at[w, s, zs]
        ref = opiece(s, r) if w else piece(s, 2 * zs + c, r)
        return rcopy(ref, ref, sem, zr.at[w, s, zs], dev)

    def x_send(w, s, zs):
        ref = opiece(s, r) if w else piece(s, 2 * zs + c, r)
        return rcopy(ref, ref, xs.at[w, s, zs], xr.at[w, s, zs], (r_x, e))

    def y_send(w, s, zs):
        ref = opiece(s, r) if w else piece(s, 2 * zs + c, r)
        return rcopy(ref, ref, ys.at[w, s, zs], yr.at[w, s, zs], (r_y, e))

    def xd_send(w, s, zs):
        ref = opiece(s, r_y) if w else piece(s, 2 * zs + c, r_y)
        return rcopy(ref, ref, xd.at[w, s, zs], dr.at[w, s, zs], (r_x, e))

    def yd_send(w, s, zs):
        ref = opiece(s, r_x) if w else piece(s, 2 * zs + c, r_x)
        return rcopy(ref, ref, yd.at[w, s, zs], dr.at[w, s, zs], (r_y, e))

    def x_recv(w, s, zs):
        ref = opiece(s, r_x) if w else piece(s, 2 * zs + c, r_x)
        return rcopy(ref, ref, xs.at[w, s, zs], xr.at[w, s, zs], (r_x, e))

    def y_recv(w, s, zs):
        ref = opiece(s, r_y) if w else piece(s, 2 * zs + c, r_y)
        return rcopy(ref, ref, ys.at[w, s, zs], yr.at[w, s, zs], (r_y, e))

    def p_send(w, s, zs, j):
        q = (r, r_x, r_y, r_d)[j]
        ref = opiece(s, q) if w else piece(s, 2 * zs + c, q)
        return rcopy(ref, ref, ps.at[w, s, zs, j], pr.at[w, s, zs, j], (r, me_p))

    def p_recv(w, s, zs, j):
        q = (r, r_x, r_y, r_d)[j]
        ref = opiece(s, q) if w else piece(s, 2 * zs + 1 - c, q)
        return rcopy(ref, ref, ps.at[w, s, zs, j], pr.at[w, s, zs, j], (r, me_p))

    def own_parts(s):
        col = pl.ds(s * wide, wide)
        return [(wq_ref, 0, col), (wk_ref, 1, col), (wv_ref, 2, col)]

    def originate(s):
        lo = pl.ds(r * quarter, quarter)

        def line(up):
            dev = (r, e + 2) if up else (r, e - 2)
            sem = (zp if up else zm)
            for w_ref, m, col in own_parts(s):
                rcopy(w_ref.at[lo, col], gw.at[s, m, pl.ds(e * rows + r * quarter, quarter), :],
                      sem.at[0, s, z], zr.at[0, s, z], dev).start()

            @pl.when(s == e)
            def _():
                rcopy(wo_ref.at[pl.ds(r * oquarter, oquarter), :], opiece(s, r), sem.at[1, s, z], zr.at[1, s, z],
                      dev).start()

        @pl.when(z > 0)
        def _():
            line(False)

        @pl.when(z < nz - 1)
        def _():
            line(True)

        for w_ref, m, col in own_parts(s):
            rcopy(w_ref.at[:, col], gw.at[s, m, pl.ds(e * rows, rows), :], ps.at[0, s, z, 0], pr.at[0, s, z, 0],
                  (r, me_p)).start()

        @pl.when(s == e)
        def _():
            rcopy(wo_ref, go.at[pl.ds(s * orows, orows), :], ps.at[1, s, z, 0], pr.at[1, s, z, 0], (r, me_p)).start()

    def for_both(s, zs, fn):
        fn(0)

        @pl.when(s == 2 * zs + c)
        def _():
            fn(1)

    def x_first(s, zs):
        return (s + zs + s // 2) % 2 == 0

    def each_side(k, fn):
        @pl.when(z - k - 1 >= 0)
        def _():
            fn(z - k - 1, True)

        @pl.when(z + k + 1 < nz)
        def _():
            fn(z + k + 1, False)

    def along_z(s, k):
        def side(zs, up):
            def one(w):
                z_send(w, s, zs, up).wait_recv()
                if up:
                    @pl.when(z < nz - 1)
                    def _():
                        z_send(w, s, zs, True).start()
                else:
                    @pl.when(z > 0)
                    def _():
                        z_send(w, s, zs, False).start()
                x_send(w, s, zs).start()
                y_send(w, s, zs).start()
                p_send(w, s, zs, 0).start()

            for_both(s, zs, one)

        each_side(k, side)

    def across(s, k):
        def side(zs, up):
            def one(w):
                x_recv(w, s, zs).wait_recv()

                @pl.when(x_first(s, zs))
                def _():
                    yd_send(w, s, zs).start()

                p_send(w, s, zs, 1).start()
                y_recv(w, s, zs).wait_recv()

                @pl.when(jnp.logical_not(x_first(s, zs)))
                def _():
                    xd_send(w, s, zs).start()

                p_send(w, s, zs, 2).start()

            for_both(s, zs, one)

        each_side(k, side)

    def diagonal(s, k):
        def side(zs, up):
            def one(w):
                ref = opiece(s, r_d) if w else piece(s, 2 * zs + c, r_d)
                rcopy(ref, ref, xd.at[w, s, zs], dr.at[w, s, zs], (r_x, e)).wait_recv()
                p_send(w, s, zs, 3).start()

            for_both(s, zs, one)

        each_side(k, side)

    def load(s, slot, f):
        return pltpu.make_async_copy(gw.at[s, :, pl.ds(f * rows, rows), :], wbuf.at[slot, :, pl.ds(f * rows, rows), :],
                                     lsem.at[slot, f])

    def oload(s, slot, own):
        src = wo_ref if own else go.at[pl.ds(s * orows, orows), :]
        return pltpu.make_async_copy(src, obuf.at[slot], lsem.at[slot, 2 * nz])

    def collect(s):
        slot = s % 2

        def side(zs, up):
            def one(w):
                for j in range(4):
                    p_recv(w, s, zs, j).wait_recv()

            one(0)

            @pl.when(s == 2 * zs + 1 - c)
            def _():
                one(1)

        for k in range(nz - 1):
            each_side(k, side)
        full = gw.at[s, :, pl.ds(me_p * rows, rows), :]
        rcopy(full, full, ps.at[0, s, z, 0], pr.at[0, s, z, 0], (r, me_p)).wait_recv()

        @pl.when(s == me_p)
        def _():
            ofull = go.at[pl.ds(s * orows, orows), :]
            rcopy(ofull, ofull, ps.at[1, s, z, 0], pr.at[1, s, z, 0], (r, me_p)).wait_recv()

        for f in range(2 * nz):
            @pl.when(f == e)
            def _():
                for w_ref, m, col in own_parts(s):
                    pltpu.make_async_copy(w_ref.at[:, col], wbuf.at[slot, m, pl.ds(f * rows, rows), :],
                                          lsem.at[slot, f]).start()

            @pl.when(f != e)
            def _():
                load(s, slot, f).start()

        @pl.when(s == e)
        def _():
            oload(s, slot, True).start()

        @pl.when(s != e)
        def _():
            oload(s, slot, False).start()

    def wait_loads(s):
        slot = s % 2
        for f in range(2 * nz):
            load(s, slot, f).wait()
        oload(s, slot, False).wait()

    pair = 2 * HEAD
    npair = wide // pair

    def compute(s, j):
        slot = s % 2
        a = a_ref[...]
        cols = slice(j * pair, (j + 1) * pair)
        cos, sin = cos_ref[...], sin_ref[...]

        def rot(v):
            return (v * cos + pltpu.roll(v, HEAD // 2, 1) * sin).astype(jnp.bfloat16)

        q = jnp.dot(a, wbuf[slot, 0, :, cols], preferred_element_type=jnp.float32)
        k = jnp.dot(a, wbuf[slot, 1, :, cols], preferred_element_type=jnp.float32)
        v = jnp.dot(a, wbuf[slot, 2, :, cols], preferred_element_type=jnp.float32).astype(jnp.bfloat16)
        tri = lax.broadcasted_iota(jnp.int32, (seq, seq), 0) >= lax.broadcasted_iota(jnp.int32, (seq, seq), 1)
        heads = []
        for hh in range(2):
            hc = slice(hh * HEAD, (hh + 1) * HEAD)
            qh, kh, vh = rot(q[:, hc]), rot(k[:, hc]), v[:, hc]
            outs = []
            for b in range(tokens // seq):
                rs = slice(b * seq, (b + 1) * seq)
                sc = lax.dot_general(qh[rs], kh[rs], (((1,), (1,)), ((), ())), preferred_element_type=jnp.float32)
                sc = jnp.where(tri, sc * (1.0 / math.sqrt(HEAD)), -jnp.inf)
                ex = jnp.exp(sc - jnp.max(sc, axis=-1, keepdims=True))
                p = (ex / jnp.sum(ex, axis=-1, keepdims=True)).astype(jnp.bfloat16)
                outs.append(jnp.dot(p, vh[rs], preferred_element_type=jnp.float32).astype(jnp.bfloat16))
            heads.append(jnp.concatenate(outs, axis=0))
        o = jnp.concatenate(heads, axis=1)
        acc[...] += jnp.dot(o, obuf[slot, j * pair:(j + 1) * pair, :], preferred_element_type=jnp.float32)

    originate(0)
    x = x_ref[...].astype(jnp.float32)
    a_ref[...] = (x * lax.rsqrt(jnp.mean(x * x, axis=-1, keepdims=True) + EPS)).astype(jnp.bfloat16)
    acc[...] = x

    def within(s, fn):
        @pl.when((s >= 0) & (s < STEPS))
        def _():
            fn()

    def turn(i, _):
        within(i + 1, lambda: originate(i + 1))
        within(i - 3, lambda: wait_loads(i - 3))
        for k in range(nz - 1):
            within(i, lambda: along_z(i, k))
            within(i - 1, lambda: across(i - 1, k))
            within(i - 2, lambda: diagonal(i - 2, k))
            if k < npair:
                within(i - 3, lambda: compute(i - 3, k))
        within(i - 2, lambda: collect(i - 2))
        return 0

    lax.fori_loop(0, STEPS + 3, turn, 0)
    h_ref[...] = acc[...].astype(jnp.bfloat16)

    def drain(s, _):
        def sent(w, zs, up):
            if up:
                @pl.when(z < nz - 1)
                def _():
                    z_send(w, s, zs, True).wait_send()
            else:
                @pl.when(z > 0)
                def _():
                    z_send(w, s, zs, False).wait_send()
            x_send(w, s, zs).wait_send()
            y_send(w, s, zs).wait_send()

            @pl.when(x_first(s, zs))
            def _():
                yd_send(w, s, zs).wait_send()

            @pl.when(jnp.logical_not(x_first(s, zs)))
            def _():
                xd_send(w, s, zs).wait_send()

            for j in range(4):
                p_send(w, s, zs, j).wait_send()

        for k in range(nz - 1):
            each_side(k, lambda zs, up: for_both(s, zs, lambda w: sent(w, zs, up)))

        def own(w):
            @pl.when(z > 0)
            def _():
                z_send(w, s, z, False).wait_send()

            @pl.when(z < nz - 1)
            def _():
                z_send(w, s, z, True).wait_send()

            full = go.at[pl.ds(s * orows, orows), :] if w else gw.at[s, :, pl.ds(e * rows, rows), :]
            rcopy(full, full, ps.at[w, s, z, 0], pr.at[w, s, z, 0], (r, me_p)).wait_send()

        for_both(s, z, own)
        return 0

    lax.fori_loop(0, STEPS, drain, 0)


def attention(x, seq, wq, wk, wv, wo):
    t, d = x.shape
    rows, hd = wq.shape
    nd = d // rows
    n = seq
    half = HEAD // 2
    freq = THETA ** (-jnp.arange(half, dtype=jnp.float32) / half)
    ang = jnp.arange(n, dtype=jnp.float32)[:, None] * freq
    c, s = jnp.cos(ang), jnp.sin(ang)
    cos = jnp.tile(jnp.concatenate([c, c], axis=1), (t // n, 1))
    sin = jnp.tile(jnp.concatenate([-s, s], axis=1), (t // n, 1))
    vmem = pl.BlockSpec(memory_space=pltpu.VMEM)
    hbm = pl.BlockSpec(memory_space=pl.ANY)
    wide = hd // STEPS
    orows = hd // STEPS
    dma = pltpu.SemaphoreType.DMA
    h, _, _ = pl.pallas_call(
        functools.partial(attn_kernel, seq),
        out_shape=(jax.ShapeDtypeStruct((t, d), jnp.bfloat16),
                   jax.ShapeDtypeStruct((STEPS, 3, d, wide), jnp.bfloat16),
                   jax.ShapeDtypeStruct((hd, d), jnp.bfloat16)),
        in_specs=[vmem] * 3 + [hbm] * 4,
        out_specs=(vmem, hbm, hbm),
        scratch_shapes=[
            pltpu.VMEM((t, d), jnp.bfloat16),
            pltpu.VMEM((t, d), jnp.float32),
            pltpu.VMEM((2, 3, d, wide), jnp.bfloat16),
            pltpu.VMEM((2, orows, d), jnp.bfloat16),
            dma((2, STEPS, 4)), dma((2, STEPS, 4)), dma((2, STEPS, 4)), dma((2, STEPS, 4)), dma((2, STEPS, 4, 4)),
            dma((2, STEPS, 4)), dma((2, STEPS, 4)), dma((2, STEPS, 4)), dma((2, STEPS, 4)), dma((2, STEPS, 4)),
            dma((2, STEPS, 4)), dma((2, STEPS, 4, 4)),
            dma((2, nd + 1)),
        ],
        compiler_params=pltpu.CompilerParams(collective_id=0, has_side_effects=True, vmem_limit_bytes=58 * 1024 * 1024),
        cost_estimate=pl.CostEstimate(flops=10 * t * d * hd, bytes_accessed=4 * d * hd * 2, transcendentals=0),
    )(x, cos, sin, wq, wk, wv, wo)
    return h


def router(h, wr, ids):
    r = rmsnorm(h)
    logits = jnp.dot(r, wr, precision=lax.Precision.HIGHEST, preferred_element_type=jnp.float32)
    pick = ids[:, :, None] == jnp.arange(wr.shape[1], dtype=ids.dtype)
    g = jax.nn.softmax(jnp.sum(jnp.where(pick, logits[:, None, :], 0.0), axis=-1), axis=-1)
    return r.astype(jnp.bfloat16), g


def moe_kernel(nt, kk, nblk_ref, be_ref, bb_ref, bn_ref, key_ref, gate_ref, u_hbm, w1_hbm, w3_hbm, w2_hbm,
               out_hbm, ub, acc, w1, w3, w2, xs, zs, lhs, usem, wsem, osem):
    cols = ub.shape[1]
    gmask = nt * kk - 1
    shift = kk.bit_length() - 1
    nexp = w1_hbm.shape[0]
    nblk = nblk_ref[0]

    def weights(e, slot):
        return (pltpu.make_async_copy(w1_hbm.at[e], w1.at[slot], wsem.at[slot, 0]),
                pltpu.make_async_copy(w3_hbm.at[e], w3.at[slot], wsem.at[slot, 1]),
                pltpu.make_async_copy(w2_hbm.at[e], w2.at[slot], wsem.at[slot, 2]))

    load_u = pltpu.make_async_copy(u_hbm, ub.at[pl.ds(0, nt)], usem)
    load_u.start()
    for c in weights(0, 0):
        c.start()

    def zero(i, _):
        acc[pl.ds(i * 8, 8)] = jnp.zeros((8,) + acc.shape[1:], jnp.float32)
        return 0

    lax.fori_loop(0, acc.shape[0] // 8, zero, 0)
    load_u.wait()

    def gather(b):
        base = bb_ref[b]
        for i in range(BM):
            t = lax.shift_right_logical(key_ref[base + i] & gmask, shift)
            xs[pl.ds(i, cols, stride=PITCH), :] = ub[t].astype(jnp.float32)

    def scatter(base, n, rows):
        new = []
        for i in rows:
            gi = key_ref[base + i] & gmask
            t = jnp.where(i < n, lax.shift_right_logical(gi, shift), nt)
            new.append((t, acc[t] + gate_ref[gi] * zs[pl.ds(i, cols, stride=PITCH), :]))
        for t, v in new:
            acc[t] = v

    gather(0)

    def body(b, e_prev):
        e = be_ref[b]
        slot = e % 2

        @pl.when(e != e_prev)
        def _():
            for c in weights(e, slot):
                c.wait()

            @pl.when(e + 1 < nexp)
            def _():
                for c in weights(e + 1, 1 - slot):
                    c.start()

        for k in range(cols):
            lhs[:, k * LANES:(k + 1) * LANES] = xs[k * PITCH:k * PITCH + BM, :].astype(jnp.bfloat16)
        gather(b + 1)
        bp = jnp.maximum(b - 1, 0)
        base, n = bb_ref[bp], jnp.where(b > 0, bn_ref[bp], 0)
        for i in range(0, BM, 8):
            scatter(base, n, range(i, i + 8))
        x = lhs[...]
        a1 = jnp.dot(x, w1[slot], preferred_element_type=jnp.float32)
        a3 = jnp.dot(x, w3[slot], preferred_element_type=jnp.float32)
        act = (jax.nn.silu(a1) * a3).astype(jnp.bfloat16)
        z = jnp.dot(act, w2[slot], preferred_element_type=jnp.float32).astype(jnp.bfloat16).astype(jnp.float32)
        for k in range(cols):
            zs[k * PITCH:k * PITCH + BM, :] = z[:, k * LANES:(k + 1) * LANES]
        return e

    lax.fori_loop(0, nblk, body, -1)
    base, n = bb_ref[nblk - 1], bn_ref[nblk - 1]
    for i in range(0, BM, 8):
        scatter(base, n, range(i, i + 8))

    def pack(i, _):
        for j in range(8):
            t = i * 8 + j
            ub[t] = acc[t].astype(jnp.bfloat16)
        return 0

    lax.fori_loop(0, nt // 8, pack, 0)
    store = pltpu.make_async_copy(ub.at[pl.ds(0, nt)], out_hbm, osem)
    store.start()
    store.wait()


def moe(nblk, be, bb, bn, keys, gates, u, w1, w3, w2):
    nt, cols, _ = u.shape
    kk = gates.shape[0] // nt
    ne, d, f = w1.shape
    smem = pl.BlockSpec(memory_space=pltpu.SMEM)
    hbm = pl.BlockSpec(memory_space=pl.ANY)
    rows = nt * kk
    return pl.pallas_call(
        functools.partial(moe_kernel, nt, kk),
        out_shape=jax.ShapeDtypeStruct((nt, cols, LANES), jnp.bfloat16),
        in_specs=[smem] * 6 + [hbm] * 4,
        out_specs=hbm,
        scratch_shapes=[
            pltpu.VMEM((nt + 8, cols, LANES), jnp.bfloat16),
            pltpu.VMEM((nt + 8, cols, LANES), jnp.float32),
            pltpu.VMEM((2, d, f), jnp.bfloat16),
            pltpu.VMEM((2, d, f), jnp.bfloat16),
            pltpu.VMEM((2, f, d), jnp.bfloat16),
            pltpu.VMEM((cols * PITCH, LANES), jnp.float32),
            pltpu.VMEM((cols * PITCH, LANES), jnp.float32),
            pltpu.VMEM((BM, d), jnp.bfloat16),
            pltpu.SemaphoreType.DMA,
            pltpu.SemaphoreType.DMA((2, 3)),
            pltpu.SemaphoreType.DMA,
        ],
        compiler_params=pltpu.CompilerParams(vmem_limit_bytes=60 * 1024 * 1024),
        cost_estimate=pl.CostEstimate(flops=6 * 5000 * d * f, bytes_accessed=ne * 3 * d * f * 2, transcendentals=0),
    )(nblk, be, bb, bn, keys, gates, u, w1, w3, w2)


def block_plan(ids, me, ne):
    nt, k = ids.shape
    le = ids - me * ne
    local = (le >= 0) & (le < ne)
    flat = jnp.arange(nt * k, dtype=jnp.int32).reshape(nt, k)
    keys = jnp.sort(jnp.where(local, le * (nt * k) + flat, ne * nt * k).reshape(-1))
    experts = jnp.arange(ne, dtype=jnp.int32)
    counts = jnp.sum((le.reshape(-1)[None, :] == experts[:, None]).astype(jnp.int32), axis=1)
    low = (experts[None, :] < experts[:, None])
    first = jnp.sum(jnp.where(low, counts[None, :], 0), axis=1)
    nb = jnp.maximum((counts + BM - 1) // BM, 1)
    bfirst = jnp.sum(jnp.where(low, nb[None, :], 0), axis=1)
    maxb = nt * k // BM + ne + 2
    b = jnp.arange(maxb, dtype=jnp.int32)
    inside = (b[:, None] >= bfirst[None, :]) & (b[:, None] < (bfirst + nb)[None, :])

    def of(v):
        return jnp.sum(jnp.where(inside, v[None, :], 0), axis=1)

    done = (b - of(bfirst)) * BM
    be, bb = of(experts), of(first) + done
    bn = jnp.clip(of(counts) - done, 0, BM)
    bb = jnp.where(jnp.any(inside, axis=1), bb, 0)
    keys = jnp.concatenate([keys, jnp.zeros((BM,), jnp.int32)])
    return jnp.sum(nb).reshape(1), be, bb, bn, keys


def solution(mesh):
    nd = mesh.shape['ep']
    nr = mesh.shape['replica']
    tok = P(('replica', 'ep'), None, None)
    rows_ep = P('ep', None)
    by_expert = P('ep', None, None)
    halves = 2

    def local(x, wq, wk, wv, wo, wr, w1, w3, w2, idx):
        b, s, d = x.shape
        t, k, ne = b * s, idx.shape[-1], w1.shape[0]
        me = lax.axis_index('ep')
        cols = d // LANES
        x = lax.all_to_all(x, 'replica', 0, 0, tiled=True)
        idx = lax.all_to_all(idx, 'replica', 0, 0, tiled=True)
        ids = idx.reshape(t, k)
        th = t // halves
        ids_all = lax.all_gather(ids.T, 'ep', axis=0, tiled=False)
        plans = []
        for c in range(halves):
            ids_c = ids_all[:, :, c * th:(c + 1) * th].transpose(0, 2, 1).reshape(nd * th, k)
            plans.append(block_plan(ids_c, me, ne))

        h = attention(x.reshape(t, d), s, wq, wk, wv, wo)
        u, g = router(h, wr, ids)
        u = u.reshape(t, cols, LANES)
        h = h.reshape(t, cols, LANES)
        g_all = lax.all_gather(g.reshape(halves, th * k), 'ep', axis=1, tiled=False)
        ys = []
        for c in range(halves):
            u_all = lax.all_gather(u[c * th:(c + 1) * th], 'ep', axis=0, tiled=True)
            part = moe(*plans[c], g_all[c].reshape(-1), u_all, w1, w3, w2)
            back = lax.all_to_all(part.reshape(nd, th, cols, LANES), 'ep', 0, 0, tiled=True)
            total = h[c * th:(c + 1) * th].astype(jnp.float32) + jnp.sum(back.astype(jnp.float32), axis=0)
            ys.append(total.astype(jnp.bfloat16))
        y = jnp.concatenate(ys, axis=0).reshape(b, s, d)
        return lax.all_to_all(y, 'replica', 0, 0, tiled=True)

    return jax.shard_map(local, mesh=mesh,
                         in_specs=(tok, rows_ep, rows_ep, rows_ep, rows_ep, P(None, None),
                                   by_expert, by_expert, by_expert, tok),
                         out_specs=tok, check_vma=False)
```

```python
import functools
import math
import jax
import jax.numpy as jnp
from jax import lax
from jax.experimental import pallas as pl
from jax.experimental.pallas import tpu as pltpu
from jax.sharding import PartitionSpec as P

HEAD = 128
EPS = 1e-6
THETA = 10000.0
BM = 128
PITCH = BM + 1
LANES = 128


def loop(n, fn):
    def step(i, carry):
        fn(i)
        return carry

    lax.fori_loop(0, n, step, 0)


def ep_at(z, c):
    return 2 * z + c


def rmsnorm(v):
    v = v.astype(jnp.float32)
    return v * lax.rsqrt(jnp.mean(v * v, axis=-1, keepdims=True) + EPS)


CUT = 48
STEPS = 8
MESH_ID = pl.DeviceIdType.MESH


def attn_kernel(seq, x_ref, cos_ref, sin_ref, wq_ref, wk_ref, wv_ref, wo_ref, h_ref, gw, go,
                a_ref, acc, wbuf, obuf, zr, xr, yr, zp, zm, xs, xd, ys, yd, dr, pr, ps, lsem):
    r, e = lax.axis_index('replica'), lax.axis_index('ep')
    nz, nq = 4, 4
    z, c = e // 2, e % 2
    me_p = e + 1 - 2 * c
    r_y = r + 1 - 2 * (r % 2)
    r_x = (r + 2) % 4
    r_d = (r_y + 2) % 4
    rows, wide = wq_ref.shape[0], wq_ref.shape[1] // STEPS
    quarter = rows // nq
    orows = go.shape[0] // STEPS
    oquarter = orows // nq
    tokens, _ = x_ref.shape

    barrier = pltpu.get_barrier_semaphore()

    def greet(dev):
        pl.semaphore_signal(barrier, inc=1, device_id=dev, device_id_type=MESH_ID)

    greet((r_x, e))
    greet((r_y, e))
    greet((r, me_p))

    @pl.when(z > 0)
    def _():
        greet((r, e - 2))

    @pl.when(z < nz - 1)
    def _():
        greet((r, e + 2))

    pl.semaphore_wait(barrier, 3 + (z + 2) // 3 + (nz + 1 - z) // 3)

    per = STEPS // (2 * nz)

    def own_wo(s, lo, n):
        return wo_ref.at[pl.ds((s % per) * orows + lo, n), :]

    def piece(s, src_e, q):
        return gw.at[s, :, pl.ds(src_e * rows + q * quarter, quarter), :]

    def opiece(s, q):
        return go.at[pl.ds(s * orows + q * oquarter, oquarter), :]

    def rcopy(src, dst, ssem, rsem, dev):
        return pltpu.make_async_remote_copy(src_ref=src, dst_ref=dst, send_sem=ssem, recv_sem=rsem,
                                            device_id=dev, device_id_type=MESH_ID)

    def z_send(w, s, zs, up):
        dev = (r, e + 2) if up else (r, e - 2)
        sem = (zp if up else zm).at[w, s, zs]
        ref = opiece(s, r) if w else piece(s, ep_at(zs, c), r)
        return rcopy(ref, ref, sem, zr.at[w, s, zs], dev)

    def x_send(w, s, zs):
        ref = opiece(s, r) if w else piece(s, ep_at(zs, c), r)
        return rcopy(ref, ref, xs.at[w, s, zs], xr.at[w, s, zs], (r_x, e))

    def y_send(w, s, zs):
        ref = opiece(s, r) if w else piece(s, ep_at(zs, c), r)
        return rcopy(ref, ref, ys.at[w, s, zs], yr.at[w, s, zs], (r_y, e))

    def half(w, s, zs, q, i):
        if w:
            return go.at[pl.ds(s * orows + q * oquarter + i * (oquarter // 2), oquarter // 2), :]
        return gw.at[s, :, pl.ds((ep_at(zs, c)) * rows + q * quarter + i * (quarter // 2), quarter // 2), :]

    def xd_send(w, s, zs):
        ref = half(w, s, zs, r_y, 1)
        return rcopy(ref, ref, xd.at[w, s, zs], dr.at[1, w, s, zs], (r_x, e))

    def yd_send(w, s, zs):
        ref = half(w, s, zs, r_x, 0)
        return rcopy(ref, ref, yd.at[w, s, zs], dr.at[0, w, s, zs], (r_y, e))

    def d_recv(w, s, zs, i):
        ref = half(w, s, zs, r_d, i)
        return rcopy(ref, ref, xd.at[w, s, zs], dr.at[i, w, s, zs], (r_x, e))

    def x_recv(w, s, zs):
        ref = opiece(s, r_x) if w else piece(s, ep_at(zs, c), r_x)
        return rcopy(ref, ref, xs.at[w, s, zs], xr.at[w, s, zs], (r_x, e))

    def y_recv(w, s, zs):
        ref = opiece(s, r_y) if w else piece(s, ep_at(zs, c), r_y)
        return rcopy(ref, ref, ys.at[w, s, zs], yr.at[w, s, zs], (r_y, e))

    def p_send(w, s, zs, j):
        q = (r, r_x, r_y, r_d)[j]
        ref = opiece(s, q) if w else piece(s, ep_at(zs, c), q)
        return rcopy(ref, ref, ps.at[w, s, zs, j], pr.at[w, s, zs, j], (r, me_p))

    def p_recv(w, s, zs, j):
        q = (r, r_x, r_y, r_d)[j]
        ref = opiece(s, q) if w else piece(s, ep_at(zs, 1 - c), q)
        return rcopy(ref, ref, ps.at[w, s, zs, j], pr.at[w, s, zs, j], (r, me_p))

    def own_parts(s):
        col = pl.ds(s * wide, wide)
        return [(wq_ref, 0, col), (wk_ref, 1, col), (wv_ref, 2, col)]

    def originate(s):
        lo = pl.ds(r * quarter, quarter)

        def line(up):
            dev = (r, e + 2) if up else (r, e - 2)
            sem = (zp if up else zm)
            for w_ref, m, col in own_parts(s):
                rcopy(w_ref.at[lo, col], gw.at[s, m, pl.ds(e * rows + r * quarter, quarter), :],
                      sem.at[0, s, z], zr.at[0, s, z], dev).start()

            @pl.when(s // per == e)
            def _():
                rcopy(own_wo(s, r * oquarter, oquarter), opiece(s, r), sem.at[1, s, z], zr.at[1, s, z],
                      dev).start()

        @pl.when(z > 0)
        def _():
            line(False)

        @pl.when(z < nz - 1)
        def _():
            line(True)

        for w_ref, m, col in own_parts(s):
            rcopy(w_ref.at[:, col], gw.at[s, m, pl.ds(e * rows, rows), :], ps.at[0, s, z, 0], pr.at[0, s, z, 0],
                  (r, me_p)).start()

        @pl.when(s // per == e)
        def _():
            rcopy(own_wo(s, 0, orows), go.at[pl.ds(s * orows, orows), :], ps.at[1, s, z, 0], pr.at[1, s, z, 0], (r, me_p)).start()

    def for_both(s, zs, fn):
        fn(0)

        @pl.when(s // per == ep_at(zs, c))
        def _():
            fn(1)

    def each_side(k, fn):
        @pl.when(z - k - 1 >= 0)
        def _():
            fn(z - k - 1, True)

        @pl.when(z + k + 1 < nz)
        def _():
            fn(z + k + 1, False)

    def along_z(s, k):
        def side(zs, up):
            def one(w):
                z_send(w, s, zs, up).wait_recv()
                if up:
                    @pl.when(z < nz - 1)
                    def _():
                        z_send(w, s, zs, True).start()
                else:
                    @pl.when(z > 0)
                    def _():
                        z_send(w, s, zs, False).start()
                x_send(w, s, zs).start()
                y_send(w, s, zs).start()
                p_send(w, s, zs, 0).start()

            for_both(s, zs, one)

        each_side(k, side)

    def across(s, k):
        def side(zs, up):
            def one(w):
                x_recv(w, s, zs).wait_recv()
                yd_send(w, s, zs).start()
                p_send(w, s, zs, 1).start()
                y_recv(w, s, zs).wait_recv()
                xd_send(w, s, zs).start()
                p_send(w, s, zs, 2).start()

            for_both(s, zs, one)

        each_side(k, side)

    def diagonal(s, k):
        def side(zs, up):
            def one(w):
                d_recv(w, s, zs, 0).wait_recv()
                d_recv(w, s, zs, 1).wait_recv()
                p_send(w, s, zs, 3).start()

            for_both(s, zs, one)

        each_side(k, side)

    def load(s, slot, f):
        return pltpu.make_async_copy(gw.at[s, :, pl.ds(f * rows, rows), :], wbuf.at[slot, :, pl.ds(f * rows, rows), :],
                                     lsem.at[slot, f])

    def oload(s, slot, own):
        src = own_wo(s, 0, orows) if own else go.at[pl.ds(s * orows, orows), :]
        return pltpu.make_async_copy(src, obuf.at[slot], lsem.at[slot, 2 * nz])

    def collect(s):
        slot = s % 2

        def side(zs, up):
            def one(w):
                for j in range(4):
                    p_recv(w, s, zs, j).wait_recv()

            one(0)

            @pl.when(s // per == ep_at(zs, 1 - c))
            def _():
                one(1)

        for k in range(nz - 1):
            each_side(k, side)
        full = gw.at[s, :, pl.ds(me_p * rows, rows), :]
        rcopy(full, full, ps.at[0, s, z, 0], pr.at[0, s, z, 0], (r, me_p)).wait_recv()

        @pl.when(s // per == me_p)
        def _():
            ofull = go.at[pl.ds(s * orows, orows), :]
            rcopy(ofull, ofull, ps.at[1, s, z, 0], pr.at[1, s, z, 0], (r, me_p)).wait_recv()

        for f in range(2 * nz):
            @pl.when(f == e)
            def _():
                for w_ref, m, col in own_parts(s):
                    pltpu.make_async_copy(w_ref.at[:, col], wbuf.at[slot, m, pl.ds(f * rows, rows), :],
                                          lsem.at[slot, f]).start()

            @pl.when(f != e)
            def _():
                load(s, slot, f).start()

        @pl.when(s // per == e)
        def _():
            oload(s, slot, True).start()

        @pl.when(s // per != e)
        def _():
            oload(s, slot, False).start()

    def wait_loads(s):
        slot = s % 2
        for f in range(2 * nz):
            load(s, slot, f).wait()
        oload(s, slot, False).wait()

    pair = 2 * HEAD
    npair = wide // pair

    def compute(s, j):
        slot = s % 2
        a = a_ref[...]
        cols = slice(j * pair, (j + 1) * pair)
        cos, sin = cos_ref[...], sin_ref[...]

        def rot(v):
            return (v * cos + pltpu.roll(v, HEAD // 2, 1) * sin).astype(jnp.bfloat16)

        q = jnp.dot(a, wbuf[slot, 0, :, cols], preferred_element_type=jnp.float32)
        k = jnp.dot(a, wbuf[slot, 1, :, cols], preferred_element_type=jnp.float32)
        v = jnp.dot(a, wbuf[slot, 2, :, cols], preferred_element_type=jnp.float32).astype(jnp.bfloat16)
        tri = lax.broadcasted_iota(jnp.int32, (seq, seq), 0) >= lax.broadcasted_iota(jnp.int32, (seq, seq), 1)
        heads = []
        for hh in range(2):
            hc = slice(hh * HEAD, (hh + 1) * HEAD)
            qh, kh, vh = rot(q[:, hc]), rot(k[:, hc]), v[:, hc]
            outs = []
            for b in range(tokens // seq):
                rs = slice(b * seq, (b + 1) * seq)
                sc = lax.dot_general(qh[rs], kh[rs], (((1,), (1,)), ((), ())), preferred_element_type=jnp.float32)
                sc = jnp.where(tri, sc * (1.0 / math.sqrt(HEAD)), -jnp.inf)
                ex = jnp.exp(sc - jnp.max(sc, axis=-1, keepdims=True))
                p = (ex / jnp.sum(ex, axis=-1, keepdims=True)).astype(jnp.bfloat16)
                outs.append(jnp.dot(p, vh[rs], preferred_element_type=jnp.float32).astype(jnp.bfloat16))
            heads.append(jnp.concatenate(outs, axis=0))
        o = jnp.concatenate(heads, axis=1)
        acc[...] += jnp.dot(o, obuf[slot, j * pair:(j + 1) * pair, :], preferred_element_type=jnp.float32)

    originate(0)
    x = x_ref[...].astype(jnp.float32)
    a_ref[...] = (x * lax.rsqrt(jnp.mean(x * x, axis=-1, keepdims=True) + EPS)).astype(jnp.bfloat16)
    acc[...] = x

    def within(s, fn):
        @pl.when((s >= 0) & (s < STEPS))
        def _():
            fn()

    def turn(i):
        within(i + 1, lambda: originate(i + 1))
        within(i - 3, lambda: wait_loads(i - 3))
        for k in range(nz - 1):
            within(i, lambda: along_z(i, k))
            within(i - 1, lambda: across(i - 1, k))
            within(i - 2, lambda: diagonal(i - 2, k))
            if k < npair:
                within(i - 3, lambda: compute(i - 3, k))
        within(i - 2, lambda: collect(i - 2))

    loop(STEPS + 3, turn)
    h_ref[...] = acc[...].astype(jnp.bfloat16)

    def drain(s):
        def sent(w, zs, up):
            if up:
                @pl.when(z < nz - 1)
                def _():
                    z_send(w, s, zs, True).wait_send()
            else:
                @pl.when(z > 0)
                def _():
                    z_send(w, s, zs, False).wait_send()
            x_send(w, s, zs).wait_send()
            y_send(w, s, zs).wait_send()
            yd_send(w, s, zs).wait_send()
            xd_send(w, s, zs).wait_send()

            for j in range(4):
                p_send(w, s, zs, j).wait_send()

        for k in range(nz - 1):
            each_side(k, lambda zs, up: for_both(s, zs, lambda w: sent(w, zs, up)))

        def own(w):
            @pl.when(z > 0)
            def _():
                z_send(w, s, z, False).wait_send()

            @pl.when(z < nz - 1)
            def _():
                z_send(w, s, z, True).wait_send()

            full = go.at[pl.ds(s * orows, orows), :] if w else gw.at[s, :, pl.ds(e * rows, rows), :]
            rcopy(full, full, ps.at[w, s, z, 0], pr.at[w, s, z, 0], (r, me_p)).wait_send()

        for_both(s, z, own)

    loop(STEPS, drain)


def attention(x, seq, wq, wk, wv, wo):
    t, d = x.shape
    rows, hd = wq.shape
    nd = d // rows
    n = seq
    half = HEAD // 2
    freq = THETA ** (-jnp.arange(half, dtype=jnp.float32) / half)
    ang = jnp.arange(n, dtype=jnp.float32)[:, None] * freq
    c, s = jnp.cos(ang), jnp.sin(ang)
    cos = jnp.tile(jnp.concatenate([c, c], axis=1), (t // n, 1))
    sin = jnp.tile(jnp.concatenate([-s, s], axis=1), (t // n, 1))
    vmem = pl.BlockSpec(memory_space=pltpu.VMEM)
    hbm = pl.BlockSpec(memory_space=pl.ANY)
    wide = hd // STEPS
    orows = hd // STEPS
    dma = pltpu.SemaphoreType.DMA
    h, _, _ = pl.pallas_call(
        functools.partial(attn_kernel, seq),
        out_shape=(jax.ShapeDtypeStruct((t, d), jnp.bfloat16),
                   jax.ShapeDtypeStruct((STEPS, 3, d, wide), jnp.bfloat16),
                   jax.ShapeDtypeStruct((hd, d), jnp.bfloat16)),
        in_specs=[vmem] * 3 + [hbm] * 4,
        out_specs=(vmem, hbm, hbm),
        scratch_shapes=[
            pltpu.VMEM((t, d), jnp.bfloat16),
            pltpu.VMEM((t, d), jnp.float32),
            pltpu.VMEM((2, 3, d, wide), jnp.bfloat16),
            pltpu.VMEM((2, orows, d), jnp.bfloat16),
            *([dma((2, STEPS, 4))] * 9), dma((2, 2, STEPS, 4)), dma((2, STEPS, 4, 4)), dma((2, STEPS, 4, 4)),
            dma((2, nd + 1)),
        ],
        compiler_params=pltpu.CompilerParams(collective_id=0, has_side_effects=True, vmem_limit_bytes=58 * 1024 * 1024),
        cost_estimate=pl.CostEstimate(flops=10 * t * d * hd, bytes_accessed=4 * d * hd * 2, transcendentals=0),
    )(x, cos, sin, wq, wk, wv, wo)
    return h


def router(h, wr, ids):
    r = rmsnorm(h)
    logits = jnp.dot(r, wr, precision=lax.Precision.HIGHEST, preferred_element_type=jnp.float32)
    pick = ids[:, :, None] == jnp.arange(wr.shape[1], dtype=ids.dtype)
    g = jax.nn.softmax(jnp.sum(jnp.where(pick, logits[:, None, :], 0.0), axis=-1), axis=-1)
    return r.astype(jnp.bfloat16), g


def span(n):
    return 1 << (n - 1).bit_length()


def moe_kernel(nt, kk, nblk_ref, be_ref, bb_ref, bn_ref, key_ref, gate_ref, u_hbm, w1_hbm, w3_hbm, w2_hbm,
               out_hbm, ub, acc, w1, w3, w2, xs, zs, lhs, usem, wsem, osem):
    cols = ub.shape[1]
    gmask = span(nt * kk) - 1
    shift = kk.bit_length() - 1
    nexp = w1_hbm.shape[0]
    nblk = nblk_ref[0]

    def weights(e, slot):
        return (pltpu.make_async_copy(w1_hbm.at[e], w1.at[slot], wsem.at[slot, 0]),
                pltpu.make_async_copy(w3_hbm.at[e], w3.at[slot], wsem.at[slot, 1]),
                pltpu.make_async_copy(w2_hbm.at[e], w2.at[slot], wsem.at[slot, 2]))

    nd = u_hbm.shape[0]
    n = nt // nd
    for dev in range(nd):
        pltpu.make_async_copy(u_hbm.at[dev, pl.ds(0, n)], ub.at[pl.ds(dev * n, n)], usem).start()

    for c in weights(0, 0):
        c.start()

    def zero(i):
        acc[pl.ds(i * 8, 8)] = jnp.zeros((8,) + acc.shape[1:], jnp.float32)

    loop(acc.shape[0] // 8, zero)
    pltpu.make_async_copy(ub.at[pl.ds(0, nt)], ub.at[pl.ds(0, nt)], usem).wait()

    def gather(b):
        base = bb_ref[b]
        for i in range(BM):
            t = lax.shift_right_logical(key_ref[base + i] & gmask, shift)
            xs[pl.ds(i, cols, stride=PITCH), :] = ub[t].astype(jnp.float32)

    def scatter(base, n, rows):
        new = []
        for i in rows:
            gi = key_ref[base + i] & gmask
            t = jnp.where(i < n, lax.shift_right_logical(gi, shift), nt)
            new.append((t, acc[t] + gate_ref[gi] * zs[pl.ds(i, cols, stride=PITCH), :]))
        for t, v in new:
            acc[t] = v

    gather(0)

    def body(b, e_prev):
        e = be_ref[b]
        slot = e % 2

        @pl.when(e != e_prev)
        def _():
            @pl.when(e + 1 < nexp)
            def _():
                for c in weights(e + 1, 1 - slot):
                    c.start()

            for c in weights(e, slot):
                c.wait()

        for k in range(cols):
            lhs[:, k * LANES:(k + 1) * LANES] = xs[k * PITCH:k * PITCH + BM, :].astype(jnp.bfloat16)
        gather(b + 1)
        bp = jnp.maximum(b - 1, 0)
        base, n = bb_ref[bp], jnp.where(b > 0, bn_ref[bp], 0)
        for i in range(0, BM, 8):
            scatter(base, n, range(i, i + 8))
        x = lhs[...]
        a1 = jnp.dot(x, w1[slot], preferred_element_type=jnp.float32)
        a3 = jnp.dot(x, w3[slot], preferred_element_type=jnp.float32)
        act = (jax.nn.silu(a1) * a3).astype(jnp.bfloat16)
        z = jnp.dot(act, w2[slot], preferred_element_type=jnp.float32).astype(jnp.bfloat16).astype(jnp.float32)
        for k in range(cols):
            zs[k * PITCH:k * PITCH + BM, :] = z[:, k * LANES:(k + 1) * LANES]
        return e

    lax.fori_loop(0, nblk, body, -1)
    base, n = bb_ref[nblk - 1], bn_ref[nblk - 1]
    for i in range(0, BM, 8):
        scatter(base, n, range(i, i + 8))

    def pack(i):
        for j in range(8):
            t = i * 8 + j
            ub[t] = acc[t].astype(jnp.bfloat16)

    loop(nt // 8, pack)
    store = pltpu.make_async_copy(ub.at[pl.ds(0, nt)], out_hbm, osem)
    store.start()
    store.wait()


def moe(nblk, be, bb, bn, keys, gates, u, n, w1, w3, w2):
    nd, _, cols, _ = u.shape
    nt = nd * n
    kk = gates.shape[0] // nt
    ne, d, f = w1.shape
    smem = pl.BlockSpec(memory_space=pltpu.SMEM)
    hbm = pl.BlockSpec(memory_space=pl.ANY)
    return pl.pallas_call(
        functools.partial(moe_kernel, nt, kk),
        out_shape=jax.ShapeDtypeStruct((nt, cols, LANES), jnp.bfloat16),
        in_specs=[smem] * 6 + [hbm] * 4,
        out_specs=hbm,
        scratch_shapes=[
            pltpu.VMEM((nt + 8, cols, LANES), jnp.bfloat16),
            pltpu.VMEM((nt + 8, cols, LANES), jnp.float32),
            pltpu.VMEM((2, d, f), jnp.bfloat16),
            pltpu.VMEM((2, d, f), jnp.bfloat16),
            pltpu.VMEM((2, f, d), jnp.bfloat16),
            pltpu.VMEM((cols * PITCH, LANES), jnp.float32),
            pltpu.VMEM((cols * PITCH, LANES), jnp.float32),
            pltpu.VMEM((BM, d), jnp.bfloat16),
            pltpu.SemaphoreType.DMA,
            pltpu.SemaphoreType.DMA((2, 3)),
            pltpu.SemaphoreType.DMA,
        ],
        compiler_params=pltpu.CompilerParams(vmem_limit_bytes=60 * 1024 * 1024),
        cost_estimate=pl.CostEstimate(flops=6 * 5000 * d * f, bytes_accessed=ne * 3 * d * f * 2, transcendentals=0),
    )(nblk, be, bb, bn, keys, gates, u, w1, w3, w2)


def back_kernel(cut, piece, part, h_ref, ya, y_out, own, prt, raw, fin, fout, yst, raw_s, raw_r, prt_s, prt_r, f_s, f_r,
                y_s, y_r, osem, lsem):
    r, e = lax.axis_index('replica'), lax.axis_index('ep')
    z, c = e // 2, e % 2
    me_p = e + 1 - 2 * c
    n = h_ref.shape[0]
    np_ = n // piece
    split = n // 4 // piece
    mid = (z + 2) // 3 + (5 - z) // 3 - 1
    is_mid, is_end = mid == 1, mid == 0
    low = z // 2
    z_mid = 1 + low
    z_end = 3 * low
    z_oth = 2 - low
    h_a, h_b, h_c = 3 - 3 * low, 2 - low, 3 * low
    replicas = [(r + i) % 4 for i in range(1, 4)]

    def rows(p):
        return pl.ds(p * piece, piece)

    def rcopy(src, dst, ssem, rsem, dev):
        return pltpu.make_async_remote_copy(src_ref=src, dst_ref=dst, send_sem=ssem, recv_sem=rsem, device_id=dev,
                                            device_id_type=MESH_ID)

    barrier = pltpu.get_barrier_semaphore()

    def greet(dev):
        pl.semaphore_signal(barrier, inc=1, device_id=dev, device_id_type=MESH_ID)

    for q in replicas:
        greet((q, e))
    greet((r, me_p))

    @pl.when(is_end)
    def _():
        greet((r, ep_at(z_mid, 0)))
        greet((r, ep_at(z_mid, 1)))

    @pl.when(is_mid)
    def _():
        greet((r, ep_at(z_end, 0)))
        greet((r, ep_at(z_end, 1)))
        greet((r, ep_at(z_oth, c)))

    pl.semaphore_wait(barrier, 6 + mid)

    def raw_send(i, c2, p):
        dest = (3 - i) + low * (2 * i - 3)
        return rcopy(part.at[ep_at(dest, c2), rows(p)], raw.at[i, c, rows(p)], raw_s.at[i, c2, p], raw_r.at[i, c, p],
                     (r, ep_at(z_mid, c2)))

    def raw_recv(i, src, p):
        return rcopy(raw.at[i, src, rows(p)], raw.at[i, src, rows(p)], raw_s.at[i, src, p], raw_r.at[i, src, p],
                     (r, ep_at(z_end, src)))

    def prt_copy(hh, p):
        return rcopy(part.at[ep_at(hh, 1 - c), rows(p)], prt.at[hh, rows(p)], prt_s.at[hh, p], prt_r.at[hh, p], (r, me_p))

    def f_copy(i, slot, p, dev):
        return rcopy(fout.at[i, rows(p)], fin.at[slot, rows(p)], f_s.at[i, p], f_r.at[slot, p], dev)

    def loadown(hh):
        return pltpu.make_async_copy(part.at[ep_at(hh, c)], own.at[hh], osem.at[hh])

    def place(half):
        return pl.ds(0, cut) if half < 0 else pl.ds(cut + half * piece, piece)

    def y_copy(src, blk, half):
        return rcopy(src, y_out.at[r, place(half)], y_s.at[blk, half + 1], y_r.at[r, half + 1], (blk, e))

    def y_local(src, half):
        return pltpu.make_async_copy(src, y_out.at[r, place(half)], lsem.at[half + 1])

    def put(src, blk, half):
        @pl.when(r == blk)
        def _():
            y_local(src, half).start()

        @pl.when(r != blk)
        def _():
            y_copy(src, blk, half).start()

    @pl.when(is_end)
    def _():
        loadown(z).start()
        for i in range(3):
            def send(p):
                for c2 in range(2):
                    raw_send(i, c2, p).start()

            loop(np_, send)

        def pass_on(p):
            prt_copy(z, p).start()

        loop(np_, pass_on)

    @pl.when(is_mid)
    def _():
        for hh in (h_a, h_b, h_c, z):
            loadown(hh).start()
        for hh in (h_a, h_b, h_c, z):
            def pass_on(p):
                prt_copy(hh, p).start()

            loop(np_, pass_on)

    for blk in range(4):
        put(ya.at[blk], blk, -1)

    def groups(p, fn):
        def g(j):
            fn(pl.ds(p * piece + j * 8, 8))

        loop(piece // 8, g)

    def f32(v):
        return v.astype(jnp.float32)

    def both(hh, s):
        return f32(own[hh, s]) + f32(prt[hh, s])

    def onward(i, hh, p, dev_slot, incoming):
        prt_copy(hh, p).wait_recv()

        def fn(s):
            fout[i, s] = both(hh, s) + incoming(s)

        groups(p, fn)
        f_copy(i, dev_slot[1], p, dev_slot[0]).start()

    def finish(p, incoming):
        prt_copy(z, p).wait_recv()

        def fn(s):
            yst[s] = (f32(h_ref[s]) + both(z, s) + incoming(s)).astype(jnp.bfloat16)

        groups(p, fn)

        for blk in range(4):
            for half in range(split):
                @pl.when(p == blk * split + half)
                def _():
                    put(yst.at[rows(p)], blk, half)

    @pl.when(is_mid)
    def _():
        loadown(h_a).wait()

        def far(p):
            raw_recv(0, 0, p).wait_recv()
            raw_recv(0, 1, p).wait_recv()
            onward(0, h_a, p, ((r, ep_at(z_oth, c)), 0), lambda s: f32(raw[0, 0, s]) + f32(raw[0, 1, s]))

        loop(np_, far)
        loadown(h_b).wait()
        loadown(h_c).wait()

        def near(p):
            f_copy(2, 0, p, (r, ep_at(z_oth, c))).wait_recv()
            onward(2, h_c, p, ((r, ep_at(z_end, c)), 0), lambda s: fin[0, s])
            raw_recv(1, 0, p).wait_recv()
            raw_recv(1, 1, p).wait_recv()
            onward(1, h_b, p, ((r, ep_at(z_oth, c)), 1), lambda s: f32(raw[1, 0, s]) + f32(raw[1, 1, s]))

        loop(np_, near)
        loadown(z).wait()

        def last(p):
            f_copy(1, 1, p, (r, ep_at(z_oth, c))).wait_recv()
            raw_recv(2, 0, p).wait_recv()
            raw_recv(2, 1, p).wait_recv()
            finish(p, lambda s: fin[1, s] + f32(raw[2, 0, s]) + f32(raw[2, 1, s]))

        loop(np_, last)

    @pl.when(is_end)
    def _():
        loadown(z).wait()

        def last(p):
            f_copy(2, 0, p, (r, ep_at(z_mid, c))).wait_recv()
            finish(p, lambda s: fin[0, s])

        loop(np_, last)

    @pl.when(is_end)
    def _():
        def sent(p):
            for i in range(3):
                for c2 in range(2):
                    raw_send(i, c2, p).wait_send()
            prt_copy(z, p).wait_send()

        loop(np_, sent)

    @pl.when(is_mid)
    def _():
        def sent(p):
            for hh in (h_a, h_b, h_c, z):
                prt_copy(hh, p).wait_send()
            f_copy(0, 0, p, (r, ep_at(z_oth, c))).wait_send()
            f_copy(1, 1, p, (r, ep_at(z_oth, c))).wait_send()
            f_copy(2, 0, p, (r, ep_at(z_end, c))).wait_send()

        loop(np_, sent)

    for blk in range(4):
        for half in range(-1, split):
            some = ya.at[blk] if half < 0 else yst.at[rows(0)]

            @pl.when(r == blk)
            def _():
                y_local(some, half).wait()

            @pl.when(r != blk)
            def _():
                y_copy(some, blk, half).wait_send()
                ref = y_out.at[blk, place(half)]
                rcopy(ref, ref, y_s.at[blk, half + 1], y_r.at[blk, half + 1], (blk, e)).wait_recv()


def back(part, h, ya):
    _, n, cols, _ = part.shape
    cut = ya.shape[1]
    seq = cut + n // 4
    piece = n // 8
    vmem = pl.BlockSpec(memory_space=pltpu.VMEM)
    hbm = pl.BlockSpec(memory_space=pl.ANY)
    dma = pltpu.SemaphoreType.DMA
    np_ = n // piece

    def tiles(lead, dtype):
        return pltpu.VMEM(lead + (cols, LANES), dtype)

    return pl.pallas_call(
        functools.partial(back_kernel, cut, piece),
        out_shape=jax.ShapeDtypeStruct((4, seq, cols, LANES), jnp.bfloat16),
        in_specs=[hbm, vmem, hbm],
        out_specs=hbm,
        scratch_shapes=[
            tiles((4, n), jnp.bfloat16), tiles((4, n), jnp.bfloat16), tiles((3, 2, n), jnp.bfloat16),
            tiles((2, n), jnp.float32), tiles((3, n), jnp.float32), tiles((n,), jnp.bfloat16),
            dma((3, 2, np_)), dma((3, 2, np_)), dma((4, np_)), dma((4, np_)), dma((3, np_)), dma((2, np_)),
            dma((4, 3)), dma((4, 3)), dma((4,)), dma((3,)),
        ],
        compiler_params=pltpu.CompilerParams(collective_id=1, has_side_effects=True, vmem_limit_bytes=58 * 1024 * 1024),
    )(part, h, ya)


def block_plan(ids, me, ne):
    nt, k = ids.shape
    le = ids - me * ne
    local = (le >= 0) & (le < ne)
    flat = jnp.arange(nt * k, dtype=jnp.int32).reshape(nt, k)
    keys = lax.sort(jnp.where(local, le * span(nt * k) + flat, ne * span(nt * k)).reshape(-1), is_stable=False)
    experts = jnp.arange(ne, dtype=jnp.int32)
    counts = jnp.sum((le.reshape(-1)[None, :] == experts[:, None]).astype(jnp.int32), axis=1)
    low = (experts[None, :] < experts[:, None])
    first = jnp.sum(jnp.where(low, counts[None, :], 0), axis=1)
    nb = jnp.maximum((counts + BM - 1) // BM, 1)
    bfirst = jnp.sum(jnp.where(low, nb[None, :], 0), axis=1)
    maxb = nt * k // BM + ne + 2
    b = jnp.arange(maxb, dtype=jnp.int32)
    inside = (b[:, None] >= bfirst[None, :]) & (b[:, None] < (bfirst + nb)[None, :])

    def of(v):
        return jnp.sum(jnp.where(inside, v[None, :], 0), axis=1)

    done = (b - of(bfirst)) * BM
    be, bb = of(experts), of(first) + done
    bn = jnp.clip(of(counts) - done, 0, BM)
    bb = jnp.where(jnp.any(inside, axis=1), bb, 0)
    keys = jnp.concatenate([keys, jnp.zeros((BM,), jnp.int32)])
    return jnp.sum(nb).reshape(1), be, bb, bn, keys


def solution(mesh):
    nd = mesh.shape['ep']
    tok = P(('replica', 'ep'), None, None)
    rows_ep = P('ep', None)
    by_expert = P('ep', None, None)
    cut = CUT

    def local(x, wq, wk, wv, wo, wr, w1, w3, w2, idx):
        b, s, d = x.shape
        t, k, ne = b * s, idx.shape[-1], w1.shape[0]
        me = lax.axis_index('ep')
        cols = d // LANES
        x = lax.all_to_all(x, 'replica', 0, 0, tiled=True)
        idx = lax.all_to_all(idx, 'replica', 0, 0, tiled=True)
        ids = idx.reshape(t, k)
        ids_all = lax.all_gather(ids.T, 'ep', axis=0, tiled=False)
        x, ids_all = lax.optimization_barrier((x, ids_all))
        h = attention(x.reshape(t, d), s, wq, wk, wv, wo)
        u, g = router(h, wr, ids)
        u = u.reshape(b, s, cols, LANES)
        h = h.reshape(b, s, cols, LANES)
        g_parts = []
        for _ in range(3):
            g_parts.append(lax.reduce_precision(g, 8, 7))
            g = g - g_parts[-1]
        gp = jnp.stack(g_parts).astype(jnp.bfloat16).reshape(3, b, s, k)

        def gathered(lo, hi):
            n = b * (hi - lo)
            gc = gp[:, :, lo:hi].reshape(3 * n * k // LANES, LANES)
            gc = jnp.pad(gc, ((0, -gc.shape[0] % cols), (0, 0))).reshape(-1, cols, LANES)
            both = lax.all_gather(jnp.concatenate([u[:, lo:hi].reshape(n, cols, LANES), gc]), 'ep', axis=0, tiled=False)
            gall = both[:, n:].reshape(nd, -1)[:, :3 * n * k].reshape(nd, 3, n * k).astype(jnp.float32)
            return both, gall[:, 0] + gall[:, 1] + gall[:, 2]

        def experts(lo, hi):
            n = b * (hi - lo)
            ids_c = ids_all.reshape(nd, k, b, s)[..., lo:hi].transpose(0, 2, 3, 1).reshape(nd * n, k)
            plan = block_plan(ids_c, me, ne)
            u_all, gates = gathered(lo, hi)
            return moe(*plan, gates.reshape(-1), u_all, n, w1, w3, w2).reshape(nd, n, cols, LANES)

        part_a = experts(0, cut)
        part_a = lax.all_to_all(part_a, 'ep', 0, 0, tiled=True)
        part_b = experts(cut, s)
        ya = h[:, :cut].astype(jnp.float32) + jnp.sum(part_a.astype(jnp.float32), axis=0).reshape(b, cut, cols, LANES)
        y = back(part_b, h[:, cut:].reshape(-1, cols, LANES), ya.astype(jnp.bfloat16))
        return y.reshape(b, s, d)

    return jax.shard_map(local, mesh=mesh,
                         in_specs=(tok, rows_ep, rows_ep, rows_ep, rows_ep, P(None, None),
                                   by_expert, by_expert, by_expert, tok),
                         out_specs=tok, check_vma=False)
```

```python
import functools
import jax
import jax.numpy as jnp
from jax import lax
from jax.experimental import pallas as pl
from jax.experimental.pallas import tpu as pltpu
from jax.sharding import PartitionSpec as P

HEAD = 128
EPS = 1e-6
THETA = 10000.0
BM = 128
PITCH = BM + 1
LANES = 128
CUT = 48
STEPS = 8
SLOT_BITS, TOKEN_BITS = 15, 12


def loop(n, fn):
    def step(i, carry):
        fn(i)
        return carry

    lax.fori_loop(0, n, step, 0)


def ep_at(z, c):
    return 2 * z + c


MESH_ID = pl.DeviceIdType.MESH


def rcopy(src, dst, ssem, rsem, dev):
    return pltpu.make_async_remote_copy(src_ref=src, dst_ref=dst, send_sem=ssem, recv_sem=rsem, device_id=dev,
                                        device_id_type=MESH_ID)


def meet(peers, count):
    barrier = pltpu.get_barrier_semaphore()
    for guard, dev in peers:
        def greet():
            pl.semaphore_signal(barrier, device_id=dev, device_id_type=MESH_ID)

        if guard is None:
            greet()
        else:
            pl.when(guard)(greet)
    pl.semaphore_wait(barrier, count)


def attn_kernel(cut, x_hbm, idt_hbm, cos_ref, sin_ref, wr_ref, wq_ref, wk_ref, wv_ref, wo_ref,
                ua_ref, ub_ref, ha_ref, hb_ref, ids_out, gw, go,
                xg, a_ref, acc, wbuf, obuf, tm, gates, idv, zr, zp, zm, xr, yr, xs, ys, xd, yd, dr, pr, ps,
                x_s, x_r, i_s, i_r, j_s, j_r, lsem, csem):
    r, e = lax.axis_index('replica'), lax.axis_index('ep')
    nz, nq = 4, 4
    z, c = e // 2, e % 2
    e_p = ep_at(z, 1 - c)
    r_x, r_y = (r + 2) % nq, r + 1 - 2 * (r % 2)
    r_d = (r_y + 2) % nq
    nd = ids_out.shape[0]
    rows, wide = wq_ref.shape[0], wq_ref.shape[1] // STEPS
    quarter = rows // nq
    orows = go.shape[0] // STEPS
    nseq, seq, d = x_hbm.shape
    partner, x_dev, y_dev = (r, e_p), (r_x, e), (r_y, e)
    per = STEPS // nd

    def mod(v, m):
        return lax.rem(v, m)

    others = [mod(r + i, nq) for i in range(1, nq)]
    mates = [mod(e + i, nd) for i in range(1, nd)]
    meet([(None, (q, e)) for q in others] + [(None, (r, f)) for f in mates], len(others) + len(mates))

    for i, q in enumerate(others):
        rcopy(idt_hbm.at[q], ids_out.at[e, r], i_s.at[i], i_r.at[r], (q, e)).start()
        rcopy(x_hbm.at[q], xg.at[r], x_s.at[i], x_r.at[r], (q, e)).start()
    keep_ids = pltpu.make_async_copy(idt_hbm.at[r], ids_out.at[e, r], csem.at[0])
    keep_x = pltpu.make_async_copy(x_hbm.at[r], xg.at[r], csem.at[1])
    keep_ids.start()
    keep_x.start()

    def spread_ids():
        keep_ids.wait()
        for i, q in enumerate(others):
            rcopy(idt_hbm.at[q], ids_out.at[e, q], i_s.at[i], i_r.at[q], (q, e)).wait_recv()
        for i, f in enumerate(mates):
            rcopy(ids_out.at[e], ids_out.at[e], j_s.at[i], j_r.at[e], (r, f)).start()

    def prepare():
        keep_x.wait()
        for i, q in enumerate(others):
            rcopy(x_hbm.at[q], xg.at[q], x_s.at[i], x_r.at[q], (q, e)).wait_recv()

        def norm(b):
            x = xg[b].astype(jnp.float32)
            at = pl.ds(b * seq, seq)
            a_ref[at, :] = (x * lax.rsqrt(jnp.mean(x * x, axis=-1, keepdims=True) + EPS)).astype(jnp.bfloat16)
            acc[at, :] = x

        loop(nseq, norm)

    def piece(w, s, f, q):
        if w:
            return go.at[pl.ds(s * orows + q * (orows // nq), orows // nq), :]
        return gw.at[s, :, pl.ds(f * rows + q * quarter, quarter), :]

    def half(w, s, zs, q, i):
        if w:
            n = orows // nq // 2
            return go.at[pl.ds(s * orows + (2 * q + i) * n, n), :]
        n = quarter // 2
        return gw.at[s, :, pl.ds(ep_at(zs, c) * rows + (2 * q + i) * n, n), :]

    def own_wo(s, lo, n):
        return wo_ref.at[pl.ds(mod(s, per) * orows + lo, n), :]

    def z_send(w, s, zs, up):
        ref = piece(w, s, ep_at(zs, c), r)
        return rcopy(ref, ref, (zp if up else zm).at[w, s, zs], zr.at[w, s, zs], (r, e + 2) if up else (r, e - 2))

    def xy_send(w, s, zs, q, ssem, rsem, dev):
        ref = piece(w, s, ep_at(zs, c), q)
        return rcopy(ref, ref, ssem.at[w, s, zs], rsem.at[w, s, zs], dev)

    def xd_send(w, s, zs, q):
        ref = half(w, s, zs, q, 1)
        return rcopy(ref, ref, xd.at[w, s, zs], dr.at[1, w, s, zs], x_dev)

    def yd_send(w, s, zs, q):
        ref = half(w, s, zs, q, 0)
        return rcopy(ref, ref, yd.at[w, s, zs], dr.at[0, w, s, zs], y_dev)

    def p_copy(w, s, zs, j, core):
        ref = piece(w, s, ep_at(zs, core), (r, r_x, r_y, r_d)[j])
        return rcopy(ref, ref, ps.at[w, s, zs, j], pr.at[w, s, zs, j], partner)

    def p_whole(w, s, f):
        ref = go.at[pl.ds(s * orows, orows), :] if w else gw.at[s, :, pl.ds(f * rows, rows), :]
        return rcopy(ref, ref, ps.at[w, s, z, 0], pr.at[w, s, z, 0], partner)

    def own_parts(s):
        return [(w.at[:, pl.ds(s * wide, wide)], m) for m, w in enumerate((wq_ref, wk_ref, wv_ref))]

    def if_wo(s, f, *fns):
        @pl.when(s // per == f)
        def _():
            for fn in fns:
                fn()

    def each_line(fn):
        pl.when(z > 0)(lambda: fn(False))
        pl.when(z < nz - 1)(lambda: fn(True))

    def each_side(k, fn):
        pl.when(z - k - 1 >= 0)(lambda: fn(z - k - 1, True))
        pl.when(z + k + 1 < nz)(lambda: fn(z + k + 1, False))

    def originate(s):
        def line(up):
            sem = zp if up else zm
            dev = (r, e + 2) if up else (r, e - 2)
            for w, m in own_parts(s):
                rcopy(w.at[pl.ds(r * quarter, quarter), :], gw.at[s, m, pl.ds(e * rows + r * quarter, quarter), :],
                      sem.at[0, s, z], zr.at[0, s, z], dev).start()
            if_wo(s, e, lambda: rcopy(own_wo(s, r * (orows // nq), orows // nq), piece(1, s, e, r), sem.at[1, s, z],
                                      zr.at[1, s, z], dev).start())

        each_line(line)
        for w, m in own_parts(s):
            rcopy(w, gw.at[s, m, pl.ds(e * rows, rows), :], ps.at[0, s, z, 0], pr.at[0, s, z, 0], partner).start()
        if_wo(s, e, lambda: rcopy(own_wo(s, 0, orows), go.at[pl.ds(s * orows, orows), :], ps.at[1, s, z, 0],
                                  pr.at[1, s, z, 0], partner).start())

    def for_both(s, f, fn):
        fn(0)
        if_wo(s, f, lambda: fn(1))

    def along_z(s, k):
        def side(zs, up):
            def one(w):
                z_send(w, s, zs, up).wait_recv()
                pl.when(z < nz - 1 if up else z > 0)(lambda: z_send(w, s, zs, up).start())
                xy_send(w, s, zs, r, xs, xr, x_dev).start()
                xy_send(w, s, zs, r, ys, yr, y_dev).start()
                p_copy(w, s, zs, 0, c).start()

            for_both(s, ep_at(zs, c), one)

        each_side(k, side)

    def across(s, k):
        def side(zs, up):
            def one(w):
                xy_send(w, s, zs, r_x, xs, xr, x_dev).wait_recv()
                yd_send(w, s, zs, r_x).start()
                p_copy(w, s, zs, 1, c).start()
                xy_send(w, s, zs, r_y, ys, yr, y_dev).wait_recv()
                xd_send(w, s, zs, r_y).start()
                p_copy(w, s, zs, 2, c).start()

            for_both(s, ep_at(zs, c), one)

        each_side(k, side)

    def diagonal(s, k):
        def side(zs, up):
            def one(w):
                xd_send(w, s, zs, r_d).wait_recv()
                yd_send(w, s, zs, r_d).wait_recv()
                p_copy(w, s, zs, 3, c).start()

            for_both(s, ep_at(zs, c), one)

        each_side(k, side)

    def load(s, f):
        slot = mod(s, 2)
        return pltpu.make_async_copy(gw.at[s, :, pl.ds(f * rows, rows), :], wbuf.at[slot, :, pl.ds(f * rows, rows), :],
                                     lsem.at[slot, f])

    def oload(s, src):
        slot = mod(s, 2)
        return pltpu.make_async_copy(src, obuf.at[slot], lsem.at[slot, nd])

    def collect(s):
        slot = mod(s, 2)
        whole = go.at[pl.ds(s * orows, orows), :]

        def side(zs, up):
            def one(w):
                for j in range(nq):
                    p_copy(w, s, zs, j, 1 - c).wait_recv()

            for_both(s, ep_at(zs, 1 - c), one)

        for k in range(nz - 1):
            each_side(k, side)
        p_whole(0, s, e_p).wait_recv()
        if_wo(s, e_p, lambda: p_whole(1, s, e_p).wait_recv())

        for f in range(nd):
            def near():
                for w, m in own_parts(s):
                    pltpu.make_async_copy(w, wbuf.at[slot, m, pl.ds(f * rows, rows), :], lsem.at[slot, f]).start()

            pl.when(f == e)(near)
            pl.when(f != e)(lambda: load(s, f).start())
        if_wo(s, e, lambda: oload(s, own_wo(s, 0, orows)).start())
        pl.when(s // per != e)(lambda: oload(s, whole).start())

    def wait_loads(s):
        for f in range(nd):
            load(s, f).wait()
        oload(s, go.at[pl.ds(s * orows, orows), :]).wait()

    pair = 2 * HEAD
    npair = wide // pair

    def compute(s, j):
        slot = mod(s, 2)
        a = a_ref[...]
        cols = slice(j * pair, (j + 1) * pair)
        cos, sin = cos_ref[...], sin_ref[...]

        def rot(v):
            return (v * cos + pltpu.roll(v, HEAD // 2, 1) * sin).astype(jnp.bfloat16)

        q, k, v = [jnp.dot(a, wbuf[slot, m, :, cols], preferred_element_type=jnp.float32) for m in range(3)]
        v = v.astype(jnp.bfloat16)
        tri = lax.broadcasted_iota(jnp.int32, (seq, seq), 0) >= lax.broadcasted_iota(jnp.int32, (seq, seq), 1)
        heads = []
        for hh in range(2):
            hc = slice(hh * HEAD, (hh + 1) * HEAD)
            outs = []
            for b in range(nseq):
                rs = slice(b * seq, (b + 1) * seq)
                sc = lax.dot_general(rot(q[rs, hc]), rot(k[rs, hc]), (((1,), (1,)), ((), ())),
                                     preferred_element_type=jnp.float32)
                sc = jnp.where(tri, sc * HEAD ** -0.5, -jnp.inf)
                ex = jnp.exp(sc - jnp.max(sc, axis=-1, keepdims=True))
                p = (ex / jnp.sum(ex, axis=-1, keepdims=True)).astype(jnp.bfloat16)
                outs.append(jnp.dot(p, v[rs, hc], preferred_element_type=jnp.float32).astype(jnp.bfloat16))
            heads.append(jnp.concatenate(outs, axis=0))
        o = jnp.concatenate(heads, axis=1)
        acc[...] += jnp.dot(o, obuf[slot, cols, :], preferred_element_type=jnp.float32)

    def within(s, fn, *args):
        pl.when((s >= 0) & (s < STEPS))(lambda: fn(s, *args))

    originate(0)

    def turn(i):
        within(i + 1, originate)
        within(i - 3, wait_loads)
        for k in range(nz - 1):
            within(i, along_z, k)
            within(i - 1, across, k)
            within(i - 2, diagonal, k)
            if k < npair:
                within(i - 3, compute, k)
        within(i - 2, collect)
        pl.when(i == 1)(spread_ids)
        pl.when(i == 2)(prepare)

    loop(STEPS + 3, turn)

    keep_own = pltpu.make_async_copy(ids_out.at[e], idv, csem.at[0])
    keep_own.start()
    keep_own.wait()
    pitch = d // LANES + 1
    tile = pl.ds(0, d // LANES)

    def spill(v, to_a, to_b, b):
        for k in range(d // LANES):
            tm[pl.ds(k, seq, stride=pitch), :] = v[:, k * LANES:(k + 1) * LANES]

        def rows_to(ref, base, lo):
            def some(g):
                for i in range(8):
                    j = g * 8 + i
                    ref[base + j] = tm[pl.ds((lo + j) * pitch, d // LANES), :].astype(jnp.bfloat16)

            return some

        loop(cut // 8, rows_to(to_a, b * cut, 0))
        loop((seq - cut) // 8, rows_to(to_b, b * (seq - cut), cut))

    def route(b):
        h = acc[pl.ds(b * seq, seq), :].astype(jnp.bfloat16).astype(jnp.float32)
        n = h * lax.rsqrt(jnp.mean(h * h, axis=-1, keepdims=True) + EPS)
        logits = jnp.dot(n, wr_ref[...], precision=lax.Precision.HIGHEST, preferred_element_type=jnp.float32).T
        expert = lax.broadcasted_iota(jnp.int32, logits.shape, 0)
        ids = idv[b]
        picked = jnp.concatenate([jnp.sum(jnp.where(expert == ids[k:k + 1, :], logits, 0.0), axis=0, keepdims=True)
                                  for k in range(ids.shape[0])], axis=0)
        ex = jnp.exp(picked - jnp.max(picked, axis=0, keepdims=True))
        gates[b] = ex / jnp.sum(ex, axis=0, keepdims=True)
        spill(n, ua_ref, ub_ref, b)
        spill(h, ha_ref, hb_ref, b)

    loop(nseq, route)
    left = gates[...].reshape(-1, LANES)
    per_tile = d // LANES
    for term in range(3):
        g = left.astype(jnp.bfloat16)
        left = left - g.astype(jnp.float32)
        for i in range(g.shape[0] // per_tile):
            ua_ref[nseq * cut + term * (g.shape[0] // per_tile) + i] = g[i * per_tile:(i + 1) * per_tile, :]

    for i, f in enumerate(mates):
        rcopy(ids_out.at[e], ids_out.at[f], j_s.at[i], j_r.at[f], (r, f)).wait()
    for i, q in enumerate(others):
        rcopy(idt_hbm.at[q], ids_out.at[e, r], i_s.at[i], i_r.at[r], (q, e)).wait_send()
        rcopy(x_hbm.at[q], xg.at[r], x_s.at[i], x_r.at[r], (q, e)).wait_send()

    def drain(s):
        def side(zs, up):
            def sent(w):
                pl.when(z < nz - 1 if up else z > 0)(lambda: z_send(w, s, zs, up).wait_send())
                for j in range(nq):
                    p_copy(w, s, zs, j, c).wait_send()
                xy_send(w, s, zs, r, xs, xr, x_dev).wait_send()
                xy_send(w, s, zs, r, ys, yr, y_dev).wait_send()
                xd_send(w, s, zs, r_y).wait_send()
                yd_send(w, s, zs, r_x).wait_send()

            for_both(s, ep_at(zs, c), sent)

        for k in range(nz - 1):
            each_side(k, side)

        def own(w):
            each_line(lambda up: z_send(w, s, z, up).wait_send())
            p_whole(w, s, e).wait_send()

        for_both(s, e, own)

    loop(STEPS, drain)


def attention(x, idt, wr, wq, wk, wv, wo, cut):
    nseq, seq, d = x.shape
    rows, hd = wq.shape
    nd, k = d // rows, idt.shape[1]
    cols = d // LANES
    half = HEAD // 2
    freq = THETA ** (-jnp.arange(half, dtype=jnp.float32) / half)
    ang = jnp.arange(seq, dtype=jnp.float32)[:, None] * freq
    cos = jnp.concatenate([jnp.cos(ang)] * 2, axis=1)
    sin = jnp.concatenate([-jnp.sin(ang), jnp.sin(ang)], axis=1)
    vmem = pl.BlockSpec(memory_space=pltpu.VMEM)
    hbm = pl.BlockSpec(memory_space=pl.ANY)
    wide = hd // STEPS
    dma = pltpu.SemaphoreType.DMA
    bf = jnp.bfloat16

    def out(*shape, dtype=bf):
        return jax.ShapeDtypeStruct(shape, dtype)

    na, nb = nseq * cut, nseq * (seq - cut)
    return pl.pallas_call(
        functools.partial(attn_kernel, cut),
        out_shape=(out(na + 3 * nseq * k // cols, cols, LANES), out(nb, cols, LANES), out(na, cols, LANES),
                   out(nb, cols, LANES), out(nd, nseq, k, seq, dtype=jnp.int32), out(STEPS, 3, d, wide), out(hd, d)),
        in_specs=[hbm, hbm] + [vmem] * 3 + [hbm] * 4,
        out_specs=(vmem, vmem, vmem, vmem, hbm, hbm, hbm),
        scratch_shapes=[
            pltpu.VMEM((nseq, seq, d), bf), pltpu.VMEM((nseq * seq, d), bf), pltpu.VMEM((nseq * seq, d), jnp.float32),
            pltpu.VMEM((2, 3, d, wide), bf), pltpu.VMEM((2, hd // STEPS, d), bf),
            pltpu.VMEM((seq * (cols + 1), LANES), jnp.float32), pltpu.VMEM((nseq, k, seq), jnp.float32),
            pltpu.VMEM((nseq, k, seq), jnp.int32),
            *([dma((2, STEPS, 4))] * 9), dma((2, 2, STEPS, 4)), *([dma((2, STEPS, 4, 4))] * 2),
            *([dma((4,))] * 4), *([dma((nd,))] * 2), dma((2, nd + 1)), dma((2,)),
        ],
        compiler_params=pltpu.CompilerParams(collective_id=0, has_side_effects=True, vmem_limit_bytes=58 * 1024 * 1024),
        cost_estimate=pl.CostEstimate(flops=10 * nseq * seq * d * hd, bytes_accessed=8 * d * hd, transcendentals=0),
    )(x, idt, cos, sin, wr, wq, wk, wv, wo)[:5]


def token_of(key):
    return lax.shift_right_logical(key, SLOT_BITS) & ((1 << TOKEN_BITS) - 1)


def moe_kernel(nt, nblk_ref, be_ref, bb_ref, bn_ref, key_ref, gate_ref, u_hbm, w1_hbm, w3_hbm, w2_hbm,
               out_hbm, ub, acc, w1, w3, w2, xs, zs, lhs, usem, wsem, osem):
    cols = ub.shape[1]
    nexp = w1_hbm.shape[0]
    nblk = nblk_ref[0]

    def weights(e, slot):
        return (pltpu.make_async_copy(w1_hbm.at[e], w1.at[slot], wsem.at[slot, 0]),
                pltpu.make_async_copy(w3_hbm.at[e], w3.at[slot], wsem.at[slot, 1]),
                pltpu.make_async_copy(w2_hbm.at[e], w2.at[slot], wsem.at[slot, 2]))

    nd = u_hbm.shape[0]
    n = nt // nd
    for dev in range(nd):
        pltpu.make_async_copy(u_hbm.at[dev, pl.ds(0, n)], ub.at[pl.ds(dev * n, n)], usem).start()

    for c in weights(0, 0):
        c.start()

    def zero(i):
        acc[pl.ds(i * 8, 8)] = jnp.zeros((8,) + acc.shape[1:], jnp.float32)

    loop(acc.shape[0] // 8, zero)
    pltpu.make_async_copy(ub.at[pl.ds(0, nt)], ub.at[pl.ds(0, nt)], usem).wait()

    def gather(b):
        base = bb_ref[b]
        for i in range(BM):
            t = token_of(key_ref[base + i])
            xs[pl.ds(i, cols, stride=PITCH), :] = ub[t].astype(jnp.float32)

    def scatter(base, n, rows):
        new = []
        for i in rows:
            key = key_ref[base + i]
            t = jnp.where(i < n, token_of(key), nt)
            new.append((t, acc[t] + gate_ref[key & ((1 << SLOT_BITS) - 1)] * zs[pl.ds(i, cols, stride=PITCH), :]))
        for t, v in new:
            acc[t] = v

    gather(0)

    def body(b, e_prev):
        e = be_ref[b]
        slot = e % 2

        @pl.when(e != e_prev)
        def _():
            @pl.when(e + 1 < nexp)
            def _():
                for c in weights(e + 1, 1 - slot):
                    c.start()

            for c in weights(e, slot):
                c.wait()

        for k in range(cols):
            lhs[:, k * LANES:(k + 1) * LANES] = xs[k * PITCH:k * PITCH + BM, :].astype(jnp.bfloat16)
        gather(b + 1)
        bp = jnp.maximum(b - 1, 0)
        base, n = bb_ref[bp], jnp.where(b > 0, bn_ref[bp], 0)
        for i in range(0, BM, 8):
            scatter(base, n, range(i, i + 8))
        x = lhs[...]
        a1 = jnp.dot(x, w1[slot], preferred_element_type=jnp.float32)
        a3 = jnp.dot(x, w3[slot], preferred_element_type=jnp.float32)
        act = (jax.nn.silu(a1) * a3).astype(jnp.bfloat16)
        z = jnp.dot(act, w2[slot], preferred_element_type=jnp.float32).astype(jnp.bfloat16).astype(jnp.float32)
        for k in range(cols):
            zs[k * PITCH:k * PITCH + BM, :] = z[:, k * LANES:(k + 1) * LANES]
        return e

    lax.fori_loop(0, nblk, body, -1)
    base, n = bb_ref[nblk - 1], bn_ref[nblk - 1]
    for i in range(0, BM, 8):
        scatter(base, n, range(i, i + 8))

    def pack(i):
        for j in range(8):
            t = i * 8 + j
            ub[t] = acc[t].astype(jnp.bfloat16)

    loop(nt // 8, pack)
    store = pltpu.make_async_copy(ub.at[pl.ds(0, nt)], out_hbm, osem)
    store.start()
    store.wait()


def moe(nblk, be, bb, bn, keys, gates, u, n, w1, w3, w2):
    nd, _, cols, _ = u.shape
    nt = nd * n
    ne, d, f = w1.shape
    smem = pl.BlockSpec(memory_space=pltpu.SMEM)
    hbm = pl.BlockSpec(memory_space=pl.ANY)
    return pl.pallas_call(
        functools.partial(moe_kernel, nt),
        out_shape=jax.ShapeDtypeStruct((nt, cols, LANES), jnp.bfloat16),
        in_specs=[smem] * 6 + [hbm] * 4,
        out_specs=hbm,
        scratch_shapes=[
            pltpu.VMEM((nt + 8, cols, LANES), jnp.bfloat16),
            pltpu.VMEM((nt + 8, cols, LANES), jnp.float32),
            pltpu.VMEM((2, d, f), jnp.bfloat16),
            pltpu.VMEM((2, d, f), jnp.bfloat16),
            pltpu.VMEM((2, f, d), jnp.bfloat16),
            pltpu.VMEM((cols * PITCH, LANES), jnp.float32),
            pltpu.VMEM((cols * PITCH, LANES), jnp.float32),
            pltpu.VMEM((BM, d), jnp.bfloat16),
            pltpu.SemaphoreType.DMA,
            pltpu.SemaphoreType.DMA((2, 3)),
            pltpu.SemaphoreType.DMA,
        ],
        compiler_params=pltpu.CompilerParams(vmem_limit_bytes=60 * 1024 * 1024),
        cost_estimate=pl.CostEstimate(flops=6 * 5000 * d * f, bytes_accessed=ne * 3 * d * f * 2, transcendentals=0),
    )(nblk, be, bb, bn, keys, gates, u, w1, w3, w2)


def back_kernel(cut, piece, part, h_ref, ya, y_out, own, prt, raw, fin, fout, yst, raw_s, raw_r, prt_s, prt_r, f_s, f_r,
                y_s, y_r, osem, lsem):
    r, e = lax.axis_index('replica'), lax.axis_index('ep')
    z, c = e // 2, e % 2
    me_p = e + 1 - 2 * c
    n = h_ref.shape[0]
    np_ = n // piece
    split = n // 4 // piece
    mid = (z + 2) // 3 + (5 - z) // 3 - 1
    is_mid, is_end = mid == 1, mid == 0
    low = z // 2
    z_mid = 1 + low
    z_end = 3 * low
    z_oth = 2 - low
    h_a, h_b, h_c = 3 - 3 * low, 2 - low, 3 * low
    replicas = [(r + i) % 4 for i in range(1, 4)]

    def rows(p):
        return pl.ds(p * piece, piece)

    meet([(None, (q, e)) for q in replicas] + [(None, (r, me_p))] +
         [(is_end, (r, ep_at(z_mid, i))) for i in range(2)] + [(is_mid, (r, ep_at(z_end, i))) for i in range(2)] +
         [(is_mid, (r, ep_at(z_oth, c)))], 6 + mid)

    def raw_send(i, c2, p):
        dest = (3 - i) + low * (2 * i - 3)
        return rcopy(part.at[ep_at(dest, c2), rows(p)], raw.at[i, c, rows(p)], raw_s.at[i, c2, p], raw_r.at[i, c, p],
                     (r, ep_at(z_mid, c2)))

    def raw_recv(i, src, p):
        return rcopy(raw.at[i, src, rows(p)], raw.at[i, src, rows(p)], raw_s.at[i, src, p], raw_r.at[i, src, p],
                     (r, ep_at(z_end, src)))

    def prt_copy(hh, p):
        return rcopy(part.at[ep_at(hh, 1 - c), rows(p)], prt.at[hh, rows(p)], prt_s.at[hh, p], prt_r.at[hh, p], (r, me_p))

    def f_copy(i, slot, p, dev):
        return rcopy(fout.at[i, rows(p)], fin.at[slot, rows(p)], f_s.at[i, p], f_r.at[slot, p], dev)

    def loadown(hh):
        return pltpu.make_async_copy(part.at[ep_at(hh, c)], own.at[hh], osem.at[hh])

    def place(half):
        return pl.ds(0, cut) if half < 0 else pl.ds(cut + half * piece, piece)

    def y_copy(src, blk, half):
        return rcopy(src, y_out.at[r, place(half)], y_s.at[blk, half + 1], y_r.at[r, half + 1], (blk, e))

    def y_local(src, half):
        return pltpu.make_async_copy(src, y_out.at[r, place(half)], lsem.at[half + 1])

    def put(src, blk, half):
        @pl.when(r == blk)
        def _():
            y_local(src, half).start()

        @pl.when(r != blk)
        def _():
            y_copy(src, blk, half).start()

    @pl.when(is_end)
    def _():
        loadown(z).start()
        for i in range(3):
            def send(p):
                for c2 in range(2):
                    raw_send(i, c2, p).start()

            loop(np_, send)

        def pass_on(p):
            prt_copy(z, p).start()

        loop(np_, pass_on)

    @pl.when(is_mid)
    def _():
        for hh in (h_a, h_b, h_c, z):
            loadown(hh).start()
        for hh in (h_a, h_b, h_c, z):
            def pass_on(p):
                prt_copy(hh, p).start()

            loop(np_, pass_on)

    for blk in range(4):
        put(ya.at[blk], blk, -1)

    def groups(p, fn):
        def g(j):
            fn(pl.ds(p * piece + j * 8, 8))

        loop(piece // 8, g)

    def f32(v):
        return v.astype(jnp.float32)

    def both(hh, s):
        return f32(own[hh, s]) + f32(prt[hh, s])

    def onward(i, hh, p, dev_slot, incoming):
        prt_copy(hh, p).wait_recv()

        def fn(s):
            fout[i, s] = both(hh, s) + incoming(s)

        groups(p, fn)
        f_copy(i, dev_slot[1], p, dev_slot[0]).start()

    def finish(p, incoming):
        prt_copy(z, p).wait_recv()

        def fn(s):
            yst[s] = (f32(h_ref[s]) + both(z, s) + incoming(s)).astype(jnp.bfloat16)

        groups(p, fn)

        for blk in range(4):
            for half in range(split):
                @pl.when(p == blk * split + half)
                def _():
                    put(yst.at[rows(p)], blk, half)

    @pl.when(is_mid)
    def _():
        loadown(h_a).wait()

        def far(p):
            raw_recv(0, 0, p).wait_recv()
            raw_recv(0, 1, p).wait_recv()
            onward(0, h_a, p, ((r, ep_at(z_oth, c)), 0), lambda s: f32(raw[0, 0, s]) + f32(raw[0, 1, s]))

        loop(np_, far)
        loadown(h_b).wait()
        loadown(h_c).wait()

        def near(p):
            f_copy(2, 0, p, (r, ep_at(z_oth, c))).wait_recv()
            onward(2, h_c, p, ((r, ep_at(z_end, c)), 0), lambda s: fin[0, s])
            raw_recv(1, 0, p).wait_recv()
            raw_recv(1, 1, p).wait_recv()
            onward(1, h_b, p, ((r, ep_at(z_oth, c)), 1), lambda s: f32(raw[1, 0, s]) + f32(raw[1, 1, s]))

        loop(np_, near)
        loadown(z).wait()

        def last(p):
            f_copy(1, 1, p, (r, ep_at(z_oth, c))).wait_recv()
            raw_recv(2, 0, p).wait_recv()
            raw_recv(2, 1, p).wait_recv()
            finish(p, lambda s: fin[1, s] + f32(raw[2, 0, s]) + f32(raw[2, 1, s]))

        loop(np_, last)

    @pl.when(is_end)
    def _():
        loadown(z).wait()

        def last(p):
            f_copy(2, 0, p, (r, ep_at(z_mid, c))).wait_recv()
            finish(p, lambda s: fin[0, s])

        loop(np_, last)

    @pl.when(is_end)
    def _():
        def sent(p):
            for i in range(3):
                for c2 in range(2):
                    raw_send(i, c2, p).wait_send()
            prt_copy(z, p).wait_send()

        loop(np_, sent)

    @pl.when(is_mid)
    def _():
        def sent(p):
            for hh in (h_a, h_b, h_c, z):
                prt_copy(hh, p).wait_send()
            f_copy(0, 0, p, (r, ep_at(z_oth, c))).wait_send()
            f_copy(1, 1, p, (r, ep_at(z_oth, c))).wait_send()
            f_copy(2, 0, p, (r, ep_at(z_end, c))).wait_send()

        loop(np_, sent)

    for blk in range(4):
        for half in range(-1, split):
            some = ya.at[blk] if half < 0 else yst.at[rows(0)]

            @pl.when(r == blk)
            def _():
                y_local(some, half).wait()

            @pl.when(r != blk)
            def _():
                y_copy(some, blk, half).wait_send()
                ref = y_out.at[blk, place(half)]
                rcopy(ref, ref, y_s.at[blk, half + 1], y_r.at[blk, half + 1], (blk, e)).wait_recv()


def back(part, h, ya):
    _, n, cols, _ = part.shape
    cut = ya.shape[1]
    seq = cut + n // 4
    piece = n // 8
    vmem = pl.BlockSpec(memory_space=pltpu.VMEM)
    hbm = pl.BlockSpec(memory_space=pl.ANY)
    dma = pltpu.SemaphoreType.DMA
    np_ = n // piece

    def tiles(lead, dtype):
        return pltpu.VMEM(lead + (cols, LANES), dtype)

    return pl.pallas_call(
        functools.partial(back_kernel, cut, piece),
        out_shape=jax.ShapeDtypeStruct((4, seq, cols, LANES), jnp.bfloat16),
        in_specs=[hbm, vmem, hbm],
        out_specs=hbm,
        scratch_shapes=[
            tiles((4, n), jnp.bfloat16), tiles((4, n), jnp.bfloat16), tiles((3, 2, n), jnp.bfloat16),
            tiles((2, n), jnp.float32), tiles((3, n), jnp.float32), tiles((n,), jnp.bfloat16),
            dma((3, 2, np_)), dma((3, 2, np_)), dma((4, np_)), dma((4, np_)), dma((3, np_)), dma((2, np_)),
            dma((4, 3)), dma((4, 3)), dma((4,)), dma((3,)),
        ],
        compiler_params=pltpu.CompilerParams(collective_id=1, has_side_effects=True, vmem_limit_bytes=58 * 1024 * 1024),
    )(part, h, ya)


def block_plan(ids, me, ne):
    _, nseq, _, n = ids.shape
    le = ids - me * ne
    local = (le >= 0) & (le < ne)
    total = ids.size
    slot = lax.iota(jnp.int32, total).reshape(ids.shape)
    token = (lax.broadcasted_iota(jnp.int32, ids.shape, 0) * nseq + lax.broadcasted_iota(jnp.int32, ids.shape, 1)) * n
    token = token + lax.broadcasted_iota(jnp.int32, ids.shape, 3)
    key = (le << (SLOT_BITS + TOKEN_BITS)) | (token << SLOT_BITS) | slot
    none = jnp.iinfo(jnp.int32).max
    keys = lax.sort(jnp.where(local, key, none).reshape(-1), is_stable=False)
    experts = jnp.arange(ne, dtype=jnp.int32)
    counts = jnp.sum((le.reshape(-1)[None, :] == experts[:, None]).astype(jnp.int32), axis=1)
    low = (experts[None, :] < experts[:, None])
    first = jnp.sum(jnp.where(low, counts[None, :], 0), axis=1)
    nb = jnp.maximum((counts + BM - 1) // BM, 1)
    bfirst = jnp.sum(jnp.where(low, nb[None, :], 0), axis=1)
    maxb = total // BM + ne + 2
    b = jnp.arange(maxb, dtype=jnp.int32)
    inside = (b[:, None] >= bfirst[None, :]) & (b[:, None] < (bfirst + nb)[None, :])

    def of(v):
        return jnp.sum(jnp.where(inside, v[None, :], 0), axis=1)

    done = (b - of(bfirst)) * BM
    be, bb = of(experts), of(first) + done
    bn = jnp.clip(of(counts) - done, 0, BM)
    bb = jnp.where(jnp.any(inside, axis=1), bb, 0)
    keys = jnp.concatenate([jnp.where(keys == none, 0, keys), jnp.zeros((BM,), jnp.int32)])
    return jnp.sum(nb).reshape(1), be, bb, bn, keys


def solution(mesh):
    nd = mesh.shape['ep']
    tok = P(('replica', 'ep'), None, None)
    rows_ep = P('ep', None)
    by_expert = P('ep', None, None)
    cut = CUT

    def local(x, wq, wk, wv, wo, wr, w1, w3, w2, idx):
        b, s, d = x.shape
        k, ne = idx.shape[-1], w1.shape[0]
        me = lax.axis_index('ep')
        cols = d // LANES
        ua, ub, ha, hb, ids = attention(x, idx.transpose(0, 2, 1), wr, wq, wk, wv, wo, cut)

        def experts(u, gates, lo, hi):
            n = b * (hi - lo)
            plan = block_plan(ids[..., lo:hi], me, ne)
            return moe(*plan, gates[..., lo:hi].reshape(-1), u, n, w1, w3, w2).reshape(nd, n, cols, LANES)

        u_all = lax.all_gather(ua, 'ep', axis=0, tiled=False)
        terms = u_all[:, b * cut:].reshape(nd, 3, b, k, s).astype(jnp.float32)
        gates = terms[:, 0] + terms[:, 1] + terms[:, 2]
        part_a = experts(u_all, gates, 0, cut)
        part_a = lax.all_to_all(part_a, 'ep', 0, 0, tiled=True)
        part_b = experts(lax.all_gather(ub, 'ep', axis=0, tiled=False), gates, cut, s)
        ya = ha.astype(jnp.float32) + jnp.sum(part_a.astype(jnp.float32), axis=0)
        y = back(part_b, hb, ya.astype(jnp.bfloat16).reshape(b, cut, cols, LANES))
        return y.reshape(b, s, d)

    return jax.shard_map(local, mesh=mesh,
                         in_specs=(tok, rows_ep, rows_ep, rows_ep, rows_ep, P(None, None),
                                   by_expert, by_expert, by_expert, tok),
                         out_specs=tok, check_vma=False)
```

```python
import functools
import jax
import jax.numpy as jnp
from jax import lax
from jax.experimental import pallas as pl
from jax.experimental.pallas import tpu as pltpu
from jax.sharding import PartitionSpec as P

HEAD = 128
EPS = 1e-6
THETA = 10000.0
BM = 128
PITCH = BM + 1
LANES = 128
CUT = 40
STEPS = 8
SLOT_BITS, TOKEN_BITS = 15, 12


def loop(n, fn):
    def step(i, carry):
        fn(i)
        return carry

    lax.fori_loop(0, n, step, 0)


def ep_at(z, c):
    return 2 * z + c


MESH_ID = pl.DeviceIdType.MESH


def rcopy(src, dst, ssem, rsem, dev):
    return pltpu.make_async_remote_copy(src_ref=src, dst_ref=dst, send_sem=ssem, recv_sem=rsem, device_id=dev,
                                        device_id_type=MESH_ID)


def meet(peers, count):
    barrier = pltpu.get_barrier_semaphore()
    for guard, dev in peers:
        def greet():
            pl.semaphore_signal(barrier, device_id=dev, device_id_type=MESH_ID)

        if guard is None:
            greet()
        else:
            pl.when(guard)(greet)
    pl.semaphore_wait(barrier, count)


def attn_kernel(cut, x_hbm, idt_hbm, cos_ref, sin_ref, wr_ref, wq_ref, wk_ref, wv_ref, wo_ref,
                ua_ref, ub_ref, ha_ref, hb_ref, ids_out, gw, go,
                xg, a_ref, acc, wbuf, obuf, tm, gates, idv, zr, zp, zm, xr, yr, xs, ys, xd, yd, dr, pr, ps,
                x_s, x_r, i_s, i_r, j_s, j_r, lsem, csem):
    r, e = lax.axis_index('replica'), lax.axis_index('ep')
    nz, nq = 4, 4
    z, c = e // 2, e % 2
    e_p = ep_at(z, 1 - c)
    r_x, r_y = (r + 2) % nq, r + 1 - 2 * (r % 2)
    r_d = (r_y + 2) % nq
    nd = ids_out.shape[0]
    rows, wide = wq_ref.shape[0], wq_ref.shape[1] // STEPS
    quarter = rows // nq
    orows = go.shape[0] // STEPS
    nseq, seq, d = x_hbm.shape
    partner, x_dev, y_dev = (r, e_p), (r_x, e), (r_y, e)
    per = STEPS // nd

    def mod(v, m):
        return lax.rem(v, m)

    others = [mod(r + i, nq) for i in range(1, nq)]
    mates = [mod(e + i, nd) for i in range(1, nd)]
    meet([(None, (q, e)) for q in others] + [(None, (r, f)) for f in mates], len(others) + len(mates))

    for i, q in enumerate(others):
        rcopy(idt_hbm.at[q], ids_out.at[e, r], i_s.at[i], i_r.at[r], (q, e)).start()
        rcopy(x_hbm.at[q], xg.at[r], x_s.at[i], x_r.at[r], (q, e)).start()
    keep_ids = pltpu.make_async_copy(idt_hbm.at[r], ids_out.at[e, r], csem.at[0])
    keep_x = pltpu.make_async_copy(x_hbm.at[r], xg.at[r], csem.at[1])
    keep_ids.start()
    keep_x.start()

    def spread_ids():
        keep_ids.wait()
        for i, q in enumerate(others):
            rcopy(idt_hbm.at[q], ids_out.at[e, q], i_s.at[i], i_r.at[q], (q, e)).wait_recv()
        for i, f in enumerate(mates):
            rcopy(ids_out.at[e], ids_out.at[e], j_s.at[i], j_r.at[e], (r, f)).start()

    def prepare():
        keep_x.wait()
        for i, q in enumerate(others):
            rcopy(x_hbm.at[q], xg.at[q], x_s.at[i], x_r.at[q], (q, e)).wait_recv()

        def norm(b):
            x = xg[b].astype(jnp.float32)
            at = pl.ds(b * seq, seq)
            a_ref[at, :] = (x * lax.rsqrt(jnp.mean(x * x, axis=-1, keepdims=True) + EPS)).astype(jnp.bfloat16)
            acc[at, :] = x

        loop(nseq, norm)

    def piece(w, s, f, q):
        if w:
            return go.at[pl.ds(s * orows + q * (orows // nq), orows // nq), :]
        return gw.at[s, :, pl.ds(f * rows + q * quarter, quarter), :]

    def half(w, s, zs, q, i):
        if w:
            n = orows // nq // 2
            return go.at[pl.ds(s * orows + (2 * q + i) * n, n), :]
        n = quarter // 2
        return gw.at[s, :, pl.ds(ep_at(zs, c) * rows + (2 * q + i) * n, n), :]

    def own_wo(s, lo, n):
        return wo_ref.at[pl.ds(mod(s, per) * orows + lo, n), :]

    def z_send(w, s, zs, up):
        ref = piece(w, s, ep_at(zs, c), r)
        return rcopy(ref, ref, (zp if up else zm).at[w, s, zs], zr.at[w, s, zs], (r, e + 2) if up else (r, e - 2))

    def xy_send(w, s, zs, q, ssem, rsem, dev):
        ref = piece(w, s, ep_at(zs, c), q)
        return rcopy(ref, ref, ssem.at[w, s, zs], rsem.at[w, s, zs], dev)

    def xd_send(w, s, zs, q):
        ref = half(w, s, zs, q, 1)
        return rcopy(ref, ref, xd.at[w, s, zs], dr.at[1, w, s, zs], x_dev)

    def yd_send(w, s, zs, q):
        ref = half(w, s, zs, q, 0)
        return rcopy(ref, ref, yd.at[w, s, zs], dr.at[0, w, s, zs], y_dev)

    def p_copy(w, s, zs, j, core):
        ref = piece(w, s, ep_at(zs, core), (r, r_x, r_y, r_d)[j])
        return rcopy(ref, ref, ps.at[w, s, zs, j], pr.at[w, s, zs, j], partner)

    def p_whole(w, s, f):
        ref = go.at[pl.ds(s * orows, orows), :] if w else gw.at[s, :, pl.ds(f * rows, rows), :]
        return rcopy(ref, ref, ps.at[w, s, z, 0], pr.at[w, s, z, 0], partner)

    def own_parts(s):
        return [(w.at[:, pl.ds(s * wide, wide)], m) for m, w in enumerate((wq_ref, wk_ref, wv_ref))]

    def if_wo(s, f, *fns):
        @pl.when(s // per == f)
        def _():
            for fn in fns:
                fn()

    def each_line(fn):
        pl.when(z > 0)(lambda: fn(False))
        pl.when(z < nz - 1)(lambda: fn(True))

    def each_side(k, fn):
        pl.when(z - k - 1 >= 0)(lambda: fn(z - k - 1, True))
        pl.when(z + k + 1 < nz)(lambda: fn(z + k + 1, False))

    def originate(s):
        def line(up):
            sem = zp if up else zm
            dev = (r, e + 2) if up else (r, e - 2)
            for w, m in own_parts(s):
                rcopy(w.at[pl.ds(r * quarter, quarter), :], gw.at[s, m, pl.ds(e * rows + r * quarter, quarter), :],
                      sem.at[0, s, z], zr.at[0, s, z], dev).start()
            if_wo(s, e, lambda: rcopy(own_wo(s, r * (orows // nq), orows // nq), piece(1, s, e, r), sem.at[1, s, z],
                                      zr.at[1, s, z], dev).start())

        each_line(line)
        for w, m in own_parts(s):
            rcopy(w, gw.at[s, m, pl.ds(e * rows, rows), :], ps.at[0, s, z, 0], pr.at[0, s, z, 0], partner).start()
        if_wo(s, e, lambda: rcopy(own_wo(s, 0, orows), go.at[pl.ds(s * orows, orows), :], ps.at[1, s, z, 0],
                                  pr.at[1, s, z, 0], partner).start())

    def for_both(s, f, fn):
        fn(0)
        if_wo(s, f, lambda: fn(1))

    def along_z(s, k):
        def side(zs, up):
            def one(w):
                z_send(w, s, zs, up).wait_recv()
                pl.when(z < nz - 1 if up else z > 0)(lambda: z_send(w, s, zs, up).start())
                xy_send(w, s, zs, r, xs, xr, x_dev).start()
                xy_send(w, s, zs, r, ys, yr, y_dev).start()
                p_copy(w, s, zs, 0, c).start()

            for_both(s, ep_at(zs, c), one)

        each_side(k, side)

    def across(s, k):
        def side(zs, up):
            def one(w):
                xy_send(w, s, zs, r_x, xs, xr, x_dev).wait_recv()
                yd_send(w, s, zs, r_x).start()
                p_copy(w, s, zs, 1, c).start()
                xy_send(w, s, zs, r_y, ys, yr, y_dev).wait_recv()
                xd_send(w, s, zs, r_y).start()
                p_copy(w, s, zs, 2, c).start()

            for_both(s, ep_at(zs, c), one)

        each_side(k, side)

    def diagonal(s, k):
        def side(zs, up):
            def one(w):
                xd_send(w, s, zs, r_d).wait_recv()
                yd_send(w, s, zs, r_d).wait_recv()
                p_copy(w, s, zs, 3, c).start()

            for_both(s, ep_at(zs, c), one)

        each_side(k, side)

    def load(s, f):
        slot = mod(s, 2)
        return pltpu.make_async_copy(gw.at[s, :, pl.ds(f * rows, rows), :], wbuf.at[slot, :, pl.ds(f * rows, rows), :],
                                     lsem.at[slot, f])

    def oload(s, src):
        slot = mod(s, 2)
        return pltpu.make_async_copy(src, obuf.at[slot], lsem.at[slot, nd])

    def collect(s):
        slot = mod(s, 2)
        whole = go.at[pl.ds(s * orows, orows), :]

        def side(zs, up):
            def one(w):
                for j in range(nq):
                    p_copy(w, s, zs, j, 1 - c).wait_recv()

            for_both(s, ep_at(zs, 1 - c), one)

        for k in range(nz - 1):
            each_side(k, side)
        p_whole(0, s, e_p).wait_recv()
        if_wo(s, e_p, lambda: p_whole(1, s, e_p).wait_recv())

        for f in range(nd):
            def near():
                for w, m in own_parts(s):
                    pltpu.make_async_copy(w, wbuf.at[slot, m, pl.ds(f * rows, rows), :], lsem.at[slot, f]).start()

            pl.when(f == e)(near)
            pl.when(f != e)(lambda: load(s, f).start())
        if_wo(s, e, lambda: oload(s, own_wo(s, 0, orows)).start())
        pl.when(s // per != e)(lambda: oload(s, whole).start())

    def wait_loads(s):
        for f in range(nd):
            load(s, f).wait()
        oload(s, go.at[pl.ds(s * orows, orows), :]).wait()

    pair = 2 * HEAD
    npair = wide // pair

    def compute(s, j):
        slot = mod(s, 2)
        a = a_ref[...]
        cols = slice(j * pair, (j + 1) * pair)
        cos, sin = cos_ref[...], sin_ref[...]

        def rot(v):
            return (v * cos + pltpu.roll(v, HEAD // 2, 1) * sin).astype(jnp.bfloat16)

        q, k, v = [jnp.dot(a, wbuf[slot, m, :, cols], preferred_element_type=jnp.float32) for m in range(3)]
        v = v.astype(jnp.bfloat16)
        tri = lax.broadcasted_iota(jnp.int32, (seq, seq), 0) >= lax.broadcasted_iota(jnp.int32, (seq, seq), 1)
        heads = []
        for hh in range(2):
            hc = slice(hh * HEAD, (hh + 1) * HEAD)
            outs = []
            for b in range(nseq):
                rs = slice(b * seq, (b + 1) * seq)
                sc = lax.dot_general(rot(q[rs, hc]), rot(k[rs, hc]), (((1,), (1,)), ((), ())),
                                     preferred_element_type=jnp.float32)
                sc = jnp.where(tri, sc * HEAD ** -0.5, -jnp.inf)
                ex = jnp.exp(sc - jnp.max(sc, axis=-1, keepdims=True))
                p = (ex / jnp.sum(ex, axis=-1, keepdims=True)).astype(jnp.bfloat16)
                outs.append(jnp.dot(p, v[rs, hc], preferred_element_type=jnp.float32).astype(jnp.bfloat16))
            heads.append(jnp.concatenate(outs, axis=0))
        o = jnp.concatenate(heads, axis=1)
        acc[...] += jnp.dot(o, obuf[slot, cols, :], preferred_element_type=jnp.float32)

    def within(s, fn, *args):
        pl.when((s >= 0) & (s < STEPS))(lambda: fn(s, *args))

    originate(0)

    def turn(i):
        within(i + 1, originate)
        within(i - 3, wait_loads)
        for k in range(nz - 1):
            within(i, along_z, k)
            within(i - 1, across, k)
            within(i - 2, diagonal, k)
            if k < npair:
                within(i - 3, compute, k)
        within(i - 2, collect)
        pl.when(i == 1)(spread_ids)
        pl.when(i == 2)(prepare)

    loop(STEPS + 3, turn)

    keep_own = pltpu.make_async_copy(ids_out.at[e], idv, csem.at[0])
    keep_own.start()
    keep_own.wait()
    pitch = d // LANES + 1
    tile = pl.ds(0, d // LANES)

    def spill(v, to_a, to_b, b):
        for k in range(d // LANES):
            tm[pl.ds(k, seq, stride=pitch), :] = v[:, k * LANES:(k + 1) * LANES]

        def rows_to(ref, base, lo):
            def some(g):
                for i in range(8):
                    j = g * 8 + i
                    ref[base + j] = tm[pl.ds((lo + j) * pitch, d // LANES), :].astype(jnp.bfloat16)

            return some

        loop(cut // 8, rows_to(to_a, b * cut, 0))
        loop((seq - cut) // 8, rows_to(to_b, b * (seq - cut), cut))

    def route(b):
        h = acc[pl.ds(b * seq, seq), :].astype(jnp.bfloat16).astype(jnp.float32)
        n = h * lax.rsqrt(jnp.mean(h * h, axis=-1, keepdims=True) + EPS)
        logits = jnp.dot(n, wr_ref[...], precision=lax.Precision.HIGHEST, preferred_element_type=jnp.float32).T
        expert = lax.broadcasted_iota(jnp.int32, logits.shape, 0)
        ids = idv[b]
        picked = jnp.concatenate([jnp.sum(jnp.where(expert == ids[k:k + 1, :], logits, 0.0), axis=0, keepdims=True)
                                  for k in range(ids.shape[0])], axis=0)
        ex = jnp.exp(picked - jnp.max(picked, axis=0, keepdims=True))
        gates[b] = ex / jnp.sum(ex, axis=0, keepdims=True)
        spill(n, ua_ref, ub_ref, b)
        spill(h, ha_ref, hb_ref, b)

    loop(nseq, route)
    left = gates[...].reshape(-1, LANES)
    per_tile = d // LANES
    for term in range(3):
        g = left.astype(jnp.bfloat16)
        left = left - g.astype(jnp.float32)
        for i in range(g.shape[0] // per_tile):
            ua_ref[nseq * cut + term * (g.shape[0] // per_tile) + i] = g[i * per_tile:(i + 1) * per_tile, :]

    for i, f in enumerate(mates):
        rcopy(ids_out.at[e], ids_out.at[f], j_s.at[i], j_r.at[f], (r, f)).wait()
    for i, q in enumerate(others):
        rcopy(idt_hbm.at[q], ids_out.at[e, r], i_s.at[i], i_r.at[r], (q, e)).wait_send()
        rcopy(x_hbm.at[q], xg.at[r], x_s.at[i], x_r.at[r], (q, e)).wait_send()

    def drain(s):
        def side(zs, up):
            def sent(w):
                pl.when(z < nz - 1 if up else z > 0)(lambda: z_send(w, s, zs, up).wait_send())
                for j in range(nq):
                    p_copy(w, s, zs, j, c).wait_send()
                xy_send(w, s, zs, r, xs, xr, x_dev).wait_send()
                xy_send(w, s, zs, r, ys, yr, y_dev).wait_send()
                xd_send(w, s, zs, r_y).wait_send()
                yd_send(w, s, zs, r_x).wait_send()

            for_both(s, ep_at(zs, c), sent)

        for k in range(nz - 1):
            each_side(k, side)

        def own(w):
            each_line(lambda up: z_send(w, s, z, up).wait_send())
            p_whole(w, s, e).wait_send()

        for_both(s, e, own)

    loop(STEPS, drain)


def attention(x, idt, wr, wq, wk, wv, wo, cut):
    nseq, seq, d = x.shape
    rows, hd = wq.shape
    nd, k = d // rows, idt.shape[1]
    cols = d // LANES
    half = HEAD // 2
    freq = THETA ** (-jnp.arange(half, dtype=jnp.float32) / half)
    ang = jnp.arange(seq, dtype=jnp.float32)[:, None] * freq
    cos = jnp.concatenate([jnp.cos(ang)] * 2, axis=1)
    sin = jnp.concatenate([-jnp.sin(ang), jnp.sin(ang)], axis=1)
    vmem = pl.BlockSpec(memory_space=pltpu.VMEM)
    hbm = pl.BlockSpec(memory_space=pl.ANY)
    wide = hd // STEPS
    dma = pltpu.SemaphoreType.DMA
    bf = jnp.bfloat16

    def out(*shape, dtype=bf):
        return jax.ShapeDtypeStruct(shape, dtype)

    na, nb = nseq * cut, nseq * (seq - cut)
    return pl.pallas_call(
        functools.partial(attn_kernel, cut),
        out_shape=(out(na + 3 * nseq * k // cols, cols, LANES), out(nb, cols, LANES), out(na, cols, LANES),
                   out(nb, cols, LANES), out(nd, nseq, k, seq, dtype=jnp.int32), out(STEPS, 3, d, wide), out(hd, d)),
        in_specs=[hbm, hbm] + [vmem] * 3 + [hbm] * 4,
        out_specs=(vmem, vmem, vmem, vmem, hbm, hbm, hbm),
        scratch_shapes=[
            pltpu.VMEM((nseq, seq, d), bf), pltpu.VMEM((nseq * seq, d), bf), pltpu.VMEM((nseq * seq, d), jnp.float32),
            pltpu.VMEM((2, 3, d, wide), bf), pltpu.VMEM((2, hd // STEPS, d), bf),
            pltpu.VMEM((seq * (cols + 1), LANES), jnp.float32), pltpu.VMEM((nseq, k, seq), jnp.float32),
            pltpu.VMEM((nseq, k, seq), jnp.int32),
            *([dma((2, STEPS, 4))] * 9), dma((2, 2, STEPS, 4)), *([dma((2, STEPS, 4, 4))] * 2),
            *([dma((4,))] * 4), *([dma((nd,))] * 2), dma((2, nd + 1)), dma((2,)),
        ],
        compiler_params=pltpu.CompilerParams(collective_id=0, has_side_effects=True, vmem_limit_bytes=58 * 1024 * 1024),
        cost_estimate=pl.CostEstimate(flops=10 * nseq * seq * d * hd, bytes_accessed=8 * d * hd, transcendentals=0),
    )(x, idt, cos, sin, wr, wq, wk, wv, wo)[:5]


def token_of(key):
    return lax.shift_right_logical(key, SLOT_BITS) & ((1 << TOKEN_BITS) - 1)


def moe_kernel(nt, nblk_ref, be_ref, bb_ref, bn_ref, key_ref, gate_ref, u_hbm, w1_hbm, w3_hbm, w2_hbm,
               out_hbm, ub, acc, w1, w3, w2, xs, zs, lhs, usem, wsem, osem):
    cols = ub.shape[1]
    nexp = w1_hbm.shape[0]
    nblk = nblk_ref[0]

    def weights(e, slot):
        return (pltpu.make_async_copy(w1_hbm.at[e], w1.at[slot], wsem.at[slot, 0]),
                pltpu.make_async_copy(w3_hbm.at[e], w3.at[slot], wsem.at[slot, 1]),
                pltpu.make_async_copy(w2_hbm.at[e], w2.at[slot], wsem.at[slot, 2]))

    nd = u_hbm.shape[0]
    n = nt // nd
    for dev in range(nd):
        pltpu.make_async_copy(u_hbm.at[dev, pl.ds(0, n)], ub.at[pl.ds(dev * n, n)], usem).start()

    for c in weights(0, 0):
        c.start()

    def zero(i):
        acc[pl.ds(i * 8, 8)] = jnp.zeros((8,) + acc.shape[1:], jnp.float32)

    loop(acc.shape[0] // 8, zero)
    pltpu.make_async_copy(ub.at[pl.ds(0, nt)], ub.at[pl.ds(0, nt)], usem).wait()

    def gather(b):
        base = bb_ref[b]
        for i in range(BM):
            t = token_of(key_ref[base + i])
            xs[pl.ds(i, cols, stride=PITCH), :] = ub[t].astype(jnp.float32)

    def scatter(base, n, rows):
        new = []
        for i in rows:
            key = key_ref[base + i]
            t = jnp.where(i < n, token_of(key), nt)
            new.append((t, acc[t] + gate_ref[key & ((1 << SLOT_BITS) - 1)] * zs[pl.ds(i, cols, stride=PITCH), :]))
        for t, v in new:
            acc[t] = v

    gather(0)

    def body(b, e_prev):
        e = be_ref[b]
        slot = e % 2

        @pl.when(e != e_prev)
        def _():
            @pl.when(e + 1 < nexp)
            def _():
                for c in weights(e + 1, 1 - slot):
                    c.start()

            for c in weights(e, slot):
                c.wait()

        for k in range(cols):
            lhs[:, k * LANES:(k + 1) * LANES] = xs[k * PITCH:k * PITCH + BM, :].astype(jnp.bfloat16)
        gather(b + 1)
        bp = jnp.maximum(b - 1, 0)
        base, n = bb_ref[bp], jnp.where(b > 0, bn_ref[bp], 0)
        for i in range(0, BM, 8):
            scatter(base, n, range(i, i + 8))
        x = lhs[...]
        a1 = jnp.dot(x, w1[slot], preferred_element_type=jnp.float32)
        a3 = jnp.dot(x, w3[slot], preferred_element_type=jnp.float32)
        act = (jax.nn.silu(a1) * a3).astype(jnp.bfloat16)
        z = jnp.dot(act, w2[slot], preferred_element_type=jnp.float32).astype(jnp.bfloat16).astype(jnp.float32)
        for k in range(cols):
            zs[k * PITCH:k * PITCH + BM, :] = z[:, k * LANES:(k + 1) * LANES]
        return e

    lax.fori_loop(0, nblk, body, -1)
    base, n = bb_ref[nblk - 1], bn_ref[nblk - 1]
    for i in range(0, BM, 8):
        scatter(base, n, range(i, i + 8))

    def pack(i):
        for j in range(8):
            t = i * 8 + j
            ub[t] = acc[t].astype(jnp.bfloat16)

    loop(nt // 8, pack)
    store = pltpu.make_async_copy(ub.at[pl.ds(0, nt)], out_hbm, osem)
    store.start()
    store.wait()


def moe(nblk, be, bb, bn, keys, gates, u, n, w1, w3, w2):
    nd, _, cols, _ = u.shape
    nt = nd * n
    ne, d, f = w1.shape
    smem = pl.BlockSpec(memory_space=pltpu.SMEM)
    hbm = pl.BlockSpec(memory_space=pl.ANY)
    return pl.pallas_call(
        functools.partial(moe_kernel, nt),
        out_shape=jax.ShapeDtypeStruct((nt, cols, LANES), jnp.bfloat16),
        in_specs=[smem] * 6 + [hbm] * 4,
        out_specs=hbm,
        scratch_shapes=[
            pltpu.VMEM((nt + 8, cols, LANES), jnp.bfloat16),
            pltpu.VMEM((nt + 8, cols, LANES), jnp.float32),
            pltpu.VMEM((2, d, f), jnp.bfloat16),
            pltpu.VMEM((2, d, f), jnp.bfloat16),
            pltpu.VMEM((2, f, d), jnp.bfloat16),
            pltpu.VMEM((cols * PITCH, LANES), jnp.float32),
            pltpu.VMEM((cols * PITCH, LANES), jnp.float32),
            pltpu.VMEM((BM, d), jnp.bfloat16),
            pltpu.SemaphoreType.DMA,
            pltpu.SemaphoreType.DMA((2, 3)),
            pltpu.SemaphoreType.DMA,
        ],
        compiler_params=pltpu.CompilerParams(vmem_limit_bytes=60 * 1024 * 1024),
        cost_estimate=pl.CostEstimate(flops=6 * 5000 * d * f, bytes_accessed=ne * 3 * d * f * 2, transcendentals=0),
    )(nblk, be, bb, bn, keys, gates, u, w1, w3, w2)


def back_kernel(cut, piece, part, h_ref, ya, y_out, own, prt, raw, fin, fout, hs, yst, raw_s, raw_r, prt_s, prt_r, f_s, f_r,
                h_s, h_r, y_s, y_r, osem, lsem):
    r, e = lax.axis_index('replica'), lax.axis_index('ep')
    z, c = e // 2, e % 2
    n = h_ref.shape[0]
    pieces = n // piece
    split = pieces // 4
    mid = (z + 2) // 3 + (5 - z) // 3 - 1
    low = z // 2
    on_mid, on_end = pl.when(mid == 1), pl.when(mid == 0)
    z_mid, z_end = 1 + low, 3 * low
    partner, across = (r, ep_at(z, 1 - c)), (r, ep_at(2 - low, c))
    to_end = (r, ep_at(z_end, c))
    others = [lax.rem(r + i, 4) for i in range(1, 4)]

    def far(i):
        return 2 + i + low * (-1 - 2 * i)

    def near(i):
        return 1 - i + low * (1 + 2 * i)

    def rows(p):
        return pl.ds(p * piece, piece)

    end, inner = mid == 0, mid == 1
    meet([(None, (q, e)) for q in others] + [(None, partner)] +
         [(end, (q, ep_at(z_mid, c))) for q in range(4)] + [(end, (r, ep_at(z_mid, 1 - c)))] +
         [(inner, (q, ep_at(z_end, c))) for q in range(4)] + [(inner, (r, ep_at(z_end, 1 - c))), (inner, across)], 9 + mid)

    def raw_send(i, core, p):
        return rcopy(part.at[ep_at(far(i), core), rows(p)], raw.at[i, c, rows(p)], raw_s.at[i, core, p], raw_r.at[i, c, p],
                     (r, ep_at(z_mid, core)))

    def raw_recv(i, core, p):
        ref = raw.at[i, core, rows(p)]
        return rcopy(ref, ref, raw_s.at[i, core, p], raw_r.at[i, core, p], (r, ep_at(z_end, core)))

    def prt_copy(chip, p):
        return rcopy(part.at[ep_at(chip, 1 - c), rows(p)], prt.at[chip, rows(p)], prt_s.at[chip, p], prt_r.at[chip, p], partner)

    def f_copy(i, p, onward):
        return rcopy(fout.at[2 * onward + i, rows(p)], fin.at[i, rows(p)], f_s.at[2 * onward + i, p], f_r.at[i, p],
                     to_end if onward else across)

    def load(chip):
        return pltpu.make_async_copy(part.at[ep_at(chip, c)], own.at[chip], osem.at[chip])

    send_h = rcopy(h_ref, hs, h_s, h_r, to_end)

    def place(half):
        return pl.ds(0, cut) if half < 0 else pl.ds(cut + half * piece, piece)

    def y_copy(src, i, blk, half, f):
        return rcopy(src, y_out.at[r, place(half)], y_s.at[i, blk, half + 1], y_r.at[r, half + 1], (blk, f))

    def y_local(src, half):
        return pltpu.make_async_copy(src, y_out.at[r, place(half)], lsem.at[half + 1])

    def put(src, blk, half):
        pl.when(r == blk)(lambda: y_local(src, half).start())
        pl.when(r != blk)(lambda: y_copy(src, 1, blk, half, e).start())

    def each(fn, count=pieces):
        loop(count, fn)

    for i in range(2):
        load(near(i)).start()

    @on_end
    def _():
        for i in range(2):
            each(lambda p: [raw_send(i, core, p).start() for core in range(2)])
            each(lambda p: prt_copy(near(i), p).start())

    @on_mid
    def _():
        send_h.start()
        for i in range(2):
            load(far(i)).start()
            each(lambda p: [prt_copy(far(i), p).start(), prt_copy(near(i), p).start()])

    for blk in range(4):
        put(ya.at[blk], blk, -1)

    def f32(v):
        return v.astype(jnp.float32)

    def add(chip, p, incoming, out, finish=f32):
        prt_copy(chip, p).wait_recv()

        def some(j):
            s = pl.ds(p * piece + j * 4, 4)
            out[s] = finish(f32(own[chip, s]) + f32(prt[chip, s]) + incoming(s))

        each(some, piece // 4)

    @on_mid
    def _():
        for i in range(2):
            load(far(i)).wait()
            load(near(i)).wait()

        def first(q):
            i, p = q // pieces, lax.rem(q, pieces)
            for core in range(2):
                raw_recv(i, core, p).wait_recv()
            add(far(i), p, lambda s: f32(raw[i, 0, s]) + f32(raw[i, 1, s]), fout.at[i])
            f_copy(i, p, 0).start()

        def second(q):
            i, p = q // pieces, lax.rem(q, pieces)
            f_copy(i, p, 0).wait_recv()
            add(near(i), p, lambda s: fin[i, s], fout.at[2 + i])
            f_copy(i, p, 1).start()

        lag = 2

        def step(q):
            pl.when(q < 2 * pieces)(lambda: first(q))
            pl.when(q >= lag)(lambda: second(q - lag))

        each(step, 2 * pieces + lag)

    @on_end
    def _():
        for i in range(2):
            load(near(i)).wait()
            if i == 0:
                send_h.wait_recv()
            h = h_ref if i else hs

            def last(p):
                f_copy(i, p, 1).wait_recv()
                add(near(i), p, lambda s: fin[i, s] + f32(h[s]), yst.at[i], lambda v: v.astype(jnp.bfloat16))
                src = yst.at[i, rows(p)]
                for blk in range(4):
                    for half in range(split):
                        @pl.when(p == blk * split + half)
                        def _():
                            if i:
                                put(src, blk, half)
                            else:
                                y_copy(src, i, blk, half, ep_at(z_mid, c)).start()

            each(last)

    @on_end
    def _():
        for i in range(2):
            each(lambda p: [raw_send(i, core, p).wait_send() for core in range(2)])
            each(lambda p: prt_copy(near(i), p).wait_send())
        for blk in range(4):
            for half in range(split):
                y_copy(yst.at[0, rows(0)], 0, blk, half, ep_at(z_mid, c)).wait_send()

    @on_mid
    def _():
        send_h.wait_send()
        for i in range(2):
            each(lambda p: [prt_copy(far(i), p).wait_send(), prt_copy(near(i), p).wait_send(),
                            f_copy(i, p, 0).wait_send(), f_copy(i, p, 1).wait_send()])

    for blk in range(4):
        for half in range(-1, split):
            src = ya.at[blk] if half < 0 else yst.at[1, rows(0)]
            ref = y_out.at[blk, place(half)]
            came = rcopy(ref, ref, y_s.at[1, blk, half + 1], y_r.at[blk, half + 1], (blk, e))
            sent_here = True if half < 0 else end

            def kept():
                y_local(src, half).wait()

            def sent():
                y_copy(src, 1, blk, half, e).wait_send()

            pl.when((r == blk) & sent_here)(kept)
            pl.when((r != blk) & sent_here)(sent)
            pl.when((r != blk) | jnp.logical_not(sent_here))(came.wait_recv)


def back(part, h, ya):
    _, n, cols, _ = part.shape
    cut = ya.shape[1]
    seq = cut + n // 4
    piece = n // 8
    vmem = pl.BlockSpec(memory_space=pltpu.VMEM)
    hbm = pl.BlockSpec(memory_space=pl.ANY)
    dma = pltpu.SemaphoreType.DMA
    pieces = n // piece

    def tiles(*lead, dtype=jnp.bfloat16):
        return pltpu.VMEM(lead + (n, cols, LANES), dtype)

    return pl.pallas_call(
        functools.partial(back_kernel, cut, piece),
        out_shape=jax.ShapeDtypeStruct((4, seq, cols, LANES), jnp.bfloat16),
        in_specs=[hbm, vmem, hbm],
        out_specs=hbm,
        scratch_shapes=[
            tiles(4), tiles(4), tiles(2, 2), tiles(2, dtype=jnp.float32), tiles(4, dtype=jnp.float32), tiles(), tiles(2),
            *([dma((2, 2, pieces))] * 2), *([dma((4, pieces))] * 2), dma((4, pieces)), dma((2, pieces)),
            dma, dma, dma((2, 4, 3)), dma((4, 3)), dma((4,)), dma((3,)),
        ],
        compiler_params=pltpu.CompilerParams(collective_id=1, has_side_effects=True, vmem_limit_bytes=58 * 1024 * 1024),
    )(part, h, ya)


def block_plan(ids, me, ne):
    _, nseq, _, n = ids.shape
    le = ids - me * ne
    local = (le >= 0) & (le < ne)
    total = ids.size
    slot = lax.iota(jnp.int32, total).reshape(ids.shape)
    token = (lax.broadcasted_iota(jnp.int32, ids.shape, 0) * nseq + lax.broadcasted_iota(jnp.int32, ids.shape, 1)) * n
    token = token + lax.broadcasted_iota(jnp.int32, ids.shape, 3)
    key = (le << (SLOT_BITS + TOKEN_BITS)) | (token << SLOT_BITS) | slot
    none = jnp.iinfo(jnp.int32).max
    keys = lax.sort(jnp.where(local, key, none).reshape(-1), is_stable=False)
    experts = jnp.arange(ne, dtype=jnp.int32)
    counts = jnp.sum((le.reshape(-1)[None, :] == experts[:, None]).astype(jnp.int32), axis=1)
    low = (experts[None, :] < experts[:, None])
    first = jnp.sum(jnp.where(low, counts[None, :], 0), axis=1)
    nb = jnp.maximum((counts + BM - 1) // BM, 1)
    bfirst = jnp.sum(jnp.where(low, nb[None, :], 0), axis=1)
    maxb = total // BM + ne + 2
    b = jnp.arange(maxb, dtype=jnp.int32)
    inside = (b[:, None] >= bfirst[None, :]) & (b[:, None] < (bfirst + nb)[None, :])

    def of(v):
        return jnp.sum(jnp.where(inside, v[None, :], 0), axis=1)

    done = (b - of(bfirst)) * BM
    be, bb = of(experts), of(first) + done
    bn = jnp.clip(of(counts) - done, 0, BM)
    bb = jnp.where(jnp.any(inside, axis=1), bb, 0)
    keys = jnp.concatenate([jnp.where(keys == none, 0, keys), jnp.zeros((BM,), jnp.int32)])
    return jnp.sum(nb).reshape(1), be, bb, bn, keys


def solution(mesh):
    nd = mesh.shape['ep']
    tok = P(('replica', 'ep'), None, None)
    rows_ep = P('ep', None)
    by_expert = P('ep', None, None)
    cut = CUT

    def local(x, wq, wk, wv, wo, wr, w1, w3, w2, idx):
        b, s, d = x.shape
        k, ne = idx.shape[-1], w1.shape[0]
        me = lax.axis_index('ep')
        cols = d // LANES
        ua, ub, ha, hb, ids = attention(x, idx.transpose(0, 2, 1), wr, wq, wk, wv, wo, cut)

        def experts(u, gates, plan, lo, hi):
            n = b * (hi - lo)
            return moe(*plan, gates[..., lo:hi].reshape(-1), u, n, w1, w3, w2).reshape(nd, n, cols, LANES)

        plan_a, plan_b = block_plan(ids[..., :cut], me, ne), block_plan(ids[..., cut:], me, ne)
        u_all = lax.all_gather(ua, 'ep', axis=0, tiled=False)
        u_all, plan_b = lax.optimization_barrier((u_all, plan_b))
        terms = u_all[:, b * cut:].reshape(nd, 3, b, k, s).astype(jnp.float32)
        gates = terms[:, 0] + terms[:, 1] + terms[:, 2]
        part_a = experts(u_all, gates, plan_a, 0, cut)
        ub_all = lax.all_gather(ub, 'ep', axis=0, tiled=False)
        part_a, ub_all = lax.optimization_barrier((part_a, ub_all))
        part_a = lax.all_to_all(part_a, 'ep', 0, 0, tiled=True)
        part_b = experts(ub_all, gates, plan_b, cut, s)
        ya = ha.astype(jnp.float32) + jnp.sum(part_a.astype(jnp.float32), axis=0)
        y = back(part_b, hb, ya.astype(jnp.bfloat16).reshape(b, cut, cols, LANES))
        return y.reshape(b, s, d)

    return jax.shard_map(local, mesh=mesh,
                         in_specs=(tok, rows_ep, rows_ep, rows_ep, rows_ep, P(None, None),
                                   by_expert, by_expert, by_expert, tok),
                         out_specs=tok, check_vma=False)
```

```python
import functools
import jax
import jax.numpy as jnp
from jax import lax
from jax.experimental import pallas as pl
from jax.experimental.pallas import tpu as pltpu
from jax.sharding import PartitionSpec as P

HEAD = 128
EPS = 1e-6
THETA = 10000.0
BM = 128
PITCH = BM + 1
LANES = 128
CORES = 2
REPLICAS = 4
CUT = 56
RET = 32
STEPS = 8
SLOT_BITS, TOKEN_BITS = 15, 12


def loop(n, fn):
    def step(i, carry):
        fn(i)
        return carry

    lax.fori_loop(0, n, step, 0)


def kept(fn, v, axis=-1):
    return fn(v, axis=axis, keepdims=True)


def ep_at(z, c):
    return 2 * z + c


MESH_ID = pl.DeviceIdType.MESH


def rcopy(src, dst, ssem, rsem, dev):
    return pltpu.make_async_remote_copy(src_ref=src, dst_ref=dst, send_sem=ssem, recv_sem=rsem, device_id=dev,
                                        device_id_type=MESH_ID)


def meet(peers, count):
    barrier = pltpu.get_barrier_semaphore()
    for guard, dev in peers:
        def greet():
            pl.semaphore_signal(barrier, device_id=dev, device_id_type=MESH_ID)

        if guard is None:
            greet()
        else:
            pl.when(guard)(greet)
    pl.semaphore_wait(barrier, count)


def attn_kernel(cut, ret, x_hbm, idt_hbm, cos_ref, sin_ref, wr_ref, wq_ref, wk_ref, wv_ref, wo_ref,
                ua_ref, ub_ref, ha_ref, hb_ref, ids_out, gw, go,
                xg, a_ref, acc, wbuf, obuf, tm, gates, idv, zr, zp, zm, xr, yr, xs, ys, xd, yd, dr, pr, ps,
                x_s, x_r, i_s, i_r, j_s, j_r, lsem, csem):
    r, e = lax.axis_index('replica'), lax.axis_index('ep')
    nz, nq = 4, 4
    z, c = e // 2, e % 2
    e_p = ep_at(z, 1 - c)
    x, y = r // 2, r % 2
    r_x, r_y = (r + 2) % nq, r + 1 - 2 * y

    def line_quarter(x, y):
        return 2 - y + x * (4 * y - 2)

    mine = line_quarter(x, y)
    q_line = (mine, line_quarter(1 - x, y), line_quarter(x, 1 - y), line_quarter(1 - x, 1 - y))
    to_x, to_y = 2 + x, y
    q_pair = (mine, 3 - x, 1 - y, to_x + to_y - mine)

    def pairs(w, k):
        return w == 0 and k == 0

    def quarters(w, k):
        return q_pair if pairs(w, k) else q_line

    nd = ids_out.shape[0]
    rows, wide = wq_ref.shape[0], wq_ref.shape[1] // STEPS
    quarter = rows // nq
    orows = go.shape[0] // STEPS
    nseq, seq, d = x_hbm.shape
    partner, x_dev, y_dev = (r, e_p), (r_x, e), (r_y, e)
    per = STEPS // nd

    def mod(v, m):
        return lax.rem(v, m)

    others = [mod(r + i, nq) for i in range(1, nq)]
    mates = [mod(e + i, nd) for i in range(1, nd)]
    meet([(None, (q, e)) for q in others] + [(None, (r, f)) for f in mates], len(others) + len(mates))

    for i, q in enumerate(others):
        rcopy(idt_hbm.at[q], ids_out.at[e, r], i_s.at[i], i_r.at[r], (q, e)).start()
        rcopy(x_hbm.at[q], xg.at[r], x_s.at[i], x_r.at[r], (q, e)).start()
    keep_ids = pltpu.make_async_copy(idt_hbm.at[r], ids_out.at[e, r], csem.at[0])
    keep_x = pltpu.make_async_copy(x_hbm.at[r], xg.at[r], csem.at[1])
    keep_ids.start()
    keep_x.start()

    def spread_ids():
        keep_ids.wait()
        for i, q in enumerate(others):
            rcopy(idt_hbm.at[q], ids_out.at[e, q], i_s.at[i], i_r.at[q], (q, e)).wait_recv()
        for i, f in enumerate(mates):
            rcopy(ids_out.at[e], ids_out.at[e], j_s.at[i], j_r.at[e], (r, f)).start()

    def prepare():
        keep_x.wait()
        for i, q in enumerate(others):
            rcopy(x_hbm.at[q], xg.at[q], x_s.at[i], x_r.at[q], (q, e)).wait_recv()

        def norm(b):
            x = xg[b].astype(jnp.float32)
            at = pl.ds(b * seq, seq)
            a_ref[at, :] = (x * lax.rsqrt(kept(jnp.mean, x * x) + EPS)).astype(jnp.bfloat16)
            acc[at, :] = x

        loop(nseq, norm)

    def piece(w, s, f, q):
        if w:
            return go.at[pl.ds(s * orows + q * (orows // nq), orows // nq), :]
        return gw.at[s, :, pl.ds(f * rows + q * quarter, quarter), :]

    def half(w, s, zs, q, i):
        if w:
            n = orows // nq // 2
            return go.at[pl.ds(s * orows + (2 * q + i) * n, n), :]
        n = quarter // 2
        return gw.at[s, :, pl.ds(ep_at(zs, c) * rows + (2 * q + i) * n, n), :]

    def own_wo(s, lo, n):
        return wo_ref.at[pl.ds(mod(s, per) * orows + lo, n), :]

    def z_send(w, s, zs, up, second=0):
        ref = piece(w, s, ep_at(zs, c), q_pair[3] if second else mine)
        i = 2 if second else w
        return rcopy(ref, ref, (zp if up else zm).at[i, s, zs], zr.at[i, s, zs], (r, e + 2) if up else (r, e - 2))

    def xy_send(w, s, zs, q, ssem, rsem, dev):
        ref = piece(w, s, ep_at(zs, c), q)
        return rcopy(ref, ref, ssem.at[w, s, zs], rsem.at[w, s, zs], dev)

    def xd_send(w, s, zs, q):
        ref = half(w, s, zs, q, 1)
        return rcopy(ref, ref, xd.at[w, s, zs], dr.at[1, w, s, zs], x_dev)

    def yd_send(w, s, zs, q):
        ref = half(w, s, zs, q, 0)
        return rcopy(ref, ref, yd.at[w, s, zs], dr.at[0, w, s, zs], y_dev)

    def p_copy(w, s, zs, k, j, core):
        ref = piece(w, s, ep_at(zs, core), quarters(w, k)[j])
        return rcopy(ref, ref, ps.at[w, s, zs, j], pr.at[w, s, zs, j], partner)

    def p_whole(w, s, f):
        ref = go.at[pl.ds(s * orows, orows), :] if w else gw.at[s, :, pl.ds(f * rows, rows), :]
        return rcopy(ref, ref, ps.at[w, s, z, 0], pr.at[w, s, z, 0], partner)

    def own_parts(s):
        return [(w.at[:, pl.ds(s * wide, wide)], m) for m, w in enumerate((wq_ref, wk_ref, wv_ref))]

    def if_wo(s, f, *fns):
        @pl.when(s // per == f)
        def _():
            for fn in fns:
                fn()

    def each_line(fn):
        pl.when(z > 0)(lambda: fn(False))
        pl.when(z < nz - 1)(lambda: fn(True))

    def each_side(k, fn):
        pl.when(z - k - 1 >= 0)(lambda: fn(z - k - 1, True))
        pl.when(z + k + 1 < nz)(lambda: fn(z + k + 1, False))

    def originate(s):
        def line(up):
            sem = zp if up else zm
            dev = (r, e + 2) if up else (r, e - 2)
            for i, q in ((0, mine), (2, q_pair[3])):
                for w, m in own_parts(s):
                    rcopy(w.at[pl.ds(q * quarter, quarter), :], gw.at[s, m, pl.ds(e * rows + q * quarter, quarter), :],
                          sem.at[i, s, z], zr.at[i, s, z], dev).start()
            if_wo(s, e, lambda: rcopy(own_wo(s, mine * (orows // nq), orows // nq), piece(1, s, e, mine), sem.at[1, s, z],
                                      zr.at[1, s, z], dev).start())

        each_line(line)
        for w, m in own_parts(s):
            rcopy(w, gw.at[s, m, pl.ds(e * rows, rows), :], ps.at[0, s, z, 0], pr.at[0, s, z, 0], partner).start()
        if_wo(s, e, lambda: rcopy(own_wo(s, 0, orows), go.at[pl.ds(s * orows, orows), :], ps.at[1, s, z, 0],
                                  pr.at[1, s, z, 0], partner).start())

    def for_both(s, f, fn):
        fn(0)
        if_wo(s, f, lambda: fn(1))

    def along_z(s, k):
        def side(zs, up):
            def one(w):
                z_send(w, s, zs, up).wait_recv()
                pl.when(z < nz - 1 if up else z > 0)(lambda: z_send(w, s, zs, up).start())
                if pairs(w, k):
                    z_send(w, s, zs, up, 1).wait_recv()
                    p_copy(w, s, zs, k, 3, c).start()
                xy_send(w, s, zs, to_x if pairs(w, k) else mine, xs, xr, x_dev).start()
                xy_send(w, s, zs, to_y if pairs(w, k) else mine, ys, yr, y_dev).start()
                p_copy(w, s, zs, k, 0, c).start()

            for_both(s, ep_at(zs, c), one)

        each_side(k, side)

    def across(s, k):
        def side(zs, up):
            def one(w):
                q = quarters(w, k)
                xy_send(w, s, zs, q[1], xs, xr, x_dev).wait_recv()
                if not pairs(w, k):
                    yd_send(w, s, zs, q[1]).start()
                p_copy(w, s, zs, k, 1, c).start()
                xy_send(w, s, zs, q[2], ys, yr, y_dev).wait_recv()
                if not pairs(w, k):
                    xd_send(w, s, zs, q[2]).start()
                p_copy(w, s, zs, k, 2, c).start()

            for_both(s, ep_at(zs, c), one)

        each_side(k, side)

    def diagonal(s, k):
        def side(zs, up):
            def one(w):
                if not pairs(w, k):
                    xd_send(w, s, zs, q_line[3]).wait_recv()
                    yd_send(w, s, zs, q_line[3]).wait_recv()
                    p_copy(w, s, zs, k, 3, c).start()

            for_both(s, ep_at(zs, c), one)

        each_side(k, side)

    def load(s, f):
        slot = mod(s, 2)
        return pltpu.make_async_copy(gw.at[s, :, pl.ds(f * rows, rows), :], wbuf.at[slot, :, pl.ds(f * rows, rows), :],
                                     lsem.at[slot, f])

    def oload(s, src):
        slot = mod(s, 2)
        return pltpu.make_async_copy(src, obuf.at[slot], lsem.at[slot, nd])

    def collect(s):
        slot = mod(s, 2)
        whole = go.at[pl.ds(s * orows, orows), :]

        def side(k, zs):
            def one(w):
                for j in range(nq):
                    p_copy(w, s, zs, k, j, 1 - c).wait_recv()

            for_both(s, ep_at(zs, 1 - c), one)

        for k in range(nz - 1):
            each_side(k, lambda zs, up: side(k, zs))
        p_whole(0, s, e_p).wait_recv()
        if_wo(s, e_p, lambda: p_whole(1, s, e_p).wait_recv())

        for f in range(nd):
            def near():
                for w, m in own_parts(s):
                    pltpu.make_async_copy(w, wbuf.at[slot, m, pl.ds(f * rows, rows), :], lsem.at[slot, f]).start()

            pl.when(f == e)(near)
            pl.when(f != e)(lambda: load(s, f).start())
        if_wo(s, e, lambda: oload(s, own_wo(s, 0, orows)).start())
        pl.when(s // per != e)(lambda: oload(s, whole).start())

    def wait_loads(s):
        for f in range(nd):
            load(s, f).wait()
        oload(s, go.at[pl.ds(s * orows, orows), :]).wait()

    pair = 2 * HEAD
    npair = wide // pair

    def compute(s, j):
        slot = mod(s, 2)
        a = a_ref[...]
        cols = slice(j * pair, (j + 1) * pair)
        cos, sin = cos_ref[...], sin_ref[...]

        def rot(v):
            return (v * cos + pltpu.roll(v, HEAD // 2, 1) * sin).astype(jnp.bfloat16)

        q, k, v = [jnp.dot(a, wbuf[slot, m, :, cols], preferred_element_type=jnp.float32) for m in range(3)]
        v = v.astype(jnp.bfloat16)
        tri = lax.broadcasted_iota(jnp.int32, (seq, seq), 0) >= lax.broadcasted_iota(jnp.int32, (seq, seq), 1)
        heads = []
        for hh in range(CORES):
            hc = slice(hh * HEAD, (hh + 1) * HEAD)
            outs = []
            for b in range(nseq):
                rs = slice(b * seq, (b + 1) * seq)
                sc = lax.dot_general(rot(q[rs, hc]), rot(k[rs, hc]), (((1,), (1,)), ((), ())),
                                     preferred_element_type=jnp.float32)
                sc = jnp.where(tri, sc * HEAD ** -0.5, -jnp.inf)
                ex = jnp.exp(sc - kept(jnp.max, sc))
                p = (ex / kept(jnp.sum, ex)).astype(jnp.bfloat16)
                outs.append(jnp.dot(p, v[rs, hc], preferred_element_type=jnp.float32).astype(jnp.bfloat16))
            heads.append(jnp.concatenate(outs, axis=0))
        o = jnp.concatenate(heads, axis=1)
        acc[...] += jnp.dot(o, obuf[slot, cols, :], preferred_element_type=jnp.float32)

    def within(s, fn, *args):
        pl.when((s >= 0) & (s < STEPS))(lambda: fn(s, *args))

    originate(0)

    def turn(i):
        within(i + 1, originate)
        within(i - 3, wait_loads)
        for k in range(nz - 1):
            within(i - 2, diagonal, k)
            within(i - 1, across, k)
            within(i, along_z, k)
            if k < npair:
                within(i - 3, compute, k)
        within(i - 2, collect)
        pl.when(i == 1)(spread_ids)
        pl.when(i == 2)(prepare)

    loop(STEPS + 3, turn)

    keep_own = pltpu.make_async_copy(ids_out.at[e], idv, csem.at[0])
    keep_own.start()
    keep_own.wait()
    pitch = d // LANES + 1
    tile = pl.ds(0, d // LANES)

    def spill(v, *parts):
        for k in range(d // LANES):
            tm[pl.ds(k, seq, stride=pitch), :] = v[:, k * LANES:(k + 1) * LANES]

        def rows_to(ref, base, lo):
            def some(g):
                for i in range(8):
                    j = g * 8 + i
                    ref[base + j] = tm[pl.ds((lo + j) * pitch, d // LANES), :].astype(jnp.bfloat16)

            return some

        for ref, base, lo, hi in parts:
            loop((hi - lo) // 8, rows_to(ref, base, lo))

    def route(b):
        h = acc[pl.ds(b * seq, seq), :].astype(jnp.bfloat16).astype(jnp.float32)
        n = h * lax.rsqrt(kept(jnp.mean, h * h) + EPS)
        logits = jnp.dot(n, wr_ref[...], precision=lax.Precision.HIGHEST, preferred_element_type=jnp.float32).T
        expert = lax.broadcasted_iota(jnp.int32, logits.shape, 0)
        ids = idv[b]
        picked = jnp.concatenate([jnp.sum(jnp.where(expert == ids[k:k + 1, :], logits, 0.0), axis=0, keepdims=True)
                                  for k in range(ids.shape[0])], axis=0)
        ex = jnp.exp(picked - kept(jnp.max, picked, 0))
        gates[b] = ex / kept(jnp.sum, ex, 0)
        rest, tail = seq - cut, cut - ret
        spill(n, (ua_ref, b * cut, 0, cut), (ub_ref, b * rest, cut, seq))
        spill(h, (ha_ref, b * ret, 0, ret), (hb_ref, b * tail, ret, cut), (hb_ref, nseq * tail + b * rest, cut, seq))

    loop(nseq, route)
    left = gates[...].reshape(-1, LANES)
    per_tile = d // LANES
    for term in range(3):
        g = left.astype(jnp.bfloat16)
        left = left - g.astype(jnp.float32)
        for i in range(g.shape[0] // per_tile):
            ua_ref[nseq * cut + term * (g.shape[0] // per_tile) + i] = g[i * per_tile:(i + 1) * per_tile, :]

    for i, f in enumerate(mates):
        rcopy(ids_out.at[e], ids_out.at[f], j_s.at[i], j_r.at[f], (r, f)).wait()
    for i, q in enumerate(others):
        rcopy(idt_hbm.at[q], ids_out.at[e, r], i_s.at[i], i_r.at[r], (q, e)).wait_send()
        rcopy(x_hbm.at[q], xg.at[r], x_s.at[i], x_r.at[r], (q, e)).wait_send()

    def drain(s):
        def side(k, zs, up):
            def sent(w):
                pl.when(z < nz - 1 if up else z > 0)(lambda: z_send(w, s, zs, up).wait_send())
                for j in range(nq):
                    p_copy(w, s, zs, k, j, c).wait_send()
                xy_send(w, s, zs, mine, xs, xr, x_dev).wait_send()
                xy_send(w, s, zs, mine, ys, yr, y_dev).wait_send()
                if not pairs(w, k):
                    xd_send(w, s, zs, mine).wait_send()
                    yd_send(w, s, zs, mine).wait_send()

            for_both(s, ep_at(zs, c), sent)

        for k in range(nz - 1):
            each_side(k, lambda zs, up: side(k, zs, up))

        def own(w):
            each_line(lambda up: z_send(w, s, z, up).wait_send())
            p_whole(w, s, e).wait_send()

        for_both(s, e, own)
        each_line(lambda up: z_send(0, s, z, up, 1).wait_send())

    loop(STEPS, drain)


def attention(x, idt, wr, wq, wk, wv, wo, cut, ret):
    nseq, seq, d = x.shape
    rows, hd = wq.shape
    nd, k = d // rows, idt.shape[1]
    cols = d // LANES
    half = HEAD // 2
    freq = THETA ** (-jnp.arange(half, dtype=jnp.float32) / half)
    ang = jnp.arange(seq, dtype=jnp.float32)[:, None] * freq
    cos = jnp.concatenate([jnp.cos(ang)] * 2, axis=1)
    sin = jnp.concatenate([-jnp.sin(ang), jnp.sin(ang)], axis=1)
    vmem = pl.BlockSpec(memory_space=pltpu.VMEM)
    hbm = pl.BlockSpec(memory_space=pl.ANY)
    wide = hd // STEPS
    dma = pltpu.SemaphoreType.DMA
    bf = jnp.bfloat16

    def out(*shape, dtype=bf):
        return jax.ShapeDtypeStruct(shape, dtype)

    na, nb = nseq * cut, nseq * (seq - cut)
    return pl.pallas_call(
        functools.partial(attn_kernel, cut, ret),
        out_shape=(out(na + 3 * nseq * k // cols, cols, LANES), out(nb, cols, LANES),
                   out(nseq * ret, cols, LANES), out(nseq * (seq - ret), cols, LANES), out(nd, nseq, k, seq, dtype=jnp.int32), out(STEPS, 3, d, wide), out(hd, d)),
        in_specs=[hbm, hbm] + [vmem] * 3 + [hbm] * 4,
        out_specs=(vmem, vmem, vmem, vmem, hbm, hbm, hbm),
        scratch_shapes=[
            pltpu.VMEM((nseq, seq, d), bf), pltpu.VMEM((nseq * seq, d), bf), pltpu.VMEM((nseq * seq, d), jnp.float32),
            pltpu.VMEM((2, 3, d, wide), bf), pltpu.VMEM((2, hd // STEPS, d), bf),
            pltpu.VMEM((seq * (cols + 1), LANES), jnp.float32), pltpu.VMEM((nseq, k, seq), jnp.float32),
            pltpu.VMEM((nseq, k, seq), jnp.int32),
            *([dma((3, STEPS, 4))] * 3), *([dma((2, STEPS, 4))] * 6), dma((2, 2, STEPS, 4)), *([dma((2, STEPS, 4, 4))] * 2),
            *([dma((4,))] * 4), *([dma((nd,))] * 2), dma((2, nd + 1)), dma((2,)),
        ],
        compiler_params=pltpu.CompilerParams(collective_id=0, has_side_effects=True, vmem_limit_bytes=58 * 1024 * 1024),
        cost_estimate=pl.CostEstimate(flops=10 * nseq * seq * d * hd, bytes_accessed=8 * d * hd, transcendentals=0),
    )(x, idt, cos, sin, wr, wq, wk, wv, wo)[:5]


def token_of(key):
    return lax.shift_right_logical(key, SLOT_BITS) & ((1 << TOKEN_BITS) - 1)


def moe_kernel(nt, stores, given, nblk_ref, be_ref, bb_ref, bn_ref, key_ref, gate_ref, u_hbm, w1_hbm, w3_hbm, w2_hbm, *refs):
    outs, (ub, acc, w1, w3, w2, xs, zs, lhs, usem, wsem, osem) = refs[given:-11], refs[-11:]
    cols = ub.shape[1]
    nexp = w1_hbm.shape[0]
    nblk = nblk_ref[0]

    def weights(e, slot):
        return (pltpu.make_async_copy(w1_hbm.at[e], w1.at[slot], wsem.at[slot, 0]),
                pltpu.make_async_copy(w3_hbm.at[e], w3.at[slot], wsem.at[slot, 1]),
                pltpu.make_async_copy(w2_hbm.at[e], w2.at[slot], wsem.at[slot, 2]))

    nd = u_hbm.shape[0]
    n = nt // nd
    for dev in range(nd):
        pltpu.make_async_copy(u_hbm.at[dev, pl.ds(0, n)], ub.at[pl.ds(dev * n, n)], usem).start()

    for c in weights(0, 0):
        c.start()

    def zero(i):
        acc[pl.ds(i * 8, 8)] = jnp.zeros((8,) + acc.shape[1:], jnp.float32)

    loop(acc.shape[0] // 8, zero)
    pltpu.make_async_copy(ub.at[pl.ds(0, nt)], ub.at[pl.ds(0, nt)], usem).wait()

    def gather(b):
        base = bb_ref[b]
        for i in range(BM):
            t = token_of(key_ref[base + i])
            xs[pl.ds(i, cols, stride=PITCH), :] = ub[t].astype(jnp.float32)

    def scatter(base, n, rows):
        new = []
        for i in rows:
            key = key_ref[base + i]
            t = jnp.where(i < n, token_of(key), nt)
            new.append((t, acc[t] + gate_ref[key & ((1 << SLOT_BITS) - 1)] * zs[pl.ds(i, cols, stride=PITCH), :]))
        for t, v in new:
            acc[t] = v

    gather(0)

    def body(b, e_prev):
        e = be_ref[b]
        slot = e % 2

        @pl.when(e != e_prev)
        def _():
            @pl.when(e + 1 < nexp)
            def _():
                for c in weights(e + 1, 1 - slot):
                    c.start()

            for c in weights(e, slot):
                c.wait()

        for k in range(cols):
            lhs[:, k * LANES:(k + 1) * LANES] = xs[k * PITCH:k * PITCH + BM, :].astype(jnp.bfloat16)
        gather(b + 1)
        bp = jnp.maximum(b - 1, 0)
        base, n = bb_ref[bp], jnp.where(b > 0, bn_ref[bp], 0)
        for i in range(0, BM, 8):
            scatter(base, n, range(i, i + 8))
        x = lhs[...]
        a1 = jnp.dot(x, w1[slot], preferred_element_type=jnp.float32)
        a3 = jnp.dot(x, w3[slot], preferred_element_type=jnp.float32)
        act = (jax.nn.silu(a1) * a3).astype(jnp.bfloat16)
        z = jnp.dot(act, w2[slot], preferred_element_type=jnp.float32).astype(jnp.bfloat16).astype(jnp.float32)
        for k in range(cols):
            zs[k * PITCH:k * PITCH + BM, :] = z[:, k * LANES:(k + 1) * LANES]
        return e

    lax.fori_loop(0, nblk, body, -1)
    for i in range(0, BM, 8):
        scatter(bb_ref[nblk - 1], bn_ref[nblk - 1], range(i, i + 8))

    def pack(i):
        for j in range(8):
            t = i * 8 + j
            ub[t] = acc[t].astype(jnp.bfloat16)

    loop(nt // 8, pack)

    def store(i):
        dev, b = i // 4, lax.rem(i, 4)
        for out, lo, hi, base in stores:
            pltpu.make_async_copy(ub.at[pl.ds(i * (n // 4) + lo, hi - lo)],
                                  outs[out].at[dev, pl.ds(base + b * (hi - lo), hi - lo)], osem).start()

    loop(nd * 4, store)
    pltpu.make_async_copy(ub.at[pl.ds(0, nt)], ub.at[pl.ds(0, nt)], osem).wait()


def moe(nblk, be, bb, bn, keys, gates, u, n, w1, w3, w2, lengths, stores, *into):
    nd, _, cols, _ = u.shape
    nt = nd * n
    ne, d, f = w1.shape
    smem = pl.BlockSpec(memory_space=pltpu.SMEM)
    hbm = pl.BlockSpec(memory_space=pl.ANY)
    return pl.pallas_call(
        functools.partial(moe_kernel, nt, stores, len(into)),
        out_shape=[jax.ShapeDtypeStruct((nd, m, cols, LANES), jnp.bfloat16) for m in lengths],
        in_specs=[smem] * 6 + [hbm] * (4 + len(into)),
        out_specs=[hbm] * len(lengths),
        input_output_aliases={10 + i: i for i in range(len(into))},
        scratch_shapes=[
            pltpu.VMEM((nt + 8, cols, LANES), jnp.bfloat16),
            pltpu.VMEM((nt + 8, cols, LANES), jnp.float32),
            pltpu.VMEM((2, d, f), jnp.bfloat16),
            pltpu.VMEM((2, d, f), jnp.bfloat16),
            pltpu.VMEM((2, f, d), jnp.bfloat16),
            pltpu.VMEM((cols * PITCH, LANES), jnp.float32),
            pltpu.VMEM((cols * PITCH, LANES), jnp.float32),
            pltpu.VMEM((BM, d), jnp.bfloat16),
            pltpu.SemaphoreType.DMA,
            pltpu.SemaphoreType.DMA((2, 3)),
            pltpu.SemaphoreType.DMA,
        ],
        compiler_params=pltpu.CompilerParams(vmem_limit_bytes=60 * 1024 * 1024),
        cost_estimate=pl.CostEstimate(flops=6 * 5000 * d * f, bytes_accessed=ne * 3 * d * f * 2, transcendentals=0),
    )(nblk, be, bb, bn, keys, gates, u, w1, w3, w2, *into)


def back_kernel(ret, piece, part, h_ref, h_mid, raw_here, raw_cross, ya, y_out, own, prt, raw, fin, fout, hs, yst, raw_s, raw_r,
                prt_s, prt_r, f_s, f_r, y_s, y_r, osem, lsem, csem):
    r, e = lax.axis_index('replica'), lax.axis_index('ep')
    z, c = e // 2, e % 2
    n = h_ref.shape[0]
    pieces = n // piece
    split = pieces // 4
    early = 4
    mid = (z + 2) // 3 + (5 - z) // 3 - 1
    low = z // 2
    on_mid, on_end = pl.when(mid == 1), pl.when(mid == 0)
    z_mid, z_end = 1 + low, 3 * low
    partner, across = (r, ep_at(z, 1 - c)), (r, ep_at(2 - low, c))
    to_end = (r, ep_at(z_end, c))
    others = [lax.rem(r + i, 4) for i in range(1, 4)]

    def far(i):
        return 2 + i + low * (-1 - 2 * i)

    def near(i):
        return 1 - i + low * (1 + 2 * i)

    def rows(p):
        return pl.ds(p * piece, piece)

    end, inner = mid == 0, mid == 1
    meet([(None, (q, e)) for q in others] + [(None, partner)] +
         [(end, (q, ep_at(z_mid, c))) for q in range(REPLICAS)] + [(end, (r, ep_at(z_mid, 1 - c)))] +
         [(inner, (q, ep_at(z_end, c))) for q in range(REPLICAS)] + [(inner, (r, ep_at(z_end, 1 - c))), (inner, across)], 9 + mid)

    def raw_send(i, core, p):
        return rcopy(part.at[ep_at(far(i), core), rows(p)], raw.at[i, c, rows(p)], raw_s.at[i, core, p], raw_r.at[i, c, p],
                     (r, ep_at(z_mid, core)))

    def raw_recv(i, core, p):
        ref = raw.at[i, core, rows(p)]
        return rcopy(ref, ref, raw_s.at[i, core, p], raw_r.at[i, core, p], (r, ep_at(z_end, core)))

    def prt_copy(chip, p):
        return rcopy(part.at[ep_at(chip, 1 - c), rows(p)], prt.at[chip, rows(p)], prt_s.at[chip, p], prt_r.at[chip, p], partner)

    def f_copy(i, p, onward):
        return rcopy(fout.at[2 * onward + i, rows(p)], fin.at[i, rows(p)], f_s.at[2 * onward + i, p], f_r.at[i, p],
                     to_end if onward else across)

    def load(chip):
        return pltpu.make_async_copy(part.at[ep_at(chip, c)], own.at[chip], osem.at[chip])

    def landed(i):
        j = i + low * (1 - 2 * i)
        rest = pl.ds(0, early * piece)
        return (pltpu.make_async_copy(raw_here.at[j], raw.at[i, c, rest], csem.at[i, 0]),
                pltpu.make_async_copy(raw_cross.at[j], raw.at[i, 1 - c, rest], csem.at[i, 1]))

    keep_h = pltpu.make_async_copy(h_mid, hs, csem.at[0, 0])

    def place(half):
        return pl.ds(0, ret) if half < 0 else pl.ds(ret + half * piece, piece)

    def y_copy(src, i, blk, half, f):
        return rcopy(src, y_out.at[r, place(half)], y_s.at[i, blk, half + 1], y_r.at[r, half + 1], (blk, f))

    def y_local(src, half):
        return pltpu.make_async_copy(src, y_out.at[r, place(half)], lsem.at[half + 1])

    def put(src, blk, half):
        pl.when(r == blk)(lambda: y_local(src, half).start())
        pl.when(r != blk)(lambda: y_copy(src, 1, blk, half, e).start())

    def each(fn, count=pieces):
        loop(count, fn)

    for i in range(CORES):
        load(near(i)).start()

    @on_end
    def _():
        keep_h.start()
        for i in range(CORES):
            each(lambda p: [raw_send(i, core, p + early).start() for core in range(CORES)], pieces - early)
            each(lambda p: prt_copy(near(i), p).start())

    @on_mid
    def _():
        for i in range(CORES):
            for copy in landed(i):
                copy.start()
            load(far(i)).start()
            each(lambda p: [prt_copy(far(i), p).start(), prt_copy(near(i), p).start()])

    for blk in range(REPLICAS):
        put(ya.at[blk], blk, -1)

    def f32(v):
        return v.astype(jnp.float32)

    def add(chip, p, incoming, out, finish=f32):
        prt_copy(chip, p).wait_recv()

        def some(j):
            s = pl.ds(p * piece + j * 4, 4)
            out[s] = finish(f32(own[chip, s]) + f32(prt[chip, s]) + incoming(s))

        each(some, piece // 4)

    @on_mid
    def _():
        for i in range(CORES):
            load(far(i)).wait()
            load(near(i)).wait()
            for copy in landed(i):
                copy.wait()

        def first(q):
            i, p = q // pieces, lax.rem(q, pieces)
            pl.when(p >= early)(lambda: [raw_recv(i, core, p).wait_recv() for core in range(CORES)][0])
            add(far(i), p, lambda s: f32(raw[i, 0, s]) + f32(raw[i, 1, s]), fout.at[i])
            f_copy(i, p, 0).start()

        def second(q):
            i, p = q // pieces, lax.rem(q, pieces)
            f_copy(i, p, 0).wait_recv()
            add(near(i), p, lambda s: fin[i, s], fout.at[2 + i])
            f_copy(i, p, 1).start()

        lag = 2

        def step(q):
            pl.when(q < 2 * pieces)(lambda: first(q))
            pl.when(q >= lag)(lambda: second(q - lag))

        each(step, 2 * pieces + lag)

    @on_end
    def _():
        for i in range(CORES):
            load(near(i)).wait()
            if i == 0:
                keep_h.wait()
            h = h_ref if i else hs

            def last(p):
                f_copy(i, p, 1).wait_recv()
                add(near(i), p, lambda s: fin[i, s] + f32(h[s]), yst.at[i], lambda v: v.astype(jnp.bfloat16))
                src = yst.at[i, rows(p)]
                for blk in range(REPLICAS):
                    for half in range(split):
                        @pl.when(p == (early + blk * (split - 1) + half - 1 if half else blk))
                        def _():
                            if i:
                                put(src, blk, half)
                            else:
                                y_copy(src, i, blk, half, ep_at(z_mid, c)).start()

            each(last)

    @on_end
    def _():
        for i in range(CORES):
            each(lambda p: [raw_send(i, core, p + early).wait_send() for core in range(CORES)], pieces - early)
            each(lambda p: prt_copy(near(i), p).wait_send())
        for blk in range(REPLICAS):
            for half in range(split):
                y_copy(yst.at[0, rows(0)], 0, blk, half, ep_at(z_mid, c)).wait_send()

    @on_mid
    def _():
        for i in range(CORES):
            each(lambda p: [prt_copy(far(i), p).wait_send(), prt_copy(near(i), p).wait_send(),
                            f_copy(i, p, 0).wait_send(), f_copy(i, p, 1).wait_send()])

    for blk in range(REPLICAS):
        for half in range(-1, split):
            src = ya.at[blk] if half < 0 else yst.at[1, rows(0)]
            ref = y_out.at[blk, place(half)]
            came = rcopy(ref, ref, y_s.at[1, blk, half + 1], y_r.at[blk, half + 1], (blk, e))
            sent_here = True if half < 0 else end

            def stayed():
                y_local(src, half).wait()

            def sent():
                y_copy(src, 1, blk, half, e).wait_send()

            pl.when((r == blk) & sent_here)(stayed)
            pl.when((r != blk) & sent_here)(sent)
            pl.when((r != blk) | jnp.logical_not(sent_here))(came.wait_recv)


def back(part, h, h_mid, raw_here, raw_cross, ya):
    _, n, cols, _ = part.shape
    ret = ya.shape[1]
    seq = ret + n // 4
    piece = raw_here.shape[1] // 4
    vmem = pl.BlockSpec(memory_space=pltpu.VMEM)
    hbm = pl.BlockSpec(memory_space=pl.ANY)
    dma = pltpu.SemaphoreType.DMA
    pieces = n // piece
    split = pieces // 4

    def tiles(*lead, dtype=jnp.bfloat16):
        return pltpu.VMEM(lead + (n, cols, LANES), dtype)

    return pl.pallas_call(
        functools.partial(back_kernel, ret, piece),
        out_shape=jax.ShapeDtypeStruct((4, seq, cols, LANES), jnp.bfloat16),
        in_specs=[hbm, vmem] + [hbm] * 4,
        out_specs=hbm,
        scratch_shapes=[
            tiles(4), tiles(4), tiles(2, 2), tiles(2, dtype=jnp.float32), tiles(4, dtype=jnp.float32), tiles(), tiles(2),
            *([dma((2, 2, pieces))] * 2), *([dma((4, pieces))] * 2), dma((4, pieces)), dma((2, pieces)),
            dma((2, 4, split + 1)), dma((4, split + 1)), dma((4,)), dma((split + 1,)), dma((2, 2)),
        ],
        compiler_params=pltpu.CompilerParams(collective_id=1, has_side_effects=True, vmem_limit_bytes=58 * 1024 * 1024),
    )(part, h, h_mid, raw_here, raw_cross, ya)


def block_plan(ids, me, ne):
    _, nseq, _, n = ids.shape
    le = ids - me * ne
    local = (le >= 0) & (le < ne)
    total = ids.size
    slot = lax.iota(jnp.int32, total).reshape(ids.shape)
    token = (lax.broadcasted_iota(jnp.int32, ids.shape, 0) * nseq + lax.broadcasted_iota(jnp.int32, ids.shape, 1)) * n
    token = token + lax.broadcasted_iota(jnp.int32, ids.shape, 3)
    key = (le << (SLOT_BITS + TOKEN_BITS)) | (token << SLOT_BITS) | slot
    none = jnp.iinfo(jnp.int32).max
    keys = lax.sort(jnp.where(local, key, none).reshape(-1), is_stable=False)
    experts = jnp.arange(ne, dtype=jnp.int32)
    counts = jnp.sum((le.reshape(-1)[None, :] == experts[:, None]).astype(jnp.int32), axis=1)
    low = (experts[None, :] < experts[:, None])
    first = jnp.sum(jnp.where(low, counts[None, :], 0), axis=1)
    nb = jnp.maximum((counts + BM - 1) // BM, 1)
    bfirst = jnp.sum(jnp.where(low, nb[None, :], 0), axis=1)
    maxb = total // BM + ne + 2
    b = jnp.arange(maxb, dtype=jnp.int32)
    inside = (b[:, None] >= bfirst[None, :]) & (b[:, None] < (bfirst + nb)[None, :])

    def of(v):
        return jnp.sum(jnp.where(inside, v[None, :], 0), axis=1)

    done = (b - of(bfirst)) * BM
    be, bb = of(experts), of(first) + done
    bn = jnp.clip(of(counts) - done, 0, BM)
    bb = jnp.where(jnp.any(inside, axis=1), bb, 0)
    keys = jnp.concatenate([jnp.where(keys == none, 0, keys), jnp.zeros((BM,), jnp.int32)])
    return jnp.sum(nb).reshape(1), be, bb, bn, keys


def solution(mesh):
    nd = mesh.shape['ep']
    tok = P(('replica', 'ep'), None, None)
    rows_ep = P('ep', None)
    by_expert = P('ep', None, None)
    cut, ret = CUT, RET

    def local(x, wq, wk, wv, wo, wr, w1, w3, w2, idx):
        b, s, d = x.shape
        k, ne = idx.shape[-1], w1.shape[0]
        me = lax.axis_index('ep')
        low, c = me // 4, me % 2
        cols = d // LANES
        tail, rest = cut - ret, s - cut
        ua, ub, ha, hb, ids = attention(x, idx.transpose(0, 2, 1), wr, wq, wk, wv, wo, cut, ret)
        plan_a, plan_b = block_plan(ids[..., :cut], me, ne), block_plan(ids[..., cut:], me, ne)
        u_all = lax.all_gather(ua, 'ep')
        u_all, plan_b = lax.optimization_barrier((u_all, plan_b))
        terms = u_all[:, b * cut:].reshape(nd, 3, b, k, s).astype(jnp.float32)
        gates = terms[:, 0] + terms[:, 1] + terms[:, 2]
        lengths = (b * ret, b * (tail + rest))
        part_a, part_b = moe(*plan_a, gates[..., :cut].reshape(-1), u_all, b * cut, w1, w3, w2, lengths,
                             ((0, 0, ret, 0), (1, ret, cut, 0)))
        ub_all = lax.all_gather(ub, 'ep')
        part_a, part_b, ub_all = lax.optimization_barrier((part_a, part_b, ub_all))
        far = lax.dynamic_index_in_dim(part_b.reshape(-1, nd // 4, CORES, b * (tail + rest), cols, LANES)[:, :, :, :b * tail], 1 - low, 0, False)
        here, cross = [lax.dynamic_index_in_dim(far, i, 1, False) for i in (c, 1 - c)]
        inward = [(0, 2), (1, 3), (6, 4), (7, 5)]
        here = lax.ppermute(here, 'ep', inward)
        cross = lax.ppermute(cross, 'ep', [(i, j ^ 1) for i, j in inward])
        h_mid = lax.ppermute(hb, 'ep', [(j, i) for i, j in inward])
        part_a = lax.all_to_all(part_a, 'ep', 0, 0, tiled=True)
        part_b, = moe(*plan_b, gates[..., cut:].reshape(-1), ub_all, b * rest, w1, w3, w2, lengths[1:],
                      ((0, 0, rest, b * tail),), part_b)
        ya = ha.astype(jnp.float32) + jnp.sum(part_a.astype(jnp.float32), axis=0)
        y = back(part_b, hb, h_mid, here, cross, ya.astype(jnp.bfloat16).reshape(b, ret, cols, LANES))
        return y.reshape(b, s, d)

    return jax.shard_map(local, mesh=mesh,
                         in_specs=(tok, rows_ep, rows_ep, rows_ep, rows_ep, P(None, None),
                                   by_expert, by_expert, by_expert, tok),
                         out_specs=tok, check_vma=False)
```

```python
import functools
import jax
import jax.numpy as jnp
from jax import lax
from jax.experimental import pallas as pl
from jax.experimental.pallas import tpu as pltpu
from jax.sharding import PartitionSpec as P

HEAD = 128
EPS = 1e-6
THETA = 10000.0
BM = 128
PITCH = BM + 1
LANES = 128
VMEM = 60 * 1024 * 1024
CORES = 2
REPLICAS = 4
CUT = 56
RET = 32
STEPS = 8
SLOT_BITS, TOKEN_BITS = 15, 12


def loop(n, fn):
    def step(i, carry):
        fn(i)
        return carry

    lax.fori_loop(0, n, step, 0)


def cost(flops, moved):
    return pl.CostEstimate(flops=flops, bytes_accessed=moved, transcendentals=0)


def kept(fn, v, axis=-1):
    return fn(v, axis=axis, keepdims=True)


def ep_at(z, c):
    return 2 * z + c


MESH_ID = pl.DeviceIdType.MESH


def rcopy(src, dst, ssem, rsem, dev):
    return pltpu.make_async_remote_copy(src_ref=src, dst_ref=dst, send_sem=ssem, recv_sem=rsem, device_id=dev,
                                        device_id_type=MESH_ID)


def meet(peers, count):
    barrier = pltpu.get_barrier_semaphore()
    for guard, dev in peers:
        def greet():
            pl.semaphore_signal(barrier, device_id=dev, device_id_type=MESH_ID)

        if guard is None:
            greet()
        else:
            pl.when(guard)(greet)
    pl.semaphore_wait(barrier, count)


def attn_kernel(cut, ret, x_hbm, idt_hbm, cos_ref, sin_ref, wr_ref, wq_ref, wk_ref, wv_ref, wo_ref,
                ua_ref, ub_ref, ha_ref, hb_ref, ids_out, gw, go,
                xg, a_ref, acc, wbuf, obuf, tm, gates, idv, zr, zp, zm, xr, yr, xs, ys, xd, yd, dr, pr, ps,
                x_s, x_r, i_s, i_r, j_s, j_r, lsem, csem):
    r, e = lax.axis_index('replica'), lax.axis_index('ep')
    nz, nq = 4, 4
    z, c = e // 2, e % 2
    e_p = ep_at(z, 1 - c)
    x, y = r // 2, r % 2
    r_x, r_y = (r + 2) % nq, r + 1 - 2 * y

    def line_quarter(x, y):
        return 2 - y + x * (4 * y - 2)

    mine = line_quarter(x, y)
    q_line = (mine, line_quarter(1 - x, y), line_quarter(x, 1 - y), line_quarter(1 - x, 1 - y))
    to_x, to_y = 2 + x, y
    q_pair = (mine, 3 - x, 1 - y, to_x + to_y - mine)

    def pairs(w, k):
        return w == 0 and k == 0

    def quarters(w, k):
        return q_pair if pairs(w, k) else q_line

    nd = ids_out.shape[0]
    rows, wide = wq_ref.shape[0], wq_ref.shape[1] // STEPS
    quarter = rows // nq
    orows = go.shape[0] // STEPS
    nseq, seq, d = x_hbm.shape
    partner, x_dev, y_dev = (r, e_p), (r_x, e), (r_y, e)
    per = STEPS // nd

    def mod(v, m):
        return lax.rem(v, m)

    others = [mod(r + i, nq) for i in range(1, nq)]
    mates = [mod(e + i, nd) for i in range(1, nd)]
    meet([(None, (q, e)) for q in others] + [(None, (r, f)) for f in mates], len(others) + len(mates))

    for i, q in enumerate(others):
        rcopy(idt_hbm.at[q], ids_out.at[e, r], i_s.at[i], i_r.at[r], (q, e)).start()
        rcopy(x_hbm.at[q], xg.at[r], x_s.at[i], x_r.at[r], (q, e)).start()
    keep_ids = pltpu.make_async_copy(idt_hbm.at[r], ids_out.at[e, r], csem.at[0])
    keep_x = pltpu.make_async_copy(x_hbm.at[r], xg.at[r], csem.at[1])
    keep_ids.start()
    keep_x.start()

    def spread_ids():
        keep_ids.wait()
        for i, q in enumerate(others):
            rcopy(idt_hbm.at[q], ids_out.at[e, q], i_s.at[i], i_r.at[q], (q, e)).wait_recv()
        for i, f in enumerate(mates):
            rcopy(ids_out.at[e], ids_out.at[e], j_s.at[i], j_r.at[e], (r, f)).start()

    def prepare():
        keep_x.wait()
        for i, q in enumerate(others):
            rcopy(x_hbm.at[q], xg.at[q], x_s.at[i], x_r.at[q], (q, e)).wait_recv()

        def norm(b):
            x = xg[b].astype(jnp.float32)
            at = pl.ds(b * seq, seq)
            a_ref[at, :] = (x * lax.rsqrt(kept(jnp.mean, x * x) + EPS)).astype(jnp.bfloat16)
            acc[at, :] = x

        loop(nseq, norm)

    def piece(w, s, f, q):
        if w:
            return go.at[pl.ds(s * orows + q * (orows // nq), orows // nq), :]
        return gw.at[s, :, pl.ds(f * rows + q * quarter, quarter), :]

    def half(w, s, zs, q, i):
        if w:
            n = orows // nq // 2
            return go.at[pl.ds(s * orows + (2 * q + i) * n, n), :]
        n = quarter // 2
        return gw.at[s, :, pl.ds(ep_at(zs, c) * rows + (2 * q + i) * n, n), :]

    def own_wo(s, lo, n):
        return wo_ref.at[pl.ds(mod(s, per) * orows + lo, n), :]

    def z_send(w, s, zs, up, second=0):
        ref = piece(w, s, ep_at(zs, c), q_pair[3] if second else mine)
        i = 2 if second else w
        return rcopy(ref, ref, (zp if up else zm).at[i, s, zs], zr.at[i, s, zs], (r, e + 2) if up else (r, e - 2))

    def xy_send(w, s, zs, q, ssem, rsem, dev):
        ref = piece(w, s, ep_at(zs, c), q)
        return rcopy(ref, ref, ssem.at[w, s, zs], rsem.at[w, s, zs], dev)

    def xd_send(w, s, zs, q):
        ref = half(w, s, zs, q, 1)
        return rcopy(ref, ref, xd.at[w, s, zs], dr.at[1, w, s, zs], x_dev)

    def yd_send(w, s, zs, q):
        ref = half(w, s, zs, q, 0)
        return rcopy(ref, ref, yd.at[w, s, zs], dr.at[0, w, s, zs], y_dev)

    def p_copy(w, s, zs, k, j, core):
        ref = piece(w, s, ep_at(zs, core), quarters(w, k)[j])
        return rcopy(ref, ref, ps.at[w, s, zs, j], pr.at[w, s, zs, j], partner)

    def p_whole(w, s, f):
        ref = go.at[pl.ds(s * orows, orows), :] if w else gw.at[s, :, pl.ds(f * rows, rows), :]
        return rcopy(ref, ref, ps.at[w, s, z, 0], pr.at[w, s, z, 0], partner)

    def own_parts(s):
        return [(w.at[:, pl.ds(s * wide, wide)], m) for m, w in enumerate((wq_ref, wk_ref, wv_ref))]

    def if_wo(s, f, *fns):
        @pl.when(s // per == f)
        def _():
            for fn in fns:
                fn()

    def each_line(fn):
        pl.when(z > 0)(lambda: fn(False))
        pl.when(z < nz - 1)(lambda: fn(True))

    def each_side(k, fn):
        pl.when(z - k - 1 >= 0)(lambda: fn(z - k - 1, True))
        pl.when(z + k + 1 < nz)(lambda: fn(z + k + 1, False))

    def originate(s):
        def line(up):
            sem = zp if up else zm
            dev = (r, e + 2) if up else (r, e - 2)
            for i, q in ((0, mine), (2, q_pair[3])):
                for w, m in own_parts(s):
                    rcopy(w.at[pl.ds(q * quarter, quarter), :], gw.at[s, m, pl.ds(e * rows + q * quarter, quarter), :],
                          sem.at[i, s, z], zr.at[i, s, z], dev).start()
            if_wo(s, e, lambda: rcopy(own_wo(s, mine * (orows // nq), orows // nq), piece(1, s, e, mine), sem.at[1, s, z],
                                      zr.at[1, s, z], dev).start())

        each_line(line)
        for w, m in own_parts(s):
            rcopy(w, gw.at[s, m, pl.ds(e * rows, rows), :], ps.at[0, s, z, 0], pr.at[0, s, z, 0], partner).start()
        if_wo(s, e, lambda: rcopy(own_wo(s, 0, orows), go.at[pl.ds(s * orows, orows), :], ps.at[1, s, z, 0],
                                  pr.at[1, s, z, 0], partner).start())

    def for_both(s, f, fn):
        fn(0)
        if_wo(s, f, lambda: fn(1))

    def along_z(s, k):
        def side(zs, up):
            def one(w):
                z_send(w, s, zs, up).wait_recv()
                pl.when(z < nz - 1 if up else z > 0)(lambda: z_send(w, s, zs, up).start())
                if pairs(w, k):
                    z_send(w, s, zs, up, 1).wait_recv()
                    p_copy(w, s, zs, k, 3, c).start()
                xy_send(w, s, zs, to_x if pairs(w, k) else mine, xs, xr, x_dev).start()
                xy_send(w, s, zs, to_y if pairs(w, k) else mine, ys, yr, y_dev).start()
                p_copy(w, s, zs, k, 0, c).start()

            for_both(s, ep_at(zs, c), one)

        each_side(k, side)

    def across(s, k):
        def side(zs, up):
            def one(w):
                q = quarters(w, k)
                xy_send(w, s, zs, q[1], xs, xr, x_dev).wait_recv()
                if not pairs(w, k):
                    yd_send(w, s, zs, q[1]).start()
                p_copy(w, s, zs, k, 1, c).start()
                xy_send(w, s, zs, q[2], ys, yr, y_dev).wait_recv()
                if not pairs(w, k):
                    xd_send(w, s, zs, q[2]).start()
                p_copy(w, s, zs, k, 2, c).start()

            for_both(s, ep_at(zs, c), one)

        each_side(k, side)

    def diagonal(s, k):
        def side(zs, up):
            def one(w):
                if not pairs(w, k):
                    xd_send(w, s, zs, q_line[3]).wait_recv()
                    yd_send(w, s, zs, q_line[3]).wait_recv()
                    p_copy(w, s, zs, k, 3, c).start()

            for_both(s, ep_at(zs, c), one)

        each_side(k, side)

    def load(s, f):
        slot = mod(s, 2)
        return pltpu.make_async_copy(gw.at[s, :, pl.ds(f * rows, rows), :], wbuf.at[slot, :, pl.ds(f * rows, rows), :],
                                     lsem.at[slot, f])

    def oload(s, src):
        slot = mod(s, 2)
        return pltpu.make_async_copy(src, obuf.at[slot], lsem.at[slot, nd])

    def collect(s):
        slot = mod(s, 2)
        whole = go.at[pl.ds(s * orows, orows), :]

        def side(k, zs):
            def one(w):
                for j in range(nq):
                    p_copy(w, s, zs, k, j, 1 - c).wait_recv()

            for_both(s, ep_at(zs, 1 - c), one)

        for k in range(nz - 1):
            each_side(k, lambda zs, up: side(k, zs))
        p_whole(0, s, e_p).wait_recv()
        if_wo(s, e_p, lambda: p_whole(1, s, e_p).wait_recv())

        for f in range(nd):
            def near():
                for w, m in own_parts(s):
                    pltpu.make_async_copy(w, wbuf.at[slot, m, pl.ds(f * rows, rows), :], lsem.at[slot, f]).start()

            pl.when(f == e)(near)
            pl.when(f != e)(lambda: load(s, f).start())
        if_wo(s, e, lambda: oload(s, own_wo(s, 0, orows)).start())
        pl.when(s // per != e)(lambda: oload(s, whole).start())

    def wait_loads(s):
        for f in range(nd):
            load(s, f).wait()
        oload(s, go.at[pl.ds(s * orows, orows), :]).wait()

    pair = 2 * HEAD
    npair = wide // pair

    def compute(s, j):
        slot = mod(s, 2)
        a = a_ref[...]
        cols = pl.ds(pl.multiple_of(j * pair, pair), pair)
        cos, sin = cos_ref[...], sin_ref[...]

        def rot(v):
            return (v * cos + pltpu.roll(v, HEAD // 2, 1) * sin).astype(jnp.bfloat16)

        q, k, v = [jnp.dot(a, wbuf[slot, m, :, cols], preferred_element_type=jnp.float32) for m in range(3)]
        v = v.astype(jnp.bfloat16)
        tri = lax.broadcasted_iota(jnp.int32, (seq, seq), 0) >= lax.broadcasted_iota(jnp.int32, (seq, seq), 1)
        heads = []
        for hh in range(CORES):
            hc = slice(hh * HEAD, (hh + 1) * HEAD)
            outs = []
            for b in range(nseq):
                rs = slice(b * seq, (b + 1) * seq)
                sc = lax.dot_general(rot(q[rs, hc]), rot(k[rs, hc]), (((1,), (1,)), ((), ())),
                                     preferred_element_type=jnp.float32)
                sc = jnp.where(tri, sc * HEAD ** -0.5, -jnp.inf)
                ex = jnp.exp(sc - kept(jnp.max, sc))
                p = (ex / kept(jnp.sum, ex)).astype(jnp.bfloat16)
                outs.append(jnp.dot(p, v[rs, hc], preferred_element_type=jnp.float32).astype(jnp.bfloat16))
            heads.append(jnp.concatenate(outs, axis=0))
        o = jnp.concatenate(heads, axis=1)
        acc[...] += jnp.dot(o, obuf[slot, cols, :], preferred_element_type=jnp.float32)

    def within(s, fn, *args):
        pl.when((s >= 0) & (s < STEPS))(lambda: fn(s, *args))

    originate(0)

    def turn(i):
        within(i + 1, originate)
        within(i - 3, wait_loads)

        def serve(k):
            within(i - 1, across, k)
            within(i, along_z, k)

        def work(j):
            within(i - 3, compute, j)

            @pl.when(j == 0)
            def _():
                within(i - 2, diagonal, 1)
                serve(1)
                within(i - 2, diagonal, 2)
                within(i - 2, collect)

        within(i - 2, diagonal, 0)
        serve(0)
        loop(npair, work)
        serve(2)
        pl.when(i == 1)(spread_ids)
        pl.when(i == 2)(prepare)

    loop(STEPS + 3, turn)

    keep_own = pltpu.make_async_copy(ids_out.at[e], idv, csem.at[0])
    keep_own.start()
    keep_own.wait()
    pitch = d // LANES + 1
    tile = pl.ds(0, d // LANES)

    def spill(v, *parts):
        for k in range(d // LANES):
            tm[pl.ds(k, seq, stride=pitch), :] = v[:, k * LANES:(k + 1) * LANES]

        def rows_to(ref, base, lo):
            def some(g):
                for i in range(8):
                    j = g * 8 + i
                    ref[base + j] = tm[pl.ds((lo + j) * pitch, d // LANES), :].astype(jnp.bfloat16)

            return some

        for ref, base, lo, hi in parts:
            loop((hi - lo) // 8, rows_to(ref, base, lo))

    def route(b):
        h = acc[pl.ds(b * seq, seq), :].astype(jnp.bfloat16).astype(jnp.float32)
        n = h * lax.rsqrt(kept(jnp.mean, h * h) + EPS)
        logits = jnp.dot(n, wr_ref[...], precision=lax.Precision.HIGHEST, preferred_element_type=jnp.float32).T
        expert = lax.broadcasted_iota(jnp.int32, logits.shape, 0)
        ids = idv[b]
        picked = jnp.concatenate([jnp.sum(jnp.where(expert == ids[k:k + 1, :], logits, 0.0), axis=0, keepdims=True)
                                  for k in range(ids.shape[0])], axis=0)
        ex = jnp.exp(picked - kept(jnp.max, picked, 0))
        gates[b] = ex / kept(jnp.sum, ex, 0)
        rest, tail = seq - cut, cut - ret
        spill(n, (ua_ref, b * cut, 0, cut), (ub_ref, b * rest, cut, seq))
        spill(h, (ha_ref, b * ret, 0, ret), (hb_ref, b * tail, ret, cut), (hb_ref, nseq * tail + b * rest, cut, seq))

    loop(nseq, route)
    left = gates[...].reshape(-1, LANES)
    per_tile = d // LANES
    for term in range(3):
        g = left.astype(jnp.bfloat16)
        left = left - g.astype(jnp.float32)
        for i in range(g.shape[0] // per_tile):
            ua_ref[nseq * cut + term * (g.shape[0] // per_tile) + i] = g[i * per_tile:(i + 1) * per_tile, :]

    for i, f in enumerate(mates):
        rcopy(ids_out.at[e], ids_out.at[f], j_s.at[i], j_r.at[f], (r, f)).wait()
    for i, q in enumerate(others):
        rcopy(idt_hbm.at[q], ids_out.at[e, r], i_s.at[i], i_r.at[r], (q, e)).wait_send()
        rcopy(x_hbm.at[q], xg.at[r], x_s.at[i], x_r.at[r], (q, e)).wait_send()

    def drain(s):
        def side(k, zs, up):
            def sent(w):
                pl.when(z < nz - 1 if up else z > 0)(lambda: z_send(w, s, zs, up).wait_send())
                for j in range(nq):
                    p_copy(w, s, zs, k, j, c).wait_send()
                xy_send(w, s, zs, mine, xs, xr, x_dev).wait_send()
                xy_send(w, s, zs, mine, ys, yr, y_dev).wait_send()
                if not pairs(w, k):
                    xd_send(w, s, zs, mine).wait_send()
                    yd_send(w, s, zs, mine).wait_send()

            for_both(s, ep_at(zs, c), sent)

        for k in range(nz - 1):
            each_side(k, lambda zs, up: side(k, zs, up))

        def own(w):
            each_line(lambda up: z_send(w, s, z, up).wait_send())
            p_whole(w, s, e).wait_send()

        for_both(s, e, own)
        each_line(lambda up: z_send(0, s, z, up, 1).wait_send())

    loop(STEPS, drain)


def attention(x, idt, wr, wq, wk, wv, wo, cut, ret):
    nseq, seq, d = x.shape
    rows, hd = wq.shape
    nd, k = d // rows, idt.shape[1]
    cols = d // LANES
    half = HEAD // 2
    freq = THETA ** (-jnp.arange(half, dtype=jnp.float32) / half)
    ang = jnp.arange(seq, dtype=jnp.float32)[:, None] * freq
    cos = jnp.concatenate([jnp.cos(ang)] * 2, axis=1)
    sin = jnp.concatenate([-jnp.sin(ang), jnp.sin(ang)], axis=1)
    vmem = pl.BlockSpec(memory_space=pltpu.VMEM)
    hbm = pl.BlockSpec(memory_space=pl.ANY)
    wide = hd // STEPS
    dma = pltpu.SemaphoreType.DMA
    bf = jnp.bfloat16

    def out(*shape, dtype=bf):
        return jax.ShapeDtypeStruct(shape, dtype)

    na, nb = nseq * cut, nseq * (seq - cut)
    return pl.pallas_call(
        functools.partial(attn_kernel, cut, ret),
        out_shape=(out(na + 3 * nseq * k // cols, cols, LANES), out(nb, cols, LANES),
                   out(nseq * ret, cols, LANES), out(nseq * (seq - ret), cols, LANES), out(nd, nseq, k, seq, dtype=jnp.int32), out(STEPS, 3, d, wide), out(hd, d)),
        in_specs=[hbm, hbm] + [vmem] * 3 + [hbm] * 4,
        out_specs=(vmem, vmem, vmem, vmem, hbm, hbm, hbm),
        scratch_shapes=[
            pltpu.VMEM((nseq, seq, d), bf), pltpu.VMEM((nseq * seq, d), bf), pltpu.VMEM((nseq * seq, d), jnp.float32),
            pltpu.VMEM((2, 3, d, wide), bf), pltpu.VMEM((2, hd // STEPS, d), bf),
            pltpu.VMEM((seq * (cols + 1), LANES), jnp.float32), pltpu.VMEM((nseq, k, seq), jnp.float32),
            pltpu.VMEM((nseq, k, seq), jnp.int32),
            *([dma((3, STEPS, 4))] * 3), *([dma((2, STEPS, 4))] * 6), dma((2, 2, STEPS, 4)), *([dma((2, STEPS, 4, 4))] * 2),
            *([dma((4,))] * 4), *([dma((nd,))] * 2), dma((2, nd + 1)), dma((2,)),
        ],
        compiler_params=pltpu.CompilerParams(collective_id=0, has_side_effects=True, vmem_limit_bytes=VMEM),
        cost_estimate=cost(10 * nseq * seq * d * hd, 8 * d * hd),
    )(x, idt, cos, sin, wr, wq, wk, wv, wo)[:5]


def token_of(key):
    return lax.shift_right_logical(key, SLOT_BITS) & ((1 << TOKEN_BITS) - 1)


def moe_kernel(nt, stores, given, nblk_ref, be_ref, bb_ref, bn_ref, key_ref, gate_ref, u_hbm, w1_hbm, w3_hbm, w2_hbm, *refs):
    outs, (ub, acc, w1, w3, w2, xs, zs, lhs, usem, wsem, osem) = refs[given:-11], refs[-11:]
    cols = ub.shape[1]
    nexp = w1_hbm.shape[0]
    nblk = nblk_ref[0]

    def weights(e, slot):
        return (pltpu.make_async_copy(w1_hbm.at[e], w1.at[slot], wsem.at[slot, 0]),
                pltpu.make_async_copy(w3_hbm.at[e], w3.at[slot], wsem.at[slot, 1]),
                pltpu.make_async_copy(w2_hbm.at[e], w2.at[slot], wsem.at[slot, 2]))

    nd = u_hbm.shape[0]
    n = nt // nd
    for c in weights(0, 0):
        c.start()
    for dev in range(nd):
        pltpu.make_async_copy(u_hbm.at[dev, pl.ds(0, n)], ub.at[pl.ds(dev * n, n)], usem).start()

    def zero(i):
        acc[pl.ds(i * 8, 8)] = jnp.zeros((8,) + acc.shape[1:], jnp.float32)

    loop(acc.shape[0] // 8, zero)
    pltpu.make_async_copy(ub.at[pl.ds(0, nt)], ub.at[pl.ds(0, nt)], usem).wait()

    def gather(b, some):
        base = bb_ref[b]
        for i in some:
            t = token_of(key_ref[base + i])
            xs[pl.ds(i, cols, stride=PITCH), :] = ub[t].astype(jnp.float32)

    def scatter(base, n, rows):
        new = []
        for i in rows:
            key = key_ref[base + i]
            t = jnp.where(i < n, token_of(key), nt)
            new.append((t, acc[t] + gate_ref[key & ((1 << SLOT_BITS) - 1)] * zs[pl.ds(i, cols, stride=PITCH), :]))
        for t, v in new:
            acc[t] = v

    def eight(g):
        return [g * 8 + i for i in range(8)]

    loop(BM // 8, lambda g: gather(0, eight(g)))

    def body(b, e_prev):
        e = be_ref[b]
        slot = e % 2

        @pl.when(e != e_prev)
        def _():
            @pl.when(e + 1 < nexp)
            def _():
                for c in weights(e + 1, 1 - slot):
                    c.start()

            for c in weights(e, slot):
                c.wait()

        for k in range(cols):
            lhs[:, k * LANES:(k + 1) * LANES] = xs[k * PITCH:k * PITCH + BM, :].astype(jnp.bfloat16)
        gather(b + 1, range(BM))
        bp = jnp.maximum(b - 1, 0)
        base, valid = bb_ref[bp], jnp.where(b > 0, bn_ref[bp], 0)
        for g in range(BM // 8):
            scatter(base, valid, eight(g))
        x = lhs[...]
        a1 = jnp.dot(x, w1[slot], preferred_element_type=jnp.float32)
        a3 = jnp.dot(x, w3[slot], preferred_element_type=jnp.float32)
        act = (jax.nn.silu(a1) * a3).astype(jnp.bfloat16)
        z = jnp.dot(act, w2[slot], preferred_element_type=jnp.float32).astype(jnp.bfloat16).astype(jnp.float32)
        for k in range(cols):
            zs[k * PITCH:k * PITCH + BM, :] = z[:, k * LANES:(k + 1) * LANES]
        return e

    lax.fori_loop(0, nblk, body, -1)
    loop(BM // 8, lambda g: scatter(bb_ref[nblk - 1], bn_ref[nblk - 1], eight(g)))

    def store(i):
        m = n // 4

        def pack(g):
            for j in eight(g):
                ub[i * m + j] = acc[i * m + j].astype(jnp.bfloat16)

        loop(m // 8, pack)
        dev, b = i // 4, lax.rem(i, 4)
        for out, lo, hi, base in stores:
            pltpu.make_async_copy(ub.at[pl.ds(i * m + lo, hi - lo)], outs[out].at[dev, pl.ds(base + b * (hi - lo), hi - lo)],
                                  osem).start()

    loop(nd * 4, store)
    pltpu.make_async_copy(ub.at[pl.ds(0, nt)], ub.at[pl.ds(0, nt)], osem).wait()


def moe(nblk, be, bb, bn, keys, gates, u, n, w1, w3, w2, lengths, stores, *into):
    nd, _, cols, _ = u.shape
    nt = nd * n
    ne, d, f = w1.shape
    smem = pl.BlockSpec(memory_space=pltpu.SMEM)
    hbm = pl.BlockSpec(memory_space=pl.ANY)
    return pl.pallas_call(
        functools.partial(moe_kernel, nt, stores, len(into)),
        out_shape=[jax.ShapeDtypeStruct((nd, m, cols, LANES), jnp.bfloat16) for m in lengths],
        in_specs=[smem] * 6 + [hbm] * (4 + len(into)),
        out_specs=[hbm] * len(lengths),
        input_output_aliases={10 + i: i for i in range(len(into))},
        scratch_shapes=[
            pltpu.VMEM((nt + 8, cols, LANES), jnp.bfloat16),
            pltpu.VMEM((nt + 8, cols, LANES), jnp.float32),
            pltpu.VMEM((2, d, f), jnp.bfloat16),
            pltpu.VMEM((2, d, f), jnp.bfloat16),
            pltpu.VMEM((2, f, d), jnp.bfloat16),
            pltpu.VMEM((cols * PITCH, LANES), jnp.float32),
            pltpu.VMEM((cols * PITCH, LANES), jnp.float32),
            pltpu.VMEM((BM, d), jnp.bfloat16),
            pltpu.SemaphoreType.DMA,
            pltpu.SemaphoreType.DMA((2, 3)),
            pltpu.SemaphoreType.DMA,
        ],
        compiler_params=pltpu.CompilerParams(vmem_limit_bytes=VMEM),
        cost_estimate=cost(30000 * d * f, 6 * ne * d * f),
    )(nblk, be, bb, bn, keys, gates, u, w1, w3, w2, *into)


def back_kernel(ret, piece, part, h_ref, h_mid, raw_here, raw_cross, first_hbm, ha_ref, y_out, own, prt, raw, fin, fout, hs, yst, yfirst, firsts, tm, raw_s, raw_r,
                prt_s, prt_r, f_s, f_r, y_s, y_r, osem, lsem, csem):
    r, e = lax.axis_index('replica'), lax.axis_index('ep')
    z, c = e // 2, e % 2
    n = h_ref.shape[0]
    pieces = n // piece
    split = pieces // 4
    early = 4
    mid = (z + 2) // 3 + (5 - z) // 3 - 1
    low = z // 2
    on_mid, on_end = pl.when(mid == 1), pl.when(mid == 0)
    z_mid, z_end = 1 + low, 3 * low
    partner, across = (r, ep_at(z, 1 - c)), (r, ep_at(2 - low, c))
    to_end = (r, ep_at(z_end, c))
    others = [lax.rem(r + i, 4) for i in range(1, 4)]

    def far(i):
        return 2 + i + low * (-1 - 2 * i)

    def near(i):
        return 1 - i + low * (1 + 2 * i)

    def rows(p):
        return pl.ds(p * piece, piece)

    end, inner = mid == 0, mid == 1
    meet([(None, (q, e)) for q in others] + [(None, partner)] +
         [(end, (q, ep_at(z_mid, c))) for q in range(REPLICAS)] + [(end, (r, ep_at(z_mid, 1 - c)))] +
         [(inner, (q, ep_at(z_end, c))) for q in range(REPLICAS)] + [(inner, (r, ep_at(z_end, 1 - c))), (inner, across)], 9 + mid)

    def raw_send(i, core, p):
        return rcopy(part.at[ep_at(far(i), core), rows(p)], raw.at[i, c, rows(p)], raw_s.at[i, core, p], raw_r.at[i, c, p],
                     (r, ep_at(z_mid, core)))

    def raw_recv(i, core, p):
        ref = raw.at[i, core, rows(p)]
        return rcopy(ref, ref, raw_s.at[i, core, p], raw_r.at[i, core, p], (r, ep_at(z_end, core)))

    def prt_copy(chip, p):
        return rcopy(part.at[ep_at(chip, 1 - c), rows(p)], prt.at[chip, rows(p)], prt_s.at[chip, p], prt_r.at[chip, p], partner)

    def f_copy(i, p, onward):
        return rcopy(fout.at[2 * onward + i, rows(p)], fin.at[i, rows(p)], f_s.at[2 * onward + i, p], f_r.at[i, p],
                     to_end if onward else across)

    def load(chip):
        return pltpu.make_async_copy(part.at[ep_at(chip, c)], own.at[chip], osem.at[chip])

    def landed(i):
        j = i + low * (1 - 2 * i)
        rest = pl.ds(0, early * piece)
        return (pltpu.make_async_copy(raw_here.at[j], raw.at[i, c, rest], csem.at[i, 0]),
                pltpu.make_async_copy(raw_cross.at[j], raw.at[i, 1 - c, rest], csem.at[i, 1]))

    keep_h = pltpu.make_async_copy(h_mid, hs, csem.at[0, 0])

    def place(half):
        return pl.ds(0, ret) if half < 0 else pl.ds(ret + half * piece, piece)

    def y_copy(src, i, blk, half, f):
        return rcopy(src, y_out.at[r, place(half), :], y_s.at[i, blk, half + 1], y_r.at[r, half + 1], (blk, f))

    def y_local(src, half):
        return pltpu.make_async_copy(src, y_out.at[r, place(half), :], lsem.at[half + 1])

    def put(src, blk, half):
        pl.when(r == blk)(lambda: y_local(src, half).start())
        pl.when(r != blk)(lambda: y_copy(src, 1, blk, half, e).start())

    def each(fn, count=pieces):
        loop(count, fn)

    for i in range(CORES):
        load(near(i)).start()

    @on_end
    def _():
        keep_h.start()
        for i in range(CORES):
            each(lambda p: [raw_send(i, core, p + early).start() for core in range(CORES)], pieces - early)
            each(lambda p: prt_copy(near(i), p).start())

    @on_mid
    def _():
        for i in range(CORES):
            for copy in landed(i):
                copy.start()
            load(far(i)).start()
            each(lambda p: [prt_copy(far(i), p).start(), prt_copy(near(i), p).start()])

    keep_first = pltpu.make_async_copy(first_hbm, firsts, csem.at[2, 0])
    keep_first.start()

    def f32(v):
        return v.astype(jnp.float32)

    def add(chip, p, incoming, put_sum):
        prt_copy(chip, p).wait_recv()

        def some(j):
            s = pl.ds(p * piece + j * 4, 4)
            put_sum(j, s, f32(own[chip, s]) + f32(prt[chip, s]) + incoming(s))

        each(some, piece // 4)

    cols = h_ref.shape[1]
    pitch = cols + 1

    def to(out):
        def put_sum(j, s, v):
            out[s] = v

        return put_sum

    def to_tiles(j, s, v):
        for i in range(v.shape[0]):
            tm[pl.ds((j * v.shape[0] + i) * pitch, cols), :] = v[i]

    def to_rows(out, count):
        for k in range(cols):
            out[:, k * LANES:(k + 1) * LANES] = tm[pl.ds(k, count, stride=pitch), :].astype(jnp.bfloat16)

    def finish_first():
        keep_first.wait()
        for blk in range(REPLICAS):
            def some(j):
                s = pl.ds(blk * ret + j * 4, 4)
                v = f32(ha_ref[s])
                for dev in range(firsts.shape[0]):
                    v = v + f32(firsts[dev, s])
                to_tiles(j, s, v)

            each(some, ret // 4)
            to_rows(yfirst.at[blk], ret)
            put(yfirst.at[blk], blk, -1)

    @on_mid
    def _():
        for i in range(CORES):
            load(far(i)).wait()
            load(near(i)).wait()
            for copy in landed(i):
                copy.wait()

        def first(q):
            i, p = q // pieces, lax.rem(q, pieces)
            pl.when(p >= early)(lambda: [raw_recv(i, core, p).wait_recv() for core in range(CORES)][0])
            add(far(i), p, lambda s: f32(raw[i, 0, s]) + f32(raw[i, 1, s]), to(fout.at[i]))
            f_copy(i, p, 0).start()

        def second(q):
            i, p = q // pieces, lax.rem(q, pieces)
            f_copy(i, p, 0).wait_recv()
            add(near(i), p, lambda s: fin[i, s], to(fout.at[2 + i]))
            f_copy(i, p, 1).start()

        lag = 2

        def step(q):
            pl.when(q < 2 * pieces)(lambda: first(q))
            pl.when(q >= lag)(lambda: second(q - lag))

        each(step, 2 * pieces + lag)
        finish_first()

    @on_end
    def _():
        finish_first()
        for i in range(CORES):
            load(near(i)).wait()
            if i == 0:
                keep_h.wait()
            h = h_ref if i else hs

            def last(p):
                f_copy(i, p, 1).wait_recv()
                add(near(i), p, lambda s: fin[i, s] + f32(h[s]), to_tiles)
                src = yst.at[i, p]
                to_rows(src, piece)
                for blk in range(REPLICAS):
                    for half in range(split):
                        @pl.when(p == (early + blk * (split - 1) + half - 1 if half else blk))
                        def _():
                            if i:
                                put(src, blk, half)
                            else:
                                y_copy(src, i, blk, half, ep_at(z_mid, c)).start()

            each(last)

    @on_end
    def _():
        for i in range(CORES):
            each(lambda p: [raw_send(i, core, p + early).wait_send() for core in range(CORES)], pieces - early)
            each(lambda p: prt_copy(near(i), p).wait_send())
        for blk in range(REPLICAS):
            for half in range(split):
                y_copy(yst.at[0, 0], 0, blk, half, ep_at(z_mid, c)).wait_send()

    @on_mid
    def _():
        for i in range(CORES):
            each(lambda p: [prt_copy(far(i), p).wait_send(), prt_copy(near(i), p).wait_send(),
                            f_copy(i, p, 0).wait_send(), f_copy(i, p, 1).wait_send()])

    for blk in range(REPLICAS):
        for half in range(-1, split):
            src = yfirst.at[blk] if half < 0 else yst.at[1, 0]
            ref = y_out.at[blk, place(half), :]
            came = rcopy(ref, ref, y_s.at[1, blk, half + 1], y_r.at[blk, half + 1], (blk, e))
            sent_here = True if half < 0 else end

            def stayed():
                y_local(src, half).wait()

            def sent():
                y_copy(src, 1, blk, half, e).wait_send()

            pl.when((r == blk) & sent_here)(stayed)
            pl.when((r != blk) & sent_here)(sent)
            pl.when((r != blk) | jnp.logical_not(sent_here))(came.wait_recv)


def back(part, h, h_mid, raw_here, raw_cross, first, ha):
    _, n, cols, _ = part.shape
    ret = ha.shape[0] // 4
    seq = ret + n // 4
    piece = raw_here.shape[1] // 4
    vmem = pl.BlockSpec(memory_space=pltpu.VMEM)
    hbm = pl.BlockSpec(memory_space=pl.ANY)
    dma = pltpu.SemaphoreType.DMA
    pieces = n // piece
    split = pieces // 4

    def tiles(*lead, dtype=jnp.bfloat16):
        return pltpu.VMEM(lead + (n, cols, LANES), dtype)

    return pl.pallas_call(
        functools.partial(back_kernel, ret, piece),
        out_shape=jax.ShapeDtypeStruct((4, seq, cols * LANES), jnp.bfloat16),
        in_specs=[hbm, vmem] + [hbm] * 4 + [vmem],
        out_specs=hbm,
        scratch_shapes=[
            tiles(4), tiles(4), tiles(2, 2), tiles(2, dtype=jnp.float32), tiles(4, dtype=jnp.float32), tiles(),
            pltpu.VMEM((2, pieces, piece, cols * LANES), jnp.bfloat16), pltpu.VMEM((4, ret, cols * LANES), jnp.bfloat16),
            pltpu.VMEM(first.shape, jnp.bfloat16), pltpu.VMEM((ret * (cols + 1), LANES), jnp.float32),
            *([dma((2, 2, pieces))] * 2), *([dma((4, pieces))] * 2), dma((4, pieces)), dma((2, pieces)),
            dma((2, 4, split + 1)), dma((4, split + 1)), dma((4,)), dma((split + 1,)), dma((3, 2)),
        ],
        compiler_params=pltpu.CompilerParams(collective_id=1, has_side_effects=True, vmem_limit_bytes=VMEM),
    )(part, h, h_mid, raw_here, raw_cross, first, ha)


def block_plan(ids, me, ne):
    _, nseq, _, n = ids.shape
    le = ids - me * ne
    local = (le >= 0) & (le < ne)
    total = ids.size
    slot = lax.iota(jnp.int32, total).reshape(ids.shape)
    token = (lax.broadcasted_iota(jnp.int32, ids.shape, 0) * nseq + lax.broadcasted_iota(jnp.int32, ids.shape, 1)) * n
    token = token + lax.broadcasted_iota(jnp.int32, ids.shape, 3)
    key = (le << (SLOT_BITS + TOKEN_BITS)) | (token << SLOT_BITS) | slot
    none = jnp.iinfo(jnp.int32).max
    keys = lax.sort(jnp.where(local, key, none).reshape(-1), is_stable=False)
    experts = jnp.arange(ne, dtype=jnp.int32)
    counts = jnp.sum((le.reshape(-1)[None, :] == experts[:, None]).astype(jnp.int32), axis=1)
    low = (experts[None, :] < experts[:, None])
    first = jnp.sum(jnp.where(low, counts[None, :], 0), axis=1)
    nb = jnp.maximum((counts + BM - 1) // BM, 1)
    bfirst = jnp.sum(jnp.where(low, nb[None, :], 0), axis=1)
    maxb = total // BM + ne + 2
    b = jnp.arange(maxb, dtype=jnp.int32)
    inside = (b[:, None] >= bfirst[None, :]) & (b[:, None] < (bfirst + nb)[None, :])

    def of(v):
        return jnp.sum(jnp.where(inside, v[None, :], 0), axis=1)

    done = (b - of(bfirst)) * BM
    be, bb = of(experts), of(first) + done
    bn = jnp.clip(of(counts) - done, 0, BM)
    bb = jnp.where(jnp.any(inside, axis=1), bb, 0)
    keys = jnp.concatenate([jnp.where(keys == none, 0, keys), jnp.zeros((BM,), jnp.int32)])
    return jnp.sum(nb).reshape(1), be, bb, bn, keys


def solution(mesh):
    nd = mesh.shape['ep']
    tok = P(('replica', 'ep'), None, None)
    rows_ep = P('ep', None)
    by_expert = P('ep', None, None)
    cut, ret = CUT, RET

    def local(x, wq, wk, wv, wo, wr, w1, w3, w2, idx):
        b, s, d = x.shape
        k, ne = idx.shape[-1], w1.shape[0]
        me = lax.axis_index('ep')
        low, c = me // 4, me % 2
        cols = d // LANES
        tail, rest = cut - ret, s - cut
        ua, ub, ha, hb, ids = attention(x, idx.transpose(0, 2, 1), wr, wq, wk, wv, wo, cut, ret)
        plan_a, plan_b = block_plan(ids[..., :cut], me, ne), block_plan(ids[..., cut:], me, ne)
        u_all = lax.all_gather(ua, 'ep')
        u_all, plan_b = lax.optimization_barrier((u_all, plan_b))
        terms = u_all[:, b * cut:].reshape(nd, 3, b, k, s).astype(jnp.float32)
        gates = terms[:, 0] + terms[:, 1] + terms[:, 2]
        lengths = (b * ret, b * (tail + rest))
        part_a, part_b = moe(*plan_a, gates[..., :cut].reshape(-1), u_all, b * cut, w1, w3, w2, lengths,
                             ((0, 0, ret, 0), (1, ret, cut, 0)))
        early = part_b.reshape(-1, nd // 4, CORES, b * (tail + rest), cols, LANES)[:, :, :, :b * tail]
        far = lax.dynamic_index_in_dim(early, 1 - low, 0, False)
        here, cross = [lax.dynamic_index_in_dim(far, i, 1, False) for i in (c, 1 - c)]
        ub_all = lax.all_gather(ub, 'ep')
        part_a, part_b, here, cross, ub_all = lax.optimization_barrier((part_a, part_b, here, cross, ub_all))
        inward = [(0, 2), (1, 3), (6, 4), (7, 5)]
        here = lax.ppermute(here, 'ep', inward)
        cross = lax.ppermute(cross, 'ep', [(i, j ^ 1) for i, j in inward])
        h_mid = lax.ppermute(hb, 'ep', [(j, i) for i, j in inward])
        part_a = lax.all_to_all(part_a, 'ep', 0, 0, tiled=True)
        part_b, = moe(*plan_b, gates[..., cut:].reshape(-1), ub_all, b * rest, w1, w3, w2, lengths[1:],
                      ((0, 0, rest, b * tail),), part_b)
        return back(part_b, hb, h_mid, here, cross, part_a, ha)

    return jax.shard_map(local, mesh=mesh,
                         in_specs=(tok, rows_ep, rows_ep, rows_ep, rows_ep, P(None, None),
                                   by_expert, by_expert, by_expert, tok),
                         out_specs=tok, check_vma=False)
```

```python
import functools
import jax
import jax.numpy as jnp
from jax import lax
from jax.experimental import pallas as pl
from jax.experimental.pallas import tpu as pltpu
from jax.sharding import PartitionSpec as P

HEAD = 128
EPS = 1e-6
THETA = 10000.0
BM = 128
PITCH = BM + 1
LANES = 128
VMEM = 60 * 1024 * 1024
CORES = 2
REPLICAS = 4
CUT = 56
RET = 32
STEPS = 8
SLOT_BITS, TOKEN_BITS = 15, 12


def loop(n, fn):
    def step(i, carry):
        fn(i)
        return carry

    lax.fori_loop(0, n, step, 0)


def cost(flops, moved):
    return pl.CostEstimate(flops=flops, bytes_accessed=moved, transcendentals=0)


def kept(fn, v, axis=-1):
    return fn(v, axis=axis, keepdims=True)


def odd(v):
    return lax.rem(v, 2)


def ep_at(z, c):
    return 2 * z + c


MESH_ID = pl.DeviceIdType.MESH


def rcopy(src, dst, ssem, rsem, dev):
    return pltpu.make_async_remote_copy(src_ref=src, dst_ref=dst, send_sem=ssem, recv_sem=rsem, device_id=dev,
                                        device_id_type=MESH_ID)


def meet(peers, count):
    barrier = pltpu.get_barrier_semaphore()
    for guard, dev in peers:
        def greet():
            pl.semaphore_signal(barrier, device_id=dev, device_id_type=MESH_ID)

        if guard is None:
            greet()
        else:
            pl.when(guard)(greet)
    pl.semaphore_wait(barrier, count)


def attn_kernel(cut, ret, x_hbm, idt_hbm, cos_ref, sin_ref, wr_ref, wq_ref, wk_ref, wv_ref, wo_ref,
                ua_ref, ub_ref, ha_ref, hb_ref, ids_out, gw, go,
                xg, a_ref, acc, wbuf, obuf, tm, gates, idv, zr, zp, zm, xr, yr, xs, ys, xd, yd, dr, pr, ps,
                x_s, x_r, i_s, i_r, j_s, j_r, lsem, csem):
    r, e = lax.axis_index('replica'), lax.axis_index('ep')
    nz, nq = 4, 4
    z, c = e // 2, e % 2
    e_p = ep_at(z, 1 - c)
    x, y = r // 2, r % 2
    r_x, r_y = (r + 2) % nq, r + 1 - 2 * y

    def line_quarter(x, y):
        return 2 - y + x * (4 * y - 2)

    mine = line_quarter(x, y)
    q_line = (mine, line_quarter(1 - x, y), line_quarter(x, 1 - y), line_quarter(1 - x, 1 - y))
    to_x, to_y = 2 + x, y
    q_pair = (mine, 3 - x, 1 - y, to_x + to_y - mine)

    def pairs(w, k):
        return w == 0 and k == 0

    def quarters(w, k):
        return q_pair if pairs(w, k) else q_line

    nd = ids_out.shape[0]
    rows, wide = wq_ref.shape[0], wq_ref.shape[1] // STEPS
    quarter = rows // nq
    orows = go.shape[0] // STEPS
    nseq, seq, d = x_hbm.shape
    partner, x_dev, y_dev = (r, e_p), (r_x, e), (r_y, e)
    srows = orows // nz

    def mod(v, m):
        return lax.rem(v, m)

    others = [mod(r + i, nq) for i in range(1, nq)]
    mates = [mod(e + i, nd) for i in range(1, nd)]
    meet([(None, (q, e)) for q in others] + [(None, (r, f)) for f in mates], len(others) + len(mates))

    for i, q in enumerate(others):
        rcopy(idt_hbm.at[q], ids_out.at[e, r], i_s.at[i], i_r.at[r], (q, e)).start()
        rcopy(x_hbm.at[q], xg.at[r], x_s.at[i], x_r.at[r], (q, e)).start()
    keep_ids = pltpu.make_async_copy(idt_hbm.at[r], ids_out.at[e, r], csem.at[0])
    keep_x = pltpu.make_async_copy(x_hbm.at[r], xg.at[r], csem.at[1])
    keep_ids.start()
    keep_x.start()

    def spread_ids():
        keep_ids.wait()
        for i, q in enumerate(others):
            rcopy(idt_hbm.at[q], ids_out.at[e, q], i_s.at[i], i_r.at[q], (q, e)).wait_recv()
        for i, f in enumerate(mates):
            rcopy(ids_out.at[e], ids_out.at[e], j_s.at[i], j_r.at[e], (r, f)).start()

    def prepare():
        keep_x.wait()
        for i, q in enumerate(others):
            rcopy(x_hbm.at[q], xg.at[q], x_s.at[i], x_r.at[q], (q, e)).wait_recv()

        def norm(b):
            x = xg[b].astype(jnp.float32)
            at = pl.ds(b * seq, seq)
            a_ref[at, :] = (x * lax.rsqrt(kept(jnp.mean, x * x) + EPS)).astype(jnp.bfloat16)
            acc[at, :] = x

        loop(nseq, norm)

    def piece(w, s, f, q):
        if w:
            return go.at[pl.ds(s * orows + f // 2 * srows + q * (srows // nq), srows // nq), :]
        return gw.at[s, :, pl.ds(f * rows + q * quarter, quarter), :]

    def half(w, s, zs, q, i):
        if w:
            n = srows // nq // 2
            return go.at[pl.ds(s * orows + zs * srows + (2 * q + i) * n, n), :]
        n = quarter // 2
        return gw.at[s, :, pl.ds(ep_at(zs, c) * rows + (2 * q + i) * n, n), :]

    def own_wo(s, lo, n):
        return wo_ref.at[pl.ds(s // 2 * srows + lo, n), :]

    def z_send(w, s, zs, up, second=0):
        ref = piece(w, s, ep_at(zs, c), q_pair[3] if second else mine)
        i = 2 if second else w
        return rcopy(ref, ref, (zp if up else zm).at[i, s, zs], zr.at[i, s, zs], (r, e + 2) if up else (r, e - 2))

    def xy_send(w, s, zs, q, ssem, rsem, dev):
        ref = piece(w, s, ep_at(zs, c), q)
        return rcopy(ref, ref, ssem.at[w, s, zs], rsem.at[w, s, zs], dev)

    def xd_send(w, s, zs, q):
        ref = half(w, s, zs, q, 1)
        return rcopy(ref, ref, xd.at[w, s, zs], dr.at[1, w, s, zs], x_dev)

    def yd_send(w, s, zs, q):
        ref = half(w, s, zs, q, 0)
        return rcopy(ref, ref, yd.at[w, s, zs], dr.at[0, w, s, zs], y_dev)

    def p_copy(w, s, zs, k, j, core):
        ref = piece(w, s, ep_at(zs, core), quarters(w, k)[j])
        return rcopy(ref, ref, ps.at[w, s, zs, j], pr.at[w, s, zs, j], partner)

    def p_whole(w, s, f):
        ref = go.at[pl.ds(s * orows + z * srows, srows), :] if w else gw.at[s, :, pl.ds(f * rows, rows), :]
        return rcopy(ref, ref, ps.at[w, s, z, 0], pr.at[w, s, z, 0], partner)

    def own_parts(s):
        out = []
        for t in range(nz):
            head = ep_at(t, odd(t + s)) * (STEPS // 2) + s // 2
            for m, w in enumerate((wq_ref, wk_ref, wv_ref)):
                out.append((w.at[:, pl.ds(head * HEAD, HEAD)], m, pl.ds(t * HEAD, HEAD)))
        return out

    def if_wo(s, zs, core, *fns):
        @pl.when(odd(zs + s + core) == 0)
        def _():
            for fn in fns:
                fn()

    def each_line(fn):
        pl.when(z > 0)(lambda: fn(False))
        pl.when(z < nz - 1)(lambda: fn(True))

    def each_side(k, fn):
        pl.when(z - k - 1 >= 0)(lambda: fn(z - k - 1, True))
        pl.when(z + k + 1 < nz)(lambda: fn(z + k + 1, False))

    def originate(s):
        def line(up):
            sem = zp if up else zm
            dev = (r, e + 2) if up else (r, e - 2)
            for i, q in ((0, mine), (2, q_pair[3])):
                for w, m, t in own_parts(s):
                    rcopy(w.at[pl.ds(q * quarter, quarter), :], gw.at[s, m, pl.ds(e * rows + q * quarter, quarter), t],
                          sem.at[i, s, z], zr.at[i, s, z], dev).start()
            if_wo(s, z, c, lambda: rcopy(own_wo(s, mine * (srows // nq), srows // nq), piece(1, s, e, mine), sem.at[1, s, z],
                                      zr.at[1, s, z], dev).start())

        each_line(line)
        for w, m, t in own_parts(s):
            rcopy(w, gw.at[s, m, pl.ds(e * rows, rows), t], ps.at[0, s, z, 0], pr.at[0, s, z, 0], partner).start()
        if_wo(s, z, c, lambda: rcopy(own_wo(s, 0, srows), go.at[pl.ds(s * orows + z * srows, srows), :], ps.at[1, s, z, 0],
                                     pr.at[1, s, z, 0], partner).start())

    def for_both(s, zs, core, fn):
        fn(0)
        if_wo(s, zs, core, lambda: fn(1))

    def along_z(s, k):
        def side(zs, up):
            def one(w):
                z_send(w, s, zs, up).wait_recv()
                pl.when(z < nz - 1 if up else z > 0)(lambda: z_send(w, s, zs, up).start())
                if pairs(w, k):
                    z_send(w, s, zs, up, 1).wait_recv()
                    p_copy(w, s, zs, k, 3, c).start()
                xy_send(w, s, zs, to_x if pairs(w, k) else mine, xs, xr, x_dev).start()
                xy_send(w, s, zs, to_y if pairs(w, k) else mine, ys, yr, y_dev).start()
                p_copy(w, s, zs, k, 0, c).start()

            for_both(s, zs, c, one)

        each_side(k, side)

    def across(s, k):
        def side(zs, up):
            def one(w):
                q = quarters(w, k)
                xy_send(w, s, zs, q[1], xs, xr, x_dev).wait_recv()
                if not pairs(w, k):
                    yd_send(w, s, zs, q[1]).start()
                p_copy(w, s, zs, k, 1, c).start()
                xy_send(w, s, zs, q[2], ys, yr, y_dev).wait_recv()
                if not pairs(w, k):
                    xd_send(w, s, zs, q[2]).start()
                p_copy(w, s, zs, k, 2, c).start()

            for_both(s, zs, c, one)

        each_side(k, side)

    def diagonal(s, k):
        def side(zs, up):
            def one(w):
                if not pairs(w, k):
                    xd_send(w, s, zs, q_line[3]).wait_recv()
                    yd_send(w, s, zs, q_line[3]).wait_recv()
                    p_copy(w, s, zs, k, 3, c).start()

            for_both(s, zs, c, one)

        each_side(k, side)

    def load(s, f):
        slot = odd(s)
        return pltpu.make_async_copy(gw.at[s, :, pl.ds(f * rows, rows), :], wbuf.at[slot, :, pl.ds(f * rows, rows), :],
                                     lsem.at[slot, f])

    def oload(s, src, t, n):
        slot = odd(s)
        return pltpu.make_async_copy(src, obuf.at[slot, pl.ds(t * srows, n), :], lsem.at[slot, nd])

    def collect(s):
        slot = odd(s)

        def side(k, zs):
            def one(w):
                for j in range(nq):
                    p_copy(w, s, zs, k, j, 1 - c).wait_recv()

            for_both(s, zs, 1 - c, one)

        for k in range(nz - 1):
            each_side(k, lambda zs, up: side(k, zs))
        p_whole(0, s, e_p).wait_recv()
        if_wo(s, z, 1 - c, lambda: p_whole(1, s, e_p).wait_recv())

        for f in range(nd):
            def near():
                for w, m, t in own_parts(s):
                    pltpu.make_async_copy(w, wbuf.at[slot, m, pl.ds(f * rows, rows), t], lsem.at[slot, f]).start()

            pl.when(f == e)(near)
            pl.when(f != e)(lambda: load(s, f).start())
        for t in range(nz):
            here = (t == z) & (odd(t + s + c) == 0)
            pl.when(here)(lambda: oload(s, own_wo(s, 0, srows), t, srows).start())
            pl.when(jnp.logical_not(here))(
                lambda: oload(s, go.at[pl.ds(s * orows + t * srows, srows), :], t, srows).start())

    def wait_loads(s):
        for f in range(nd):
            load(s, f).wait()
        oload(s, go.at[pl.ds(s * orows, orows), :], 0, orows).wait()

    pair = 2 * HEAD
    npair = wide // pair

    def compute(s, j):
        slot = odd(s)
        a = a_ref[...]
        cols = pl.ds(pl.multiple_of(j * pair, pair), pair)
        cos, sin = cos_ref[...], sin_ref[...]

        def rot(v):
            return (v * cos + pltpu.roll(v, HEAD // 2, 1) * sin).astype(jnp.bfloat16)

        q, k, v = [jnp.dot(a, wbuf[slot, m, :, cols], preferred_element_type=jnp.float32) for m in range(3)]
        v = v.astype(jnp.bfloat16)
        tri = lax.broadcasted_iota(jnp.int32, (seq, seq), 0) >= lax.broadcasted_iota(jnp.int32, (seq, seq), 1)
        heads = []
        for hh in range(CORES):
            hc = slice(hh * HEAD, (hh + 1) * HEAD)
            outs = []
            for b in range(nseq):
                rs = slice(b * seq, (b + 1) * seq)
                sc = lax.dot_general(rot(q[rs, hc]), rot(k[rs, hc]), (((1,), (1,)), ((), ())),
                                     preferred_element_type=jnp.float32)
                sc = jnp.where(tri, sc * HEAD ** -0.5, -jnp.inf)
                ex = jnp.exp(sc - kept(jnp.max, sc))
                p = (ex / kept(jnp.sum, ex)).astype(jnp.bfloat16)
                outs.append(jnp.dot(p, v[rs, hc], preferred_element_type=jnp.float32).astype(jnp.bfloat16))
            heads.append(jnp.concatenate(outs, axis=0))
        o = jnp.concatenate(heads, axis=1)
        acc[...] += jnp.dot(o, obuf[slot, cols, :], preferred_element_type=jnp.float32)

    def within(s, fn, *args):
        pl.when((s >= 0) & (s < STEPS))(lambda: fn(s, *args))

    originate(0)

    def turn(i):
        within(i + 1, originate)
        within(i - 3, wait_loads)

        def serve(k):
            within(i - 1, across, k)
            within(i, along_z, k)

        def work(j):
            within(i - 3, compute, j)

            @pl.when(j == 0)
            def _():
                within(i - 2, diagonal, 1)
                serve(1)
                within(i - 2, diagonal, 2)
                within(i - 2, collect)

        within(i - 2, diagonal, 0)
        serve(0)
        loop(npair, work)
        serve(2)
        pl.when(i == 1)(spread_ids)
        pl.when(i == 2)(prepare)

    loop(STEPS + 3, turn)

    keep_own = pltpu.make_async_copy(ids_out.at[e], idv, csem.at[0])
    keep_own.start()
    keep_own.wait()
    pitch = d // LANES + 1
    tile = pl.ds(0, d // LANES)

    def spill(v, *parts):
        for k in range(d // LANES):
            tm[pl.ds(k, seq, stride=pitch), :] = v[:, k * LANES:(k + 1) * LANES]

        def rows_to(ref, base, lo):
            def some(g):
                for i in range(8):
                    j = g * 8 + i
                    ref[base + j] = tm[pl.ds((lo + j) * pitch, d // LANES), :].astype(jnp.bfloat16)

            return some

        for ref, base, lo, hi in parts:
            loop((hi - lo) // 8, rows_to(ref, base, lo))

    def route(b):
        h = acc[pl.ds(b * seq, seq), :].astype(jnp.bfloat16).astype(jnp.float32)
        n = h * lax.rsqrt(kept(jnp.mean, h * h) + EPS)
        logits = jnp.dot(n, wr_ref[...], precision=lax.Precision.HIGHEST, preferred_element_type=jnp.float32).T
        expert = lax.broadcasted_iota(jnp.int32, logits.shape, 0)
        ids = idv[b]
        picked = jnp.concatenate([jnp.sum(jnp.where(expert == ids[k:k + 1, :], logits, 0.0), axis=0, keepdims=True)
                                  for k in range(ids.shape[0])], axis=0)
        ex = jnp.exp(picked - kept(jnp.max, picked, 0))
        gates[b] = ex / kept(jnp.sum, ex, 0)
        rest, tail = seq - cut, cut - ret
        spill(n, (ua_ref, b * cut, 0, cut), (ub_ref, b * rest, cut, seq))
        spill(h, (ha_ref, b * ret, 0, ret), (hb_ref, b * tail, ret, cut), (hb_ref, nseq * tail + b * rest, cut, seq))

    loop(nseq, route)
    left = gates[...].reshape(-1, LANES)
    per_tile = d // LANES
    for term in range(3):
        g = left.astype(jnp.bfloat16)
        left = left - g.astype(jnp.float32)
        for i in range(g.shape[0] // per_tile):
            ua_ref[nseq * cut + term * (g.shape[0] // per_tile) + i] = g[i * per_tile:(i + 1) * per_tile, :]

    for i, f in enumerate(mates):
        rcopy(ids_out.at[e], ids_out.at[f], j_s.at[i], j_r.at[f], (r, f)).wait()
    for i, q in enumerate(others):
        rcopy(idt_hbm.at[q], ids_out.at[e, r], i_s.at[i], i_r.at[r], (q, e)).wait_send()
        rcopy(x_hbm.at[q], xg.at[r], x_s.at[i], x_r.at[r], (q, e)).wait_send()

    def drain(s):
        def side(k, zs, up):
            def sent(w):
                pl.when(z < nz - 1 if up else z > 0)(lambda: z_send(w, s, zs, up).wait_send())
                for j in range(nq):
                    p_copy(w, s, zs, k, j, c).wait_send()
                xy_send(w, s, zs, mine, xs, xr, x_dev).wait_send()
                xy_send(w, s, zs, mine, ys, yr, y_dev).wait_send()
                if not pairs(w, k):
                    xd_send(w, s, zs, mine).wait_send()
                    yd_send(w, s, zs, mine).wait_send()

            for_both(s, zs, c, sent)

        for k in range(nz - 1):
            each_side(k, lambda zs, up: side(k, zs, up))

        def own(w):
            each_line(lambda up: z_send(w, s, z, up).wait_send())
            p_whole(w, s, e).wait_send()

        for_both(s, z, c, own)
        each_line(lambda up: z_send(0, s, z, up, 1).wait_send())

    loop(STEPS, drain)


def attention(x, idt, wr, wq, wk, wv, wo, cut, ret):
    nseq, seq, d = x.shape
    rows, hd = wq.shape
    nd, k = d // rows, idt.shape[1]
    cols = d // LANES
    half = HEAD // 2
    freq = THETA ** (-jnp.arange(half, dtype=jnp.float32) / half)
    ang = jnp.arange(seq, dtype=jnp.float32)[:, None] * freq
    cos = jnp.concatenate([jnp.cos(ang)] * 2, axis=1)
    sin = jnp.concatenate([-jnp.sin(ang), jnp.sin(ang)], axis=1)
    vmem = pl.BlockSpec(memory_space=pltpu.VMEM)
    hbm = pl.BlockSpec(memory_space=pl.ANY)
    wide = hd // STEPS
    dma = pltpu.SemaphoreType.DMA
    bf = jnp.bfloat16

    def out(*shape, dtype=bf):
        return jax.ShapeDtypeStruct(shape, dtype)

    na, nb = nseq * cut, nseq * (seq - cut)
    return pl.pallas_call(
        functools.partial(attn_kernel, cut, ret),
        out_shape=(out(na + 3 * nseq * k // cols, cols, LANES), out(nb, cols, LANES),
                   out(nseq * ret, cols, LANES), out(nseq * (seq - ret), cols, LANES), out(nd, nseq, k, seq, dtype=jnp.int32), out(STEPS, 3, d, wide), out(hd, d)),
        in_specs=[hbm, hbm] + [vmem] * 3 + [hbm] * 4,
        out_specs=(vmem, vmem, vmem, vmem, hbm, hbm, hbm),
        scratch_shapes=[
            pltpu.VMEM((nseq, seq, d), bf), pltpu.VMEM((nseq * seq, d), bf), pltpu.VMEM((nseq * seq, d), jnp.float32),
            pltpu.VMEM((2, 3, d, wide), bf), pltpu.VMEM((2, hd // STEPS, d), bf),
            pltpu.VMEM((seq * (cols + 1), LANES), jnp.float32), pltpu.VMEM((nseq, k, seq), jnp.float32),
            pltpu.VMEM((nseq, k, seq), jnp.int32),
            *([dma((3, STEPS, REPLICAS))] * 3), *([dma((2, STEPS, REPLICAS))] * 6), dma((2, 2, STEPS, REPLICAS)), *([dma((2, STEPS, REPLICAS, REPLICAS))] * 2),
            *([dma((REPLICAS,))] * 4), *([dma((nd,))] * 2), dma((2, nd + 1)), dma((2,)),
        ],
        compiler_params=pltpu.CompilerParams(collective_id=0, has_side_effects=True, vmem_limit_bytes=VMEM),
        cost_estimate=cost(10 * nseq * seq * d * hd, 8 * d * hd),
    )(x, idt, cos, sin, wr, wq, wk, wv, wo)[:5]


def token_of(key):
    return lax.shift_right_logical(key, SLOT_BITS) & ((1 << TOKEN_BITS) - 1)


def moe_kernel(nt, stores, given, nblk_ref, be_ref, bb_ref, bn_ref, key_ref, gate_ref, u_hbm, w1_hbm, w3_hbm, w2_hbm, *refs):
    outs, (ub, acc, w1, w3, w2, xs, zs, lhs, usem, wsem, osem) = refs[given:-11], refs[-11:]
    cols = ub.shape[1]
    nexp = w1_hbm.shape[0]
    nblk = nblk_ref[0]

    def weights(e, slot):
        return (pltpu.make_async_copy(w1_hbm.at[e], w1.at[slot], wsem.at[slot, 0]),
                pltpu.make_async_copy(w3_hbm.at[e], w3.at[slot], wsem.at[slot, 1]),
                pltpu.make_async_copy(w2_hbm.at[e], w2.at[slot], wsem.at[slot, 2]))

    nd = u_hbm.shape[0]
    n = nt // nd
    for c in weights(0, 0):
        c.start()
    for dev in range(nd):
        pltpu.make_async_copy(u_hbm.at[dev, pl.ds(0, n)], ub.at[pl.ds(dev * n, n)], usem).start()

    def zero(i):
        acc[pl.ds(i * 8, 8)] = jnp.zeros((8,) + acc.shape[1:], jnp.float32)

    loop(acc.shape[0] // 8, zero)
    pltpu.make_async_copy(ub.at[pl.ds(0, nt)], ub.at[pl.ds(0, nt)], usem).wait()

    def gather(b, some):
        base = bb_ref[b]
        for i in some:
            t = token_of(key_ref[base + i])
            xs[pl.ds(i, cols, stride=PITCH), :] = ub[t].astype(jnp.float32)

    def scatter(base, n, rows):
        new = []
        for i in rows:
            key = key_ref[base + i]
            t = jnp.where(i < n, token_of(key), nt)
            new.append((t, acc[t] + gate_ref[key & ((1 << SLOT_BITS) - 1)] * zs[pl.ds(i, cols, stride=PITCH), :]))
        for t, v in new:
            acc[t] = v

    def eight(g):
        return [g * 8 + i for i in range(8)]

    loop(BM // 8, lambda g: gather(0, eight(g)))

    def body(b, e_prev):
        e = be_ref[b]
        slot = e % 2

        @pl.when(e != e_prev)
        def _():
            @pl.when(e + 1 < nexp)
            def _():
                for c in weights(e + 1, 1 - slot):
                    c.start()

            for c in weights(e, slot):
                c.wait()

        for k in range(cols):
            lhs[:, k * LANES:(k + 1) * LANES] = xs[k * PITCH:k * PITCH + BM, :].astype(jnp.bfloat16)
        gather(b + 1, range(BM))
        bp = jnp.maximum(b - 1, 0)
        base, valid = bb_ref[bp], jnp.where(b > 0, bn_ref[bp], 0)
        for g in range(BM // 8):
            scatter(base, valid, eight(g))
        x = lhs[...]
        a1 = jnp.dot(x, w1[slot], preferred_element_type=jnp.float32)
        a3 = jnp.dot(x, w3[slot], preferred_element_type=jnp.float32)
        act = (jax.nn.silu(a1) * a3).astype(jnp.bfloat16)
        z = jnp.dot(act, w2[slot], preferred_element_type=jnp.float32).astype(jnp.bfloat16).astype(jnp.float32)
        for k in range(cols):
            zs[k * PITCH:k * PITCH + BM, :] = z[:, k * LANES:(k + 1) * LANES]
        return e

    lax.fori_loop(0, nblk, body, -1)
    loop(BM // 8, lambda g: scatter(bb_ref[nblk - 1], bn_ref[nblk - 1], eight(g)))

    def store(i):
        m = n // 4

        def pack(g):
            for j in eight(g):
                ub[i * m + j] = acc[i * m + j].astype(jnp.bfloat16)

        loop(m // 8, pack)
        dev, b = i // 4, lax.rem(i, 4)
        for out, lo, hi, base in stores:
            pltpu.make_async_copy(ub.at[pl.ds(i * m + lo, hi - lo)], outs[out].at[dev, pl.ds(base + b * (hi - lo), hi - lo)],
                                  osem).start()

    loop(nd * 4, store)
    pltpu.make_async_copy(ub.at[pl.ds(0, nt)], ub.at[pl.ds(0, nt)], osem).wait()


def moe(nblk, be, bb, bn, keys, gates, u, n, w1, w3, w2, lengths, stores, *into):
    nd, _, cols, _ = u.shape
    nt = nd * n
    ne, d, f = w1.shape
    smem = pl.BlockSpec(memory_space=pltpu.SMEM)
    hbm = pl.BlockSpec(memory_space=pl.ANY)
    return pl.pallas_call(
        functools.partial(moe_kernel, nt, stores, len(into)),
        out_shape=[jax.ShapeDtypeStruct((nd, m, cols, LANES), jnp.bfloat16) for m in lengths],
        in_specs=[smem] * 6 + [hbm] * (4 + len(into)),
        out_specs=[hbm] * len(lengths),
        input_output_aliases={10 + i: i for i in range(len(into))},
        scratch_shapes=[
            pltpu.VMEM((nt + 8, cols, LANES), jnp.bfloat16),
            pltpu.VMEM((nt + 8, cols, LANES), jnp.float32),
            pltpu.VMEM((2, d, f), jnp.bfloat16),
            pltpu.VMEM((2, d, f), jnp.bfloat16),
            pltpu.VMEM((2, f, d), jnp.bfloat16),
            pltpu.VMEM((cols * PITCH, LANES), jnp.float32),
            pltpu.VMEM((cols * PITCH, LANES), jnp.float32),
            pltpu.VMEM((BM, d), jnp.bfloat16),
            pltpu.SemaphoreType.DMA,
            pltpu.SemaphoreType.DMA((2, 3)),
            pltpu.SemaphoreType.DMA,
        ],
        compiler_params=pltpu.CompilerParams(vmem_limit_bytes=VMEM),
        cost_estimate=cost(30000 * d * f, 6 * ne * d * f),
    )(nblk, be, bb, bn, keys, gates, u, w1, w3, w2, *into)


def back_kernel(ret, piece, part, h_ref, h_mid, raw_here, raw_cross, first_hbm, ha_ref, y_out, own, prt, raw, fin, fout, hs, yst, yfirst, firsts, tm, raw_s, raw_r,
                prt_s, prt_r, f_s, f_r, y_s, y_r, osem, lsem, csem):
    r, e = lax.axis_index('replica'), lax.axis_index('ep')
    z, c = e // 2, e % 2
    n = h_ref.shape[0]
    pieces = n // piece
    split = pieces // 4
    early = 4
    mid = (z + 2) // 3 + (5 - z) // 3 - 1
    low = z // 2
    on_mid, on_end = pl.when(mid == 1), pl.when(mid == 0)
    z_mid, z_end = 1 + low, 3 * low
    partner, across = (r, ep_at(z, 1 - c)), (r, ep_at(2 - low, c))
    to_end = (r, ep_at(z_end, c))
    others = [lax.rem(r + i, 4) for i in range(1, 4)]

    def far(i):
        return 2 + i + low * (-1 - 2 * i)

    def near(i):
        return 1 - i + low * (1 + 2 * i)

    def rows(p):
        return pl.ds(p * piece, piece)

    end, inner = mid == 0, mid == 1
    meet([(None, (q, e)) for q in others] + [(None, partner)] +
         [(end, (q, ep_at(z_mid, c))) for q in range(REPLICAS)] + [(end, (r, ep_at(z_mid, 1 - c)))] +
         [(inner, (q, ep_at(z_end, c))) for q in range(REPLICAS)] + [(inner, (r, ep_at(z_end, 1 - c))), (inner, across)], 9 + mid)

    def raw_send(i, core, p):
        return rcopy(part.at[ep_at(far(i), core), rows(p)], raw.at[i, c, rows(p)], raw_s.at[i, core, p], raw_r.at[i, c, p],
                     (r, ep_at(z_mid, core)))

    def raw_recv(i, core, p):
        ref = raw.at[i, core, rows(p)]
        return rcopy(ref, ref, raw_s.at[i, core, p], raw_r.at[i, core, p], (r, ep_at(z_end, core)))

    def prt_copy(chip, p):
        return rcopy(part.at[ep_at(chip, 1 - c), rows(p)], prt.at[chip, rows(p)], prt_s.at[chip, p], prt_r.at[chip, p], partner)

    def f_copy(i, p, onward):
        return rcopy(fout.at[2 * onward + i, rows(p)], fin.at[i, rows(p)], f_s.at[2 * onward + i, p], f_r.at[i, p],
                     to_end if onward else across)

    def load(chip):
        return pltpu.make_async_copy(part.at[ep_at(chip, c)], own.at[chip], osem.at[chip])

    def landed(i):
        j = i + low * (1 - 2 * i)
        rest = pl.ds(0, early * piece)
        return (pltpu.make_async_copy(raw_here.at[j], raw.at[i, c, rest], csem.at[i, 0]),
                pltpu.make_async_copy(raw_cross.at[j], raw.at[i, 1 - c, rest], csem.at[i, 1]))

    keep_h = pltpu.make_async_copy(h_mid, hs, csem.at[0, 0])

    def place(half):
        return pl.ds(0, ret) if half < 0 else pl.ds(ret + half * piece, piece)

    def y_copy(src, i, blk, half, f):
        return rcopy(src, y_out.at[r, place(half), :], y_s.at[i, blk, half + 1], y_r.at[r, half + 1], (blk, f))

    def y_local(src, half):
        return pltpu.make_async_copy(src, y_out.at[r, place(half), :], lsem.at[half + 1])

    def put(src, blk, half):
        pl.when(r == blk)(lambda: y_local(src, half).start())
        pl.when(r != blk)(lambda: y_copy(src, 1, blk, half, e).start())

    def each(fn, count=pieces):
        loop(count, fn)

    for i in range(CORES):
        load(near(i)).start()

    @on_end
    def _():
        keep_h.start()
        for i in range(CORES):
            each(lambda p: [raw_send(i, core, p + early).start() for core in range(CORES)], pieces - early)
            each(lambda p: prt_copy(near(i), p).start())

    @on_mid
    def _():
        for i in range(CORES):
            for copy in landed(i):
                copy.start()
            load(far(i)).start()
            each(lambda p: [prt_copy(far(i), p).start(), prt_copy(near(i), p).start()])

    keep_first = pltpu.make_async_copy(first_hbm, firsts, csem.at[2, 0])
    keep_first.start()

    def f32(v):
        return v.astype(jnp.float32)

    def add(chip, p, incoming, put_sum):
        prt_copy(chip, p).wait_recv()

        def some(j):
            s = pl.ds(p * piece + j * 4, 4)
            put_sum(j, s, f32(own[chip, s]) + f32(prt[chip, s]) + incoming(s))

        each(some, piece // 4)

    cols = h_ref.shape[1]
    pitch = cols + 1

    def to(out):
        def put_sum(j, s, v):
            out[s] = v

        return put_sum

    def to_tiles(j, s, v):
        for i in range(v.shape[0]):
            tm[pl.ds((j * v.shape[0] + i) * pitch, cols), :] = v[i]

    def to_rows(out, count):
        for k in range(cols):
            out[:, k * LANES:(k + 1) * LANES] = tm[pl.ds(k, count, stride=pitch), :].astype(jnp.bfloat16)

    def finish_first():
        keep_first.wait()
        for blk in range(REPLICAS):
            def some(j):
                s = pl.ds(blk * ret + j * 4, 4)
                v = f32(ha_ref[s])
                for dev in range(firsts.shape[0]):
                    v = v + f32(firsts[dev, s])
                to_tiles(j, s, v)

            each(some, ret // 4)
            to_rows(yfirst.at[blk], ret)
            put(yfirst.at[blk], blk, -1)

    @on_mid
    def _():
        for i in range(CORES):
            load(far(i)).wait()
            load(near(i)).wait()
            for copy in landed(i):
                copy.wait()

        def first(q):
            i, p = q // pieces, lax.rem(q, pieces)
            pl.when(p >= early)(lambda: [raw_recv(i, core, p).wait_recv() for core in range(CORES)][0])
            add(far(i), p, lambda s: f32(raw[i, 0, s]) + f32(raw[i, 1, s]), to(fout.at[i]))
            f_copy(i, p, 0).start()

        def second(q):
            i, p = q // pieces, lax.rem(q, pieces)
            f_copy(i, p, 0).wait_recv()
            add(near(i), p, lambda s: fin[i, s], to(fout.at[2 + i]))
            f_copy(i, p, 1).start()

        lag = 2

        def step(q):
            pl.when(q < 2 * pieces)(lambda: first(q))
            pl.when(q >= lag)(lambda: second(q - lag))

        each(step, 2 * pieces + lag)
        finish_first()

    @on_end
    def _():
        finish_first()
        for i in range(CORES):
            load(near(i)).wait()
            if i == 0:
                keep_h.wait()
            h = h_ref if i else hs

            def last(p):
                f_copy(i, p, 1).wait_recv()
                add(near(i), p, lambda s: fin[i, s] + f32(h[s]), to_tiles)
                src = yst.at[i, p]
                to_rows(src, piece)
                for blk in range(REPLICAS):
                    for half in range(split):
                        @pl.when(p == (early + blk * (split - 1) + half - 1 if half else blk))
                        def _():
                            if i:
                                put(src, blk, half)
                            else:
                                y_copy(src, i, blk, half, ep_at(z_mid, c)).start()

            each(last)

    @on_end
    def _():
        for i in range(CORES):
            each(lambda p: [raw_send(i, core, p + early).wait_send() for core in range(CORES)], pieces - early)
            each(lambda p: prt_copy(near(i), p).wait_send())
        for blk in range(REPLICAS):
            for half in range(split):
                y_copy(yst.at[0, 0], 0, blk, half, ep_at(z_mid, c)).wait_send()

    @on_mid
    def _():
        for i in range(CORES):
            each(lambda p: [prt_copy(far(i), p).wait_send(), prt_copy(near(i), p).wait_send(),
                            f_copy(i, p, 0).wait_send(), f_copy(i, p, 1).wait_send()])

    for blk in range(REPLICAS):
        for half in range(-1, split):
            src = yfirst.at[blk] if half < 0 else yst.at[1, 0]
            ref = y_out.at[blk, place(half), :]
            came = rcopy(ref, ref, y_s.at[1, blk, half + 1], y_r.at[blk, half + 1], (blk, e))
            sent_here = True if half < 0 else end

            def stayed():
                y_local(src, half).wait()

            def sent():
                y_copy(src, 1, blk, half, e).wait_send()

            pl.when((r == blk) & sent_here)(stayed)
            pl.when((r != blk) & sent_here)(sent)
            pl.when((r != blk) | jnp.logical_not(sent_here))(came.wait_recv)


def back(part, h, h_mid, raw_here, raw_cross, first, ha):
    _, n, cols, _ = part.shape
    ret = ha.shape[0] // REPLICAS
    seq = ret + n // REPLICAS
    piece = raw_here.shape[1] // REPLICAS
    vmem = pl.BlockSpec(memory_space=pltpu.VMEM)
    hbm = pl.BlockSpec(memory_space=pl.ANY)
    dma = pltpu.SemaphoreType.DMA
    pieces = n // piece
    split = pieces // REPLICAS

    def tiles(*lead, dtype=jnp.bfloat16):
        return pltpu.VMEM(lead + (n, cols, LANES), dtype)

    return pl.pallas_call(
        functools.partial(back_kernel, ret, piece),
        out_shape=jax.ShapeDtypeStruct((4, seq, cols * LANES), jnp.bfloat16),
        in_specs=[hbm, vmem] + [hbm] * 4 + [vmem],
        out_specs=hbm,
        scratch_shapes=[
            tiles(REPLICAS), tiles(REPLICAS), tiles(2, 2), tiles(2, dtype=jnp.float32), tiles(REPLICAS, dtype=jnp.float32), tiles(),
            pltpu.VMEM((2, pieces, piece, cols * LANES), jnp.bfloat16), pltpu.VMEM((REPLICAS, ret, cols * LANES), jnp.bfloat16),
            pltpu.VMEM(first.shape, jnp.bfloat16), pltpu.VMEM((ret * (cols + 1), LANES), jnp.float32),
            *([dma((2, 2, pieces))] * 2), *([dma((REPLICAS, pieces))] * 2), dma((REPLICAS, pieces)), dma((2, pieces)),
            dma((2, 4, split + 1)), dma((REPLICAS, split + 1)), dma((REPLICAS,)), dma((split + 1,)), dma((3, 2)),
        ],
        compiler_params=pltpu.CompilerParams(collective_id=1, has_side_effects=True, vmem_limit_bytes=VMEM),
    )(part, h, h_mid, raw_here, raw_cross, first, ha)


def block_plan(ids, me, ne):
    _, nseq, _, n = ids.shape
    le = ids - me * ne
    local = (le >= 0) & (le < ne)
    total = ids.size
    slot = lax.iota(jnp.int32, total).reshape(ids.shape)
    token = (lax.broadcasted_iota(jnp.int32, ids.shape, 0) * nseq + lax.broadcasted_iota(jnp.int32, ids.shape, 1)) * n
    token = token + lax.broadcasted_iota(jnp.int32, ids.shape, 3)
    key = (le << (SLOT_BITS + TOKEN_BITS)) | (token << SLOT_BITS) | slot
    none = jnp.iinfo(jnp.int32).max
    keys = lax.sort(jnp.where(local, key, none).reshape(-1), is_stable=False)
    experts = jnp.arange(ne, dtype=jnp.int32)
    counts = jnp.sum((le.reshape(-1)[None, :] == experts[:, None]).astype(jnp.int32), axis=1)
    low = (experts[None, :] < experts[:, None])
    first = jnp.sum(jnp.where(low, counts[None, :], 0), axis=1)
    nb = jnp.maximum((counts + BM - 1) // BM, 1)
    bfirst = jnp.sum(jnp.where(low, nb[None, :], 0), axis=1)
    maxb = total // BM + ne + 2
    b = jnp.arange(maxb, dtype=jnp.int32)
    inside = (b[:, None] >= bfirst[None, :]) & (b[:, None] < (bfirst + nb)[None, :])

    def of(v):
        return jnp.sum(jnp.where(inside, v[None, :], 0), axis=1)

    done = (b - of(bfirst)) * BM
    be, bb = of(experts), of(first) + done
    bn = jnp.clip(of(counts) - done, 0, BM)
    bb = jnp.where(jnp.any(inside, axis=1), bb, 0)
    keys = jnp.concatenate([jnp.where(keys == none, 0, keys), jnp.zeros((BM,), jnp.int32)])
    return jnp.sum(nb).reshape(1), be, bb, bn, keys


def solution(mesh):
    nd = mesh.shape['ep']
    tok = P(('replica', 'ep'), None, None)
    rows_ep = P('ep', None)
    by_expert = P('ep', None, None)
    cut, ret = CUT, RET

    def local(x, wq, wk, wv, wo, wr, w1, w3, w2, idx):
        b, s, d = x.shape
        k, ne = idx.shape[-1], w1.shape[0]
        me = lax.axis_index('ep')
        low, c = me // 4, me % 2
        cols = d // LANES
        tail, rest = cut - ret, s - cut
        ua, ub, ha, hb, ids = attention(x, idx.transpose(0, 2, 1), wr, wq, wk, wv, wo, cut, ret)
        plan_a, plan_b = block_plan(ids[..., :cut], me, ne), block_plan(ids[..., cut:], me, ne)
        u_all = lax.all_gather(ua, 'ep')
        u_all, plan_b = lax.optimization_barrier((u_all, plan_b))
        terms = u_all[:, b * cut:].reshape(nd, 3, b, k, s).astype(jnp.float32)
        gates = terms[:, 0] + terms[:, 1] + terms[:, 2]
        lengths = (b * ret, b * (tail + rest))
        part_a, part_b = moe(*plan_a, gates[..., :cut].reshape(-1), u_all, b * cut, w1, w3, w2, lengths,
                             ((0, 0, ret, 0), (1, ret, cut, 0)))
        early = part_b.reshape(-1, nd // 4, CORES, b * (tail + rest), cols, LANES)[:, :, :, :b * tail]
        far = lax.dynamic_index_in_dim(early, 1 - low, 0, False)
        here, cross = [lax.dynamic_index_in_dim(far, i, 1, False) for i in (c, 1 - c)]
        ub_all = lax.all_gather(ub, 'ep')
        part_a, part_b, here, cross, ub_all = lax.optimization_barrier((part_a, part_b, here, cross, ub_all))
        inward = [(0, 2), (1, 3), (6, 4), (7, 5)]
        here = lax.ppermute(here, 'ep', inward)
        cross = lax.ppermute(cross, 'ep', [(i, j ^ 1) for i, j in inward])
        h_mid = lax.ppermute(hb, 'ep', [(j, i) for i, j in inward])
        part_a = lax.all_to_all(part_a, 'ep', 0, 0, tiled=True)
        part_b, = moe(*plan_b, gates[..., cut:].reshape(-1), ub_all, b * rest, w1, w3, w2, lengths[1:],
                      ((0, 0, rest, b * tail),), part_b)
        return back(part_b, hb, h_mid, here, cross, part_a, ha)

    return jax.shard_map(local, mesh=mesh,
                         in_specs=(tok, rows_ep, rows_ep, rows_ep, rows_ep, P(None, None),
                                   by_expert, by_expert, by_expert, tok),
                         out_specs=tok, check_vma=False)
```

```python
import functools
import jax
import jax.numpy as jnp
from jax import lax
from jax.experimental import pallas as pl
from jax.experimental.pallas import tpu as pltpu
from jax.sharding import PartitionSpec as P

HEAD = 128
EPS = 1e-6
THETA = 10000.0
BM = 128
SLOTS = 3
PITCH = BM + 1
LANES = 128
VMEM = 60 * 1024 * 1024
CORES = 2
REPLICAS = 4
CUT = 56
RET = 32
STEPS = 8
SLOT_BITS, TOKEN_BITS = 15, 12


def loop(n, fn):
    def step(i, carry):
        fn(i)
        return carry

    lax.fori_loop(0, n, step, 0)


def cost(flops, moved):
    return pl.CostEstimate(flops=flops, bytes_accessed=moved, transcendentals=0)


def kept(fn, v, axis=-1):
    return fn(v, axis=axis, keepdims=True)


def odd(v):
    return lax.rem(v, 2)


def ep_at(z, c):
    return 2 * z + c


MESH_ID = pl.DeviceIdType.MESH


def rcopy(src, dst, ssem, rsem, dev):
    return pltpu.make_async_remote_copy(src_ref=src, dst_ref=dst, send_sem=ssem, recv_sem=rsem, device_id=dev,
                                        device_id_type=MESH_ID)


def meet(peers, count):
    barrier = pltpu.get_barrier_semaphore()
    for guard, dev in peers:
        def greet():
            pl.semaphore_signal(barrier, device_id=dev, device_id_type=MESH_ID)

        if guard is None:
            greet()
        else:
            pl.when(guard)(greet)
    pl.semaphore_wait(barrier, count)


def attn_kernel(cut, ret, x_hbm, idt_hbm, cos_ref, sin_ref, wr_ref, wq_ref, wk_ref, wv_ref, wo_ref,
                ua_ref, ub_ref, ha_ref, hb_ref, ids_out, gw, go,
                xg, a_ref, acc, wbuf, obuf, tm, gates, idv, zr, zp, zm, xr, yr, xs, ys, xd, yd, dr, pr, ps,
                x_s, x_r, i_s, i_r, j_s, j_r, lsem, csem):
    r, e = lax.axis_index('replica'), lax.axis_index('ep')
    nz, nq = 4, 4
    z, c = e // 2, e % 2
    e_p = ep_at(z, 1 - c)
    x, y = r // 2, r % 2
    r_x, r_y = (r + 2) % nq, r + 1 - 2 * y

    def line_quarter(x, y):
        return 2 - y + x * (4 * y - 2)

    mine = line_quarter(x, y)
    q_line = (mine, line_quarter(1 - x, y), line_quarter(x, 1 - y), line_quarter(1 - x, 1 - y))
    to_x, to_y = 2 + x, y
    q_pair = (mine, 3 - x, 1 - y, to_x + to_y - mine)

    def pairs(w, k):
        return w == 0 and k == 0

    def quarters(w, k):
        return q_pair if pairs(w, k) else q_line

    nd = ids_out.shape[0]
    rows, wide = wq_ref.shape[0], wq_ref.shape[1] // STEPS
    quarter = rows // nq
    orows = go.shape[0] // STEPS
    nseq, seq, d = x_hbm.shape
    partner, x_dev, y_dev = (r, e_p), (r_x, e), (r_y, e)
    srows = orows // nz

    def mod(v, m):
        return lax.rem(v, m)

    others = [mod(r + i, nq) for i in range(1, nq)]
    mates = [mod(e + i, nd) for i in range(1, nd)]
    meet([(None, (q, e)) for q in others] + [(None, (r, f)) for f in mates], len(others) + len(mates))

    for i, q in enumerate(others):
        rcopy(idt_hbm.at[q], ids_out.at[e, r], i_s.at[i], i_r.at[r], (q, e)).start()
        rcopy(x_hbm.at[q], xg.at[r], x_s.at[i], x_r.at[r], (q, e)).start()
    keep_ids = pltpu.make_async_copy(idt_hbm.at[r], ids_out.at[e, r], csem.at[0])
    keep_x = pltpu.make_async_copy(x_hbm.at[r], xg.at[r], csem.at[1])
    keep_ids.start()
    keep_x.start()

    def spread_ids():
        keep_ids.wait()
        for i, q in enumerate(others):
            rcopy(idt_hbm.at[q], ids_out.at[e, q], i_s.at[i], i_r.at[q], (q, e)).wait_recv()
        for i, f in enumerate(mates):
            rcopy(ids_out.at[e], ids_out.at[e], j_s.at[i], j_r.at[e], (r, f)).start()

    def prepare():
        keep_x.wait()
        for i, q in enumerate(others):
            rcopy(x_hbm.at[q], xg.at[q], x_s.at[i], x_r.at[q], (q, e)).wait_recv()

        def norm(b):
            x = xg[b].astype(jnp.float32)
            at = pl.ds(b * seq, seq)
            a_ref[at, :] = (x * lax.rsqrt(kept(jnp.mean, x * x) + EPS)).astype(jnp.bfloat16)
            acc[at, :] = x

        loop(nseq, norm)

    def piece(w, s, f, q):
        if w:
            return go.at[pl.ds(s * orows + f // 2 * srows + q * (srows // nq), srows // nq), :]
        return gw.at[s, :, pl.ds(f * rows + q * quarter, quarter), :]

    def half(w, s, zs, q, i):
        if w:
            n = srows // nq // 2
            return go.at[pl.ds(s * orows + zs * srows + (2 * q + i) * n, n), :]
        n = quarter // 2
        return gw.at[s, :, pl.ds(ep_at(zs, c) * rows + (2 * q + i) * n, n), :]

    def own_wo(s, lo, n):
        return wo_ref.at[pl.ds(s // 2 * srows + lo, n), :]

    def z_send(w, s, zs, up, second=0):
        ref = piece(w, s, ep_at(zs, c), q_pair[3] if second else mine)
        i = 2 if second else w
        return rcopy(ref, ref, (zp if up else zm).at[i, s, zs], zr.at[i, s, zs], (r, e + 2) if up else (r, e - 2))

    def xy_send(w, s, zs, q, ssem, rsem, dev):
        ref = piece(w, s, ep_at(zs, c), q)
        return rcopy(ref, ref, ssem.at[w, s, zs], rsem.at[w, s, zs], dev)

    def xd_send(w, s, zs, q):
        ref = half(w, s, zs, q, 1)
        return rcopy(ref, ref, xd.at[w, s, zs], dr.at[1, w, s, zs], x_dev)

    def yd_send(w, s, zs, q):
        ref = half(w, s, zs, q, 0)
        return rcopy(ref, ref, yd.at[w, s, zs], dr.at[0, w, s, zs], y_dev)

    def p_copy(w, s, zs, k, j, core):
        ref = piece(w, s, ep_at(zs, core), quarters(w, k)[j])
        return rcopy(ref, ref, ps.at[w, s, zs, j], pr.at[w, s, zs, j], partner)

    def p_whole(w, s, f):
        ref = go.at[pl.ds(s * orows + z * srows, srows), :] if w else gw.at[s, :, pl.ds(f * rows, rows), :]
        return rcopy(ref, ref, ps.at[w, s, z, 0], pr.at[w, s, z, 0], partner)

    def own_parts(s):
        out = []
        for t in range(nz):
            head = ep_at(t, odd(t + s)) * (STEPS // 2) + s // 2
            for m, w in enumerate((wq_ref, wk_ref, wv_ref)):
                out.append((w.at[:, pl.ds(head * HEAD, HEAD)], m, pl.ds(t * HEAD, HEAD)))
        return out

    def if_wo(s, zs, core, *fns):
        @pl.when(odd(zs + s + core) == 0)
        def _():
            for fn in fns:
                fn()

    def each_line(fn):
        pl.when(z > 0)(lambda: fn(False))
        pl.when(z < nz - 1)(lambda: fn(True))

    def each_side(k, fn):
        pl.when(z - k - 1 >= 0)(lambda: fn(z - k - 1, True))
        pl.when(z + k + 1 < nz)(lambda: fn(z + k + 1, False))

    def originate(s):
        def line(up):
            sem = zp if up else zm
            dev = (r, e + 2) if up else (r, e - 2)
            for i, q in ((0, mine), (2, q_pair[3])):
                for w, m, t in own_parts(s):
                    rcopy(w.at[pl.ds(q * quarter, quarter), :], gw.at[s, m, pl.ds(e * rows + q * quarter, quarter), t],
                          sem.at[i, s, z], zr.at[i, s, z], dev).start()
            if_wo(s, z, c, lambda: rcopy(own_wo(s, mine * (srows // nq), srows // nq), piece(1, s, e, mine), sem.at[1, s, z],
                                      zr.at[1, s, z], dev).start())

        each_line(line)
        for w, m, t in own_parts(s):
            rcopy(w, gw.at[s, m, pl.ds(e * rows, rows), t], ps.at[0, s, z, 0], pr.at[0, s, z, 0], partner).start()
        if_wo(s, z, c, lambda: rcopy(own_wo(s, 0, srows), go.at[pl.ds(s * orows + z * srows, srows), :], ps.at[1, s, z, 0],
                                     pr.at[1, s, z, 0], partner).start())

    def for_both(s, zs, core, fn):
        fn(0)
        if_wo(s, zs, core, lambda: fn(1))

    def along_z(s, k):
        def side(zs, up):
            def one(w):
                z_send(w, s, zs, up).wait_recv()
                pl.when(z < nz - 1 if up else z > 0)(lambda: z_send(w, s, zs, up).start())
                if pairs(w, k):
                    z_send(w, s, zs, up, 1).wait_recv()
                    p_copy(w, s, zs, k, 3, c).start()
                xy_send(w, s, zs, to_x if pairs(w, k) else mine, xs, xr, x_dev).start()
                xy_send(w, s, zs, to_y if pairs(w, k) else mine, ys, yr, y_dev).start()
                p_copy(w, s, zs, k, 0, c).start()

            for_both(s, zs, c, one)

        each_side(k, side)

    def across(s, k):
        def side(zs, up):
            def one(w):
                q = quarters(w, k)
                xy_send(w, s, zs, q[1], xs, xr, x_dev).wait_recv()
                if not pairs(w, k):
                    yd_send(w, s, zs, q[1]).start()
                p_copy(w, s, zs, k, 1, c).start()
                xy_send(w, s, zs, q[2], ys, yr, y_dev).wait_recv()
                if not pairs(w, k):
                    xd_send(w, s, zs, q[2]).start()
                p_copy(w, s, zs, k, 2, c).start()

            for_both(s, zs, c, one)

        each_side(k, side)

    def diagonal(s, k):
        def side(zs, up):
            def one(w):
                if not pairs(w, k):
                    xd_send(w, s, zs, q_line[3]).wait_recv()
                    yd_send(w, s, zs, q_line[3]).wait_recv()
                    p_copy(w, s, zs, k, 3, c).start()

            for_both(s, zs, c, one)

        each_side(k, side)

    def load(s, f):
        slot = odd(s)
        return pltpu.make_async_copy(gw.at[s, :, pl.ds(f * rows, rows), :], wbuf.at[slot, :, pl.ds(f * rows, rows), :],
                                     lsem.at[slot, f])

    def oload(s, src, t, n):
        slot = odd(s)
        return pltpu.make_async_copy(src, obuf.at[slot, pl.ds(t * srows, n), :], lsem.at[slot, nd])

    def collect(s):
        slot = odd(s)

        def side(k, zs):
            def one(w):
                for j in range(nq):
                    p_copy(w, s, zs, k, j, 1 - c).wait_recv()

            for_both(s, zs, 1 - c, one)

        for k in range(nz - 1):
            each_side(k, lambda zs, up: side(k, zs))
        p_whole(0, s, e_p).wait_recv()
        if_wo(s, z, 1 - c, lambda: p_whole(1, s, e_p).wait_recv())

        for f in range(nd):
            def near():
                for w, m, t in own_parts(s):
                    pltpu.make_async_copy(w, wbuf.at[slot, m, pl.ds(f * rows, rows), t], lsem.at[slot, f]).start()

            pl.when(f == e)(near)
            pl.when(f != e)(lambda: load(s, f).start())
        for t in range(nz):
            here = (t == z) & (odd(t + s + c) == 0)
            pl.when(here)(lambda: oload(s, own_wo(s, 0, srows), t, srows).start())
            pl.when(jnp.logical_not(here))(
                lambda: oload(s, go.at[pl.ds(s * orows + t * srows, srows), :], t, srows).start())

    def wait_loads(s):
        for f in range(nd):
            load(s, f).wait()
        oload(s, go.at[pl.ds(s * orows, orows), :], 0, orows).wait()

    pair = 2 * HEAD
    npair = wide // pair

    def compute(s, j):
        slot = odd(s)
        a = a_ref[...]
        cols = pl.ds(pl.multiple_of(j * pair, pair), pair)
        cos, sin = cos_ref[...], sin_ref[...]

        def rot(v):
            return (v * cos + pltpu.roll(v, HEAD // 2, 1) * sin).astype(jnp.bfloat16)

        q, k, v = [jnp.dot(a, wbuf[slot, m, :, cols], preferred_element_type=jnp.float32) for m in range(3)]
        v = v.astype(jnp.bfloat16)
        tri = lax.broadcasted_iota(jnp.int32, (seq, seq), 0) >= lax.broadcasted_iota(jnp.int32, (seq, seq), 1)
        heads = []
        for hh in range(CORES):
            hc = slice(hh * HEAD, (hh + 1) * HEAD)
            outs = []
            for b in range(nseq):
                rs = slice(b * seq, (b + 1) * seq)
                sc = lax.dot_general(rot(q[rs, hc]), rot(k[rs, hc]), (((1,), (1,)), ((), ())),
                                     preferred_element_type=jnp.float32)
                sc = jnp.where(tri, sc * HEAD ** -0.5, -jnp.inf)
                ex = jnp.exp(sc - kept(jnp.max, sc))
                p = (ex / kept(jnp.sum, ex)).astype(jnp.bfloat16)
                outs.append(jnp.dot(p, v[rs, hc], preferred_element_type=jnp.float32).astype(jnp.bfloat16))
            heads.append(jnp.concatenate(outs, axis=0))
        o = jnp.concatenate(heads, axis=1)
        acc[...] += jnp.dot(o, obuf[slot, cols, :], preferred_element_type=jnp.float32)

    def within(s, fn, *args):
        pl.when((s >= 0) & (s < STEPS))(lambda: fn(s, *args))

    originate(0)

    def turn(i):
        within(i + 1, originate)
        within(i - 3, wait_loads)

        def serve(k):
            within(i - 1, across, k)
            within(i, along_z, k)

        def work(j):
            within(i - 3, compute, j)

            @pl.when(j == 0)
            def _():
                within(i - 2, diagonal, 0)
                within(i - 2, diagonal, 1)
                serve(1)
                within(i - 2, diagonal, 2)
                within(i - 2, collect)

        serve(0)
        loop(npair, work)
        serve(2)
        pl.when(i == 1)(spread_ids)
        pl.when(i == 2)(prepare)

    loop(STEPS + 3, turn)

    keep_own = pltpu.make_async_copy(ids_out.at[e], idv, csem.at[0])
    keep_own.start()
    keep_own.wait()
    pitch = d // LANES + 1
    tile = pl.ds(0, d // LANES)

    def spill(v, *parts):
        for k in range(d // LANES):
            tm[pl.ds(k, seq, stride=pitch), :] = v[:, k * LANES:(k + 1) * LANES]

        def rows_to(ref, base, lo):
            def some(g):
                for i in range(8):
                    j = g * 8 + i
                    ref[base + j] = tm[pl.ds((lo + j) * pitch, d // LANES), :].astype(jnp.bfloat16)

            return some

        for ref, base, lo, hi in parts:
            loop((hi - lo) // 8, rows_to(ref, base, lo))

    def route(b):
        h = acc[pl.ds(b * seq, seq), :].astype(jnp.bfloat16).astype(jnp.float32)
        n = h * lax.rsqrt(kept(jnp.mean, h * h) + EPS)
        logits = jnp.dot(n, wr_ref[...], precision=lax.Precision.HIGHEST, preferred_element_type=jnp.float32).T
        expert = lax.broadcasted_iota(jnp.int32, logits.shape, 0)
        ids = idv[b]
        picked = jnp.concatenate([jnp.sum(jnp.where(expert == ids[k:k + 1, :], logits, 0.0), axis=0, keepdims=True)
                                  for k in range(ids.shape[0])], axis=0)
        ex = jnp.exp(picked - kept(jnp.max, picked, 0))
        gates[b] = ex / kept(jnp.sum, ex, 0)
        rest, tail = seq - cut, cut - ret
        spill(n, (ua_ref, b * cut, 0, cut), (ub_ref, b * rest, cut, seq))
        spill(h, (ha_ref, b * ret, 0, ret), (hb_ref, b * tail, ret, cut), (hb_ref, nseq * tail + b * rest, cut, seq))

    loop(nseq, route)
    left = gates[...].reshape(-1, LANES)
    per_tile = d // LANES
    for term in range(3):
        g = left.astype(jnp.bfloat16)
        left = left - g.astype(jnp.float32)
        for i in range(g.shape[0] // per_tile):
            ua_ref[nseq * cut + term * (g.shape[0] // per_tile) + i] = g[i * per_tile:(i + 1) * per_tile, :]

    for i, f in enumerate(mates):
        rcopy(ids_out.at[e], ids_out.at[f], j_s.at[i], j_r.at[f], (r, f)).wait()
    for i, q in enumerate(others):
        rcopy(idt_hbm.at[q], ids_out.at[e, r], i_s.at[i], i_r.at[r], (q, e)).wait_send()
        rcopy(x_hbm.at[q], xg.at[r], x_s.at[i], x_r.at[r], (q, e)).wait_send()

    def drain(s):
        def side(k, zs, up):
            def sent(w):
                pl.when(z < nz - 1 if up else z > 0)(lambda: z_send(w, s, zs, up).wait_send())
                for j in range(nq):
                    p_copy(w, s, zs, k, j, c).wait_send()
                xy_send(w, s, zs, mine, xs, xr, x_dev).wait_send()
                xy_send(w, s, zs, mine, ys, yr, y_dev).wait_send()
                if not pairs(w, k):
                    xd_send(w, s, zs, mine).wait_send()
                    yd_send(w, s, zs, mine).wait_send()

            for_both(s, zs, c, sent)

        for k in range(nz - 1):
            each_side(k, lambda zs, up: side(k, zs, up))

        def own(w):
            each_line(lambda up: z_send(w, s, z, up).wait_send())
            p_whole(w, s, e).wait_send()

        for_both(s, z, c, own)
        each_line(lambda up: z_send(0, s, z, up, 1).wait_send())

    loop(STEPS, drain)


def attention(x, idt, wr, wq, wk, wv, wo, cut, ret):
    nseq, seq, d = x.shape
    rows, hd = wq.shape
    nd, k = d // rows, idt.shape[1]
    cols = d // LANES
    half = HEAD // 2
    freq = THETA ** (-jnp.arange(half, dtype=jnp.float32) / half)
    ang = jnp.arange(seq, dtype=jnp.float32)[:, None] * freq
    cos = jnp.concatenate([jnp.cos(ang)] * 2, axis=1)
    sin = jnp.concatenate([-jnp.sin(ang), jnp.sin(ang)], axis=1)
    vmem = pl.BlockSpec(memory_space=pltpu.VMEM)
    hbm = pl.BlockSpec(memory_space=pl.ANY)
    wide = hd // STEPS
    dma = pltpu.SemaphoreType.DMA
    bf = jnp.bfloat16

    def out(*shape, dtype=bf):
        return jax.ShapeDtypeStruct(shape, dtype)

    na, nb = nseq * cut, nseq * (seq - cut)
    return pl.pallas_call(
        functools.partial(attn_kernel, cut, ret),
        out_shape=(out(na + 3 * nseq * k // cols, cols, LANES), out(nb, cols, LANES),
                   out(nseq * ret, cols, LANES), out(nseq * (seq - ret), cols, LANES), out(nd, nseq, k, seq, dtype=jnp.int32), out(STEPS, 3, d, wide), out(hd, d)),
        in_specs=[hbm, hbm] + [vmem] * 3 + [hbm] * 4,
        out_specs=(vmem, vmem, vmem, vmem, hbm, hbm, hbm),
        scratch_shapes=[
            pltpu.VMEM((nseq, seq, d), bf), pltpu.VMEM((nseq * seq, d), bf), pltpu.VMEM((nseq * seq, d), jnp.float32),
            pltpu.VMEM((2, 3, d, wide), bf), pltpu.VMEM((2, hd // STEPS, d), bf),
            pltpu.VMEM((seq * (cols + 1), LANES), jnp.float32), pltpu.VMEM((nseq, k, seq), jnp.float32),
            pltpu.VMEM((nseq, k, seq), jnp.int32),
            *([dma((3, STEPS, REPLICAS))] * 3), *([dma((2, STEPS, REPLICAS))] * 6), dma((2, 2, STEPS, REPLICAS)), *([dma((2, STEPS, REPLICAS, REPLICAS))] * 2),
            *([dma((REPLICAS,))] * 4), *([dma((nd,))] * 2), dma((2, nd + 1)), dma((2,)),
        ],
        compiler_params=pltpu.CompilerParams(collective_id=0, has_side_effects=True, vmem_limit_bytes=VMEM),
        cost_estimate=cost(10 * nseq * seq * d * hd, 8 * d * hd),
    )(x, idt, cos, sin, wr, wq, wk, wv, wo)[:5]


def token_of(key):
    return lax.shift_right_logical(key, SLOT_BITS) & ((1 << TOKEN_BITS) - 1)


def moe_kernel(nt, stores, given, nblk_ref, order_ref, be_ref, bb_ref, bn_ref, key_ref, gate_ref, u_hbm, w1_hbm, w3_hbm, w2_hbm, *refs):
    outs, (ub, acc, w1, w3, w2, xs, zs, lhs, usem, wsem, osem) = refs[given:-11], refs[-11:]
    cols = ub.shape[1]
    nexp = w1_hbm.shape[0]
    nblk = nblk_ref[0]

    def weights(turn):
        e, slot = order_ref[turn], lax.rem(turn, SLOTS)
        return (pltpu.make_async_copy(w1_hbm.at[e], w1.at[slot], wsem.at[slot, 0]),
                pltpu.make_async_copy(w3_hbm.at[e], w3.at[slot], wsem.at[slot, 1]),
                pltpu.make_async_copy(w2_hbm.at[e], w2.at[slot], wsem.at[slot, 2]))

    nd = u_hbm.shape[0]
    n = nt // nd
    for turn in range(SLOTS - 1):
        for c in weights(turn):
            c.start()
    for dev in range(nd):
        pltpu.make_async_copy(u_hbm.at[dev, pl.ds(0, n)], ub.at[pl.ds(dev * n, n)], usem).start()

    def zero(i):
        acc[pl.ds(i * 8, 8)] = jnp.zeros((8,) + acc.shape[1:], jnp.float32)

    loop(acc.shape[0] // 8, zero)
    pltpu.make_async_copy(ub.at[pl.ds(0, nt)], ub.at[pl.ds(0, nt)], usem).wait()

    def gather(b, some):
        base = bb_ref[b]
        for i in some:
            t = token_of(key_ref[base + i])
            xs[pl.ds(i, cols, stride=PITCH), :] = ub[t].astype(jnp.float32)

    def scatter(base, n, rows):
        new = []
        for i in rows:
            key = key_ref[base + i]
            t = jnp.where(i < n, token_of(key), nt)
            new.append((t, acc[t] + gate_ref[key & ((1 << SLOT_BITS) - 1)] * zs[pl.ds(i, cols, stride=PITCH), :]))
        for t, v in new:
            acc[t] = v

    def eight(g):
        return [g * 8 + i for i in range(8)]

    loop(BM // 8, lambda g: gather(0, eight(g)))

    def body(b, e_prev):
        e = be_ref[b]
        slot = lax.rem(e, SLOTS)

        @pl.when(e != e_prev)
        def _():
            @pl.when(e + SLOTS - 1 < nexp)
            def _():
                for c in weights(e + SLOTS - 1):
                    c.start()

            for c in weights(e):
                c.wait()

        for k in range(cols):
            lhs[:, k * LANES:(k + 1) * LANES] = xs[k * PITCH:k * PITCH + BM, :].astype(jnp.bfloat16)
        gather(b + 1, range(BM))
        bp = jnp.maximum(b - 1, 0)
        base, valid = bb_ref[bp], jnp.where(b > 0, bn_ref[bp], 0)
        for g in range(BM // 8):
            scatter(base, valid, eight(g))
        x = lhs[...]
        a1 = jnp.dot(x, w1[slot], preferred_element_type=jnp.float32)
        a3 = jnp.dot(x, w3[slot], preferred_element_type=jnp.float32)
        act = (jax.nn.silu(a1) * a3).astype(jnp.bfloat16)
        z = jnp.dot(act, w2[slot], preferred_element_type=jnp.float32).astype(jnp.bfloat16).astype(jnp.float32)
        for k in range(cols):
            zs[k * PITCH:k * PITCH + BM, :] = z[:, k * LANES:(k + 1) * LANES]
        return e

    lax.fori_loop(0, nblk, body, -1)
    loop(BM // 8, lambda g: scatter(bb_ref[nblk - 1], bn_ref[nblk - 1], eight(g)))

    def store(i):
        m = n // 4

        def pack(g):
            for j in eight(g):
                ub[i * m + j] = acc[i * m + j].astype(jnp.bfloat16)

        loop(m // 8, pack)
        dev, b = i // 4, lax.rem(i, 4)
        for out, lo, hi, base in stores:
            pltpu.make_async_copy(ub.at[pl.ds(i * m + lo, hi - lo)], outs[out].at[dev, pl.ds(base + b * (hi - lo), hi - lo)],
                                  osem).start()

    loop(nd * 4, store)
    pltpu.make_async_copy(ub.at[pl.ds(0, nt)], ub.at[pl.ds(0, nt)], osem).wait()


def moe(nblk, order, be, bb, bn, keys, gates, u, n, w1, w3, w2, lengths, stores, *into):
    nd, _, cols, _ = u.shape
    nt = nd * n
    ne, d, f = w1.shape
    smem = pl.BlockSpec(memory_space=pltpu.SMEM)
    hbm = pl.BlockSpec(memory_space=pl.ANY)
    return pl.pallas_call(
        functools.partial(moe_kernel, nt, stores, len(into)),
        out_shape=[jax.ShapeDtypeStruct((nd, m, cols, LANES), jnp.bfloat16) for m in lengths],
        in_specs=[smem] * 7 + [hbm] * (4 + len(into)),
        out_specs=[hbm] * len(lengths),
        input_output_aliases={11 + i: i for i in range(len(into))},
        scratch_shapes=[
            pltpu.VMEM((nt + 8, cols, LANES), jnp.bfloat16),
            pltpu.VMEM((nt + 8, cols, LANES), jnp.float32),
            pltpu.VMEM((SLOTS, d, f), jnp.bfloat16),
            pltpu.VMEM((SLOTS, d, f), jnp.bfloat16),
            pltpu.VMEM((SLOTS, f, d), jnp.bfloat16),
            pltpu.VMEM((cols * PITCH, LANES), jnp.float32),
            pltpu.VMEM((cols * PITCH, LANES), jnp.float32),
            pltpu.VMEM((BM, d), jnp.bfloat16),
            pltpu.SemaphoreType.DMA,
            pltpu.SemaphoreType.DMA((SLOTS, 3)),
            pltpu.SemaphoreType.DMA,
        ],
        compiler_params=pltpu.CompilerParams(vmem_limit_bytes=VMEM),
        cost_estimate=cost(30000 * d * f, 6 * ne * d * f),
    )(nblk, order, be, bb, bn, keys, gates, u, w1, w3, w2, *into)


def back_kernel(ret, piece, part, h_ref, h_mid, raw_here, raw_cross, first_hbm, ha_ref, y_out, own, prt, raw, fin, fout, hs, yst, yfirst, firsts, tm, raw_s, raw_r,
                prt_s, prt_r, f_s, f_r, y_s, y_r, osem, lsem, csem):
    r, e = lax.axis_index('replica'), lax.axis_index('ep')
    z, c = e // 2, e % 2
    n = h_ref.shape[0]
    pieces = n // piece
    split = pieces // 4
    early = 4
    mid = (z + 2) // 3 + (5 - z) // 3 - 1
    low = z // 2
    on_mid, on_end = pl.when(mid == 1), pl.when(mid == 0)
    z_mid, z_end = 1 + low, 3 * low
    partner, across = (r, ep_at(z, 1 - c)), (r, ep_at(2 - low, c))
    to_end = (r, ep_at(z_end, c))
    others = [lax.rem(r + i, 4) for i in range(1, 4)]

    def far(i):
        return 2 + i + low * (-1 - 2 * i)

    def near(i):
        return 1 - i + low * (1 + 2 * i)

    def rows(p):
        return pl.ds(p * piece, piece)

    end, inner = mid == 0, mid == 1
    meet([(None, (q, e)) for q in others] + [(None, partner)] +
         [(end, (q, ep_at(z_mid, c))) for q in range(REPLICAS)] + [(end, (r, ep_at(z_mid, 1 - c)))] +
         [(inner, (q, ep_at(z_end, c))) for q in range(REPLICAS)] + [(inner, (r, ep_at(z_end, 1 - c))), (inner, across)], 9 + mid)

    def raw_send(i, core, p):
        return rcopy(part.at[ep_at(far(i), core), rows(p)], raw.at[i, c, rows(p)], raw_s.at[i, core, p], raw_r.at[i, c, p],
                     (r, ep_at(z_mid, core)))

    def raw_recv(i, core, p):
        ref = raw.at[i, core, rows(p)]
        return rcopy(ref, ref, raw_s.at[i, core, p], raw_r.at[i, core, p], (r, ep_at(z_end, core)))

    def prt_copy(chip, p):
        return rcopy(part.at[ep_at(chip, 1 - c), rows(p)], prt.at[chip, rows(p)], prt_s.at[chip, p], prt_r.at[chip, p], partner)

    def f_copy(i, p, onward):
        return rcopy(fout.at[2 * onward + i, rows(p)], fin.at[i, rows(p)], f_s.at[2 * onward + i, p], f_r.at[i, p],
                     to_end if onward else across)

    def load(chip):
        return pltpu.make_async_copy(part.at[ep_at(chip, c)], own.at[chip], osem.at[chip])

    def landed(i):
        j = i + low * (1 - 2 * i)
        rest = pl.ds(0, early * piece)
        return (pltpu.make_async_copy(raw_here.at[j], raw.at[i, c, rest], csem.at[i, 0]),
                pltpu.make_async_copy(raw_cross.at[j], raw.at[i, 1 - c, rest], csem.at[i, 1]))

    keep_h = pltpu.make_async_copy(h_mid, hs, csem.at[0, 0])

    def place(half):
        return pl.ds(0, ret) if half < 0 else pl.ds(ret + half * piece, piece)

    def y_copy(src, i, blk, half, f):
        return rcopy(src, y_out.at[r, place(half), :], y_s.at[i, blk, half + 1], y_r.at[r, half + 1], (blk, f))

    def y_local(src, half):
        return pltpu.make_async_copy(src, y_out.at[r, place(half), :], lsem.at[half + 1])

    def put(src, blk, half):
        pl.when(r == blk)(lambda: y_local(src, half).start())
        pl.when(r != blk)(lambda: y_copy(src, 1, blk, half, e).start())

    def each(fn, count=pieces):
        loop(count, fn)

    for i in range(CORES):
        load(near(i)).start()

    @on_end
    def _():
        keep_h.start()
        for i in range(CORES):
            each(lambda p: [raw_send(i, core, p + early).start() for core in range(CORES)], pieces - early)
            each(lambda p: prt_copy(near(i), p).start())

    @on_mid
    def _():
        for i in range(CORES):
            for copy in landed(i):
                copy.start()
            load(far(i)).start()
            each(lambda p: [prt_copy(far(i), p).start(), prt_copy(near(i), p).start()])

    keep_first = pltpu.make_async_copy(first_hbm, firsts, csem.at[2, 0])
    keep_first.start()

    def f32(v):
        return v.astype(jnp.float32)

    def add(chip, p, incoming, put_sum):
        prt_copy(chip, p).wait_recv()

        def some(j):
            s = pl.ds(p * piece + j * 4, 4)
            put_sum(j, s, f32(own[chip, s]) + f32(prt[chip, s]) + incoming(s))

        each(some, piece // 4)

    cols = h_ref.shape[1]
    pitch = cols + 1

    def to(out):
        def put_sum(j, s, v):
            out[s] = v

        return put_sum

    def to_tiles(j, s, v):
        for i in range(v.shape[0]):
            tm[pl.ds((j * v.shape[0] + i) * pitch, cols), :] = v[i]

    def to_rows(out, count):
        for k in range(cols):
            out[:, k * LANES:(k + 1) * LANES] = tm[pl.ds(k, count, stride=pitch), :].astype(jnp.bfloat16)

    def finish_first():
        keep_first.wait()
        for blk in range(REPLICAS):
            def some(j):
                s = pl.ds(blk * ret + j * 4, 4)
                v = f32(ha_ref[s])
                for dev in range(firsts.shape[0]):
                    v = v + f32(firsts[dev, s])
                to_tiles(j, s, v)

            each(some, ret // 4)
            to_rows(yfirst.at[blk], ret)
            put(yfirst.at[blk], blk, -1)

    @on_mid
    def _():
        for i in range(CORES):
            load(far(i)).wait()
            load(near(i)).wait()
            for copy in landed(i):
                copy.wait()

        def first(q):
            i, p = q // pieces, lax.rem(q, pieces)
            pl.when(p >= early)(lambda: [raw_recv(i, core, p).wait_recv() for core in range(CORES)][0])
            add(far(i), p, lambda s: f32(raw[i, 0, s]) + f32(raw[i, 1, s]), to(fout.at[i]))
            f_copy(i, p, 0).start()

        def second(q):
            i, p = q // pieces, lax.rem(q, pieces)
            f_copy(i, p, 0).wait_recv()
            add(near(i), p, lambda s: fin[i, s], to(fout.at[2 + i]))
            f_copy(i, p, 1).start()

        lag = 4

        def step(q):
            pl.when(q < 2 * pieces)(lambda: first(q))
            pl.when(q >= lag)(lambda: second(q - lag))

        each(step, 2 * pieces + lag)
        finish_first()

    @on_end
    def _():
        finish_first()
        for i in range(CORES):
            load(near(i)).wait()
            if i == 0:
                keep_h.wait()
            h = h_ref if i else hs

            def last(p):
                f_copy(i, p, 1).wait_recv()
                add(near(i), p, lambda s: fin[i, s] + f32(h[s]), to_tiles)
                src = yst.at[i, p]
                to_rows(src, piece)
                for blk in range(REPLICAS):
                    for half in range(split):
                        @pl.when(p == (early + blk * (split - 1) + half - 1 if half else blk))
                        def _():
                            if i:
                                put(src, blk, half)
                            else:
                                y_copy(src, i, blk, half, ep_at(z_mid, c)).start()

            each(last)

    @on_end
    def _():
        for i in range(CORES):
            each(lambda p: [raw_send(i, core, p + early).wait_send() for core in range(CORES)], pieces - early)
            each(lambda p: prt_copy(near(i), p).wait_send())
        for blk in range(REPLICAS):
            for half in range(split):
                y_copy(yst.at[0, 0], 0, blk, half, ep_at(z_mid, c)).wait_send()

    @on_mid
    def _():
        for i in range(CORES):
            each(lambda p: [prt_copy(far(i), p).wait_send(), prt_copy(near(i), p).wait_send(),
                            f_copy(i, p, 0).wait_send(), f_copy(i, p, 1).wait_send()])

    for blk in range(REPLICAS):
        for half in range(-1, split):
            src = yfirst.at[blk] if half < 0 else yst.at[1, 0]
            ref = y_out.at[blk, place(half), :]
            came = rcopy(ref, ref, y_s.at[1, blk, half + 1], y_r.at[blk, half + 1], (blk, e))
            sent_here = True if half < 0 else end

            def stayed():
                y_local(src, half).wait()

            def sent():
                y_copy(src, 1, blk, half, e).wait_send()

            pl.when((r == blk) & sent_here)(stayed)
            pl.when((r != blk) & sent_here)(sent)
            pl.when((r != blk) | jnp.logical_not(sent_here))(came.wait_recv)


def back(part, h, h_mid, raw_here, raw_cross, first, ha):
    _, n, cols, _ = part.shape
    ret = ha.shape[0] // REPLICAS
    seq = ret + n // REPLICAS
    piece = raw_here.shape[1] // REPLICAS
    vmem = pl.BlockSpec(memory_space=pltpu.VMEM)
    hbm = pl.BlockSpec(memory_space=pl.ANY)
    dma = pltpu.SemaphoreType.DMA
    pieces = n // piece
    split = pieces // REPLICAS

    def tiles(*lead, dtype=jnp.bfloat16):
        return pltpu.VMEM(lead + (n, cols, LANES), dtype)

    return pl.pallas_call(
        functools.partial(back_kernel, ret, piece),
        out_shape=jax.ShapeDtypeStruct((4, seq, cols * LANES), jnp.bfloat16),
        in_specs=[hbm, vmem] + [hbm] * 4 + [vmem],
        out_specs=hbm,
        scratch_shapes=[
            tiles(REPLICAS), tiles(REPLICAS), tiles(2, 2), tiles(2, dtype=jnp.float32), tiles(REPLICAS, dtype=jnp.float32), tiles(),
            pltpu.VMEM((2, pieces, piece, cols * LANES), jnp.bfloat16), pltpu.VMEM((REPLICAS, ret, cols * LANES), jnp.bfloat16),
            pltpu.VMEM(first.shape, jnp.bfloat16), pltpu.VMEM((ret * (cols + 1), LANES), jnp.float32),
            *([dma((2, 2, pieces))] * 2), *([dma((REPLICAS, pieces))] * 2), dma((REPLICAS, pieces)), dma((2, pieces)),
            dma((2, 4, split + 1)), dma((REPLICAS, split + 1)), dma((REPLICAS,)), dma((split + 1,)), dma((3, 2)),
        ],
        compiler_params=pltpu.CompilerParams(collective_id=1, has_side_effects=True, vmem_limit_bytes=VMEM),
    )(part, h, h_mid, raw_here, raw_cross, first, ha)


def block_plan(ids, me, ne):
    _, nseq, _, n = ids.shape
    le = ids - me * ne
    local = (le >= 0) & (le < ne)
    total = ids.size
    experts = lax.iota(jnp.int32, ne)
    load = jnp.sum((le.reshape(1, -1) == experts[:, None]).astype(jnp.int32), axis=1)
    weight = load * ne + experts
    rank = jnp.sum((weight[None, :] > weight[:, None]).astype(jnp.int32), axis=1)
    turn = jnp.minimum(2 * rank, 2 * (ne - rank) - 1)
    is_turn = turn[None, :] == experts[:, None]
    order, counts = [jnp.sum(jnp.where(is_turn, v[None, :], 0), axis=1) for v in (experts, load)]
    at = sum(jnp.where(le == e, turn[e], 0) for e in range(ne))
    slot = lax.iota(jnp.int32, total).reshape(ids.shape)
    token = (lax.broadcasted_iota(jnp.int32, ids.shape, 0) * nseq + lax.broadcasted_iota(jnp.int32, ids.shape, 1)) * n
    token = token + lax.broadcasted_iota(jnp.int32, ids.shape, 3)
    key = (at << (SLOT_BITS + TOKEN_BITS)) | (token << SLOT_BITS) | slot
    none = jnp.iinfo(jnp.int32).max
    keys = lax.sort(jnp.where(local, key, none).reshape(-1), is_stable=False)
    low = (experts[None, :] < experts[:, None])
    first = jnp.sum(jnp.where(low, counts[None, :], 0), axis=1)
    nb = jnp.maximum((counts + BM - 1) // BM, 1)
    bfirst = jnp.sum(jnp.where(low, nb[None, :], 0), axis=1)
    maxb = total // BM + ne + 2
    b = jnp.arange(maxb, dtype=jnp.int32)
    inside = (b[:, None] >= bfirst[None, :]) & (b[:, None] < (bfirst + nb)[None, :])

    def of(v):
        return jnp.sum(jnp.where(inside, v[None, :], 0), axis=1)

    done = (b - of(bfirst)) * BM
    be, bb = of(experts), of(first) + done
    bn = jnp.clip(of(counts) - done, 0, BM)
    bb = jnp.where(jnp.any(inside, axis=1), bb, 0)
    keys = jnp.concatenate([jnp.where(keys == none, 0, keys), jnp.zeros((BM,), jnp.int32)])
    return jnp.sum(nb).reshape(1), order, be, bb, bn, keys


def solution(mesh):
    nd = mesh.shape['ep']
    tok = P(('replica', 'ep'), None, None)
    rows_ep = P('ep', None)
    by_expert = P('ep', None, None)
    cut, ret = CUT, RET

    def local(x, wq, wk, wv, wo, wr, w1, w3, w2, idx):
        b, s, d = x.shape
        k, ne = idx.shape[-1], w1.shape[0]
        me = lax.axis_index('ep')
        low, c = me // 4, me % 2
        cols = d // LANES
        tail, rest = cut - ret, s - cut
        ua, ub, ha, hb, ids = attention(x, idx.transpose(0, 2, 1), wr, wq, wk, wv, wo, cut, ret)
        plan_a, plan_b = block_plan(ids[..., :cut], me, ne), block_plan(ids[..., cut:], me, ne)
        u_all = lax.all_gather(ua, 'ep')
        u_all, plan_b = lax.optimization_barrier((u_all, plan_b))
        terms = u_all[:, b * cut:].reshape(nd, 3, b, k, s).astype(jnp.float32)
        gates = terms[:, 0] + terms[:, 1] + terms[:, 2]
        lengths = (b * ret, b * (tail + rest))
        part_a, part_b = moe(*plan_a, gates[..., :cut].reshape(-1), u_all, b * cut, w1, w3, w2, lengths,
                             ((0, 0, ret, 0), (1, ret, cut, 0)))
        early = part_b.reshape(-1, nd // 4, CORES, b * (tail + rest), cols, LANES)[:, :, :, :b * tail]
        far = lax.dynamic_index_in_dim(early, 1 - low, 0, False)
        here, cross = [lax.dynamic_index_in_dim(far, i, 1, False) for i in (c, 1 - c)]
        ub_all = lax.all_gather(ub, 'ep')
        part_a, part_b, here, cross, hb, ub_all = lax.optimization_barrier((part_a, part_b, here, cross, hb, ub_all))
        inward = [(0, 2), (1, 3), (6, 4), (7, 5)]
        here = lax.ppermute(here, 'ep', inward)
        cross = lax.ppermute(cross, 'ep', [(i, j ^ 1) for i, j in inward])
        h_mid = lax.ppermute(hb, 'ep', [(j, i) for i, j in inward])
        part_a = lax.all_to_all(part_a, 'ep', 0, 0, tiled=True)
        part_b, = moe(*plan_b, gates[..., cut:].reshape(-1), ub_all, b * rest, w1, w3, w2, lengths[1:],
                      ((0, 0, rest, b * tail),), part_b)
        return back(part_b, hb, h_mid, here, cross, part_a, ha)

    return jax.shard_map(local, mesh=mesh,
                         in_specs=(tok, rows_ep, rows_ep, rows_ep, rows_ep, P(None, None),
                                   by_expert, by_expert, by_expert, tok),
                         out_specs=tok, check_vma=False)
```
